8 devices in a mesh: dp: 4 (over z, y, x), tp: 2 (over core).
Axes of the slice: x: 2, y: 2, z: 1, core: 2. Of those that a mesh axis runs over, the one named last changes fastest.
Arguments:
- block_in: bfloat16 [3, 8, 2048, 1408], P(None, 'dp')
- pre_act: bfloat16 [3, 8, 2048, 6144], P(None, 'dp', None, 'tp')
- w_in: bfloat16 [3, 1408, 6144], P(None, None, 'tp')
- w_out: bfloat16 [3, 6144, 1408], P(None, 'tp')
- d_out: bfloat16 [8, 2048, 1408], P('dp')
- noise_in: float32 [3, 1408, 6144], P(None, None, 'tp')
- noise_out: float32 [3, 6144, 1408], P(None, 'tp')
- clip_norm: float32 [], replicated
- noise_mult: float32 [], replicated
Outputs:
- output 1: float32 [3, 1408, 6144], P(None, None, 'tp')
- output 2: float32 [3, 6144, 1408], P(None, 'tp')
All inputs are finite; a program needn't handle non-finite values.
Results may differ from the reference program's by a relative error of at most 0.00950181.
Values are sent between devices in bfloat16 or wider.
A program may use at most 1.5 GiB of HBM per device.

```python
import math
import jax
import jax.numpy as jnp
from jax import lax

NUM_LAYERS = 3
BATCH_SIZE = 8
SEQ_LEN = 2048
D_MODEL = 1408
D_FF = 6144

GAIN_IN = 0.7
GROWTH = 1.0 + 0.456 * GAIN_IN * GAIN_IN
GROWTH_SUM = (GROWTH ** NUM_LAYERS - 1.0) / (GROWTH - 1.0)
NORM_REF = math.sqrt(SEQ_LEN * D_MODEL * D_FF * (0.43 + 0.46 * D_MODEL / D_FF) * GROWTH_SUM)
NOISE_REF = math.sqrt(0.1 * BATCH_SIZE / (NUM_LAYERS * D_MODEL * D_FF))
ROW_COUNT = BATCH_SIZE * SEQ_LEN
INV_SQRT2 = 0.7071067811865476
INV_SQRT_2PI = 0.3989422804014327


def setup_inputs(seed: int = 0) -> dict:
    rng_keys = jax.random.split(jax.random.key(seed), 10)
    act_shape = (NUM_LAYERS, BATCH_SIZE, SEQ_LEN, D_MODEL)
    hid_shape = (NUM_LAYERS, BATCH_SIZE, SEQ_LEN, D_FF)
    in_shape = (NUM_LAYERS, D_MODEL, D_FF)
    out_shape = (NUM_LAYERS, D_FF, D_MODEL)
    block_in = jax.random.normal(rng_keys[0], act_shape, jnp.float32)
    pre_act = jax.random.normal(rng_keys[1], hid_shape, jnp.float32)
    w_in = jax.random.normal(rng_keys[2], in_shape, jnp.float32) * (GAIN_IN / math.sqrt(D_MODEL))
    w_out = jax.random.normal(rng_keys[3], out_shape, jnp.float32) * (1.0 / math.sqrt(D_FF))
    row_scale = 2.0 ** jax.random.uniform(rng_keys[4], (BATCH_SIZE, 1, 1), jnp.float32, -1.5, 1.5)
    d_out = jax.random.normal(rng_keys[5], (BATCH_SIZE, SEQ_LEN, D_MODEL), jnp.float32) * row_scale
    noise_in = jax.random.normal(rng_keys[6], in_shape, jnp.float32)
    noise_out = jax.random.normal(rng_keys[7], out_shape, jnp.float32)
    clip_norm = NORM_REF * jax.random.uniform(rng_keys[8], (), jnp.float32, 0.4, 0.7)
    noise_mult = NOISE_REF * 2.0 ** jax.random.uniform(rng_keys[9], (), jnp.float32, -3.0, -0.25)
    return {
        'block_in': block_in.astype(jnp.bfloat16),
        'pre_act': pre_act.astype(jnp.bfloat16),
        'w_in': w_in.astype(jnp.bfloat16),
        'w_out': w_out.astype(jnp.bfloat16),
        'd_out': d_out.astype(jnp.bfloat16),
        'noise_in': noise_in,
        'noise_out': noise_out,
        'clip_norm': clip_norm,
        'noise_mult': noise_mult,
    }


def gelu_parts(u_vals):
    u_wide = u_vals.astype(jnp.float32)
    norm_cdf = 0.5 * (1.0 + lax.erf(u_wide * INV_SQRT2))
    hidden = (u_wide * norm_cdf).astype(jnp.bfloat16)
    gelu_slope = norm_cdf + u_wide * jnp.exp(-0.5 * u_wide * u_wide) * INV_SQRT_2PI
    return hidden, gelu_slope


def example_norm(blocks):
    x_ex, h_ex, dh_ex, dz_ex = blocks
    gram_h = jnp.dot(h_ex, h_ex.T, preferred_element_type=jnp.float32)
    gram_z = jnp.dot(dz_ex, dz_ex.T, preferred_element_type=jnp.float32)
    gram_x = jnp.dot(x_ex, x_ex.T, preferred_element_type=jnp.float32)
    gram_d = jnp.dot(dh_ex, dh_ex.T, preferred_element_type=jnp.float32)
    return jnp.sum(gram_h * gram_z) + jnp.sum(gram_x * gram_d)


def reference(block_in, pre_act, w_in, w_out, d_out, noise_in, noise_out, clip_norm, noise_mult):
    def back_step(d_z, layer_in):
        x_layer, u_layer, w_first, w_second = layer_in
        hidden, gelu_slope = gelu_parts(u_layer)
        back_h = jnp.dot(d_z.reshape(ROW_COUNT, D_MODEL), w_second.T, preferred_element_type=jnp.float32)
        d_hid = (gelu_slope * back_h.reshape(BATCH_SIZE, SEQ_LEN, D_FF)).astype(jnp.bfloat16)
        back_x = jnp.dot(d_hid.reshape(ROW_COUNT, D_FF), w_first.T, preferred_element_type=jnp.float32)
        d_x = (d_z.astype(jnp.float32) + back_x.reshape(BATCH_SIZE, SEQ_LEN, D_MODEL)).astype(jnp.bfloat16)
        sq_layer = lax.map(example_norm, (x_layer, hidden, d_hid, d_z))
        return d_x, (hidden, d_hid, d_z, sq_layer)

    _, saved = lax.scan(back_step, d_out, (block_in[::-1], pre_act[::-1], w_in[::-1], w_out[::-1]))
    hiddens, d_hids, d_zs, sq_layers = [arr[::-1] for arr in saved]
    total_sq = jnp.sum(sq_layers, axis=0)
    clip_factor = jnp.minimum(1.0, clip_norm / jnp.sqrt(total_sq))
    scale_rows = clip_factor[:, None, None]
    noise_coef = noise_mult * clip_norm

    def layer_grads(blocks):
        x_layer, hidden, d_hid, d_z, n_first, n_second = blocks
        d_hid_c = (d_hid.astype(jnp.float32) * scale_rows).astype(jnp.bfloat16)
        d_z_c = (d_z.astype(jnp.float32) * scale_rows).astype(jnp.bfloat16)
        g_first = jnp.dot(x_layer.reshape(ROW_COUNT, D_MODEL).T, d_hid_c.reshape(ROW_COUNT, D_FF), preferred_element_type=jnp.float32)
        g_second = jnp.dot(hidden.reshape(ROW_COUNT, D_FF).T, d_z_c.reshape(ROW_COUNT, D_MODEL), preferred_element_type=jnp.float32)
        return (g_first + noise_coef * n_first) / BATCH_SIZE, (g_second + noise_coef * n_second) / BATCH_SIZE

    grad_in, grad_out = lax.map(layer_grads, (block_in, hiddens, d_hids, d_zs, noise_in, noise_out))
    return grad_in, grad_out
```

```python
import functools

import jax
import jax.numpy as jnp
from jax import lax
from jax.experimental import pallas as pl
from jax.experimental.pallas import tpu as pltpu
from jax.sharding import PartitionSpec as P


INV_SQRT2 = 0.7071067811865476
INV_SQRT_2PI = 0.3989422804014327
F_BLOCK = 512
T_CHUNK = 512
IN_CHUNK = 128
IN_SLOTS = 4
ROW_STEPS = 2
VMEM_LIMIT = 66_500_000

F32 = jnp.float32
BF16 = jnp.bfloat16
ANY = pl.ANY


def dot_nn(a, b):
    return lax.dot_general(a, b, (((1,), (0,)), ((), ())), preferred_element_type=F32)


def dot_nt(a, b):
    return lax.dot_general(a, b, (((1,), (1,)), ((), ())), preferred_element_type=F32)


def layer_kernel(first, last, n_steps, sc_ref, u_ref, w1_ref, w2_ref, x_hbm, dz_hbm, *refs):
    refs = list(refs)
    p_hbm, q_hbm = (None, None) if first else (refs.pop(0), refs.pop(0))
    refs.pop(0)
    if last:
        g1_hbm, g2_hbm = refs.pop(0), refs.pop(0)
    else:
        g1k_hbm, g1s_hbm, g2k_hbm, g2s_hbm, dx_hbm = [refs.pop(0) for _ in range(5)]
    dzo_hbm = None if (first or last) else refs.pop(0)
    ss_ref = refs.pop(0)
    x_t, dz, dz_t, dh, h, bh, x_st = [refs.pop(0) for _ in range(7)]
    p_st, q_st = (None, None) if first else (refs.pop(0), refs.pop(0))
    if last:
        g1_st, g2_st = refs.pop(0), refs.pop(0)
    else:
        acc, g1k_st, g1s_st, g2k_st, g2s_st = [refs.pop(0) for _ in range(5)]
    in_sem, out_sem = refs.pop(0), refs.pop(0)

    step = pl.program_id(0)
    layer, example, x_pos, y_pos = sc_ref[0], sc_ref[1], sc_ref[2], sc_ref[3]
    n_tok, d_model = dz.shape
    half_d = d_model // 2
    n_t = n_tok // T_CHUNK
    n_in = n_tok // IN_CHUNK

    def in_copies(c):
        slot = lax.rem(c, IN_SLOTS)
        rows = pl.ds(pl.multiple_of(c * IN_CHUNK, IN_CHUNK), IN_CHUNK)
        dz_src = dz_hbm.at[rows, :] if last else dz_hbm.at[example, rows, :]
        pairs = [(x_hbm.at[layer, example, rows, :], x_st.at[slot]), (dz_src, dz.at[rows, :])]
        if not first:
            pairs += [(p_hbm.at[rows, :], p_st.at[slot]), (q_hbm.at[rows, :], q_st.at[slot])]
        return [pltpu.make_async_copy(a, b, in_sem.at[k, slot]) for k, (a, b) in enumerate(pairs)]

    @pl.when(step == 0)
    def _():
        for c in range(IN_SLOTS - 1):
            for cp in in_copies(c):
                cp.start()
        if not last:
            acc[...] = jnp.zeros_like(acc)
        ss_ref[...] = jnp.zeros_like(ss_ref)

        def load(c, carry):
            @pl.when(c + IN_SLOTS - 1 < n_in)
            def _():
                for cp in in_copies(c + IN_SLOTS - 1):
                    cp.start()

            for cp in in_copies(c):
                cp.wait()
            slot = lax.rem(c, IN_SLOTS)
            at = pl.ds(pl.multiple_of(c * IN_CHUNK, IN_CHUNK), IN_CHUNK)
            x_t[:, at] = x_st[slot].T
            if first:
                z = dz[at, :]
            else:
                z = (dz[at, :].astype(F32) + (p_st[slot].astype(F32) + q_st[slot].astype(F32))).astype(BF16)
                dz[at, :] = z
            dz_t[:, at] = z.T
            return carry

        lax.fori_loop(0, n_in, load, 0)
        if dzo_hbm is not None:
            pltpu.make_async_copy(dz, dzo_hbm, out_sem.at[4]).start()

    for s in range(n_t + (1 if last else 2)):
        if s < n_t:
            bh[s % 2] = dot_nt(dz[pl.ds(s * T_CHUNK, T_CHUNK), :], w2_ref[0])
        if 1 <= s <= n_t:
            rows = pl.ds((s - 1) * T_CHUNK, T_CHUNK)
            u = u_ref[0, 0, rows, :].astype(F32)
            cdf = 0.5 * (1.0 + lax.erf(u * INV_SQRT2))
            h[rows, :] = (u * cdf).astype(BF16)
            slope = cdf + u * jnp.exp(-0.5 * u * u) * INV_SQRT_2PI
            dh[rows, :] = (slope * bh[(s - 1) % 2]).astype(BF16)
        if s >= 2 and not last:
            rows = pl.ds((s - 2) * T_CHUNK, T_CHUNK)
            acc[rows, :] = acc[rows, :] + dot_nt(dh[rows, :], w1_ref[0])

    cols = lambda k: pl.ds(pl.multiple_of(k * F_BLOCK, F_BLOCK), F_BLOCK)

    if last:
        def out_copies(k):
            yield pltpu.make_async_copy(g1_st, g1_hbm.at[:, cols(k)], out_sem.at[0]), None
            yield pltpu.make_async_copy(g2_st, g2_hbm.at[:, cols(k)], out_sem.at[1]), None
    else:
        fb = lambda k: lax.rem(k + (n_steps // 2) * (1 - y_pos), n_steps)

        def out_copies(k):
            yield pltpu.make_async_copy(g1k_st, g1k_hbm.at[:, cols(fb(k))], out_sem.at[0]), None
            yield pltpu.make_async_copy(g1s_st, g1s_hbm.at[:, cols(fb(k))], out_sem.at[1]), None
            yield pltpu.make_async_copy(g2s_st, g2s_hbm.at[:, cols(k)], out_sem.at[2]), k < n_steps // 2
            yield pltpu.make_async_copy(g2k_st, g2k_hbm.at[:, cols(k - n_steps // 2)], out_sem.at[3]), k >= n_steps // 2

    def run(copies, act):
        for cp, cond in copies:
            if cond is None:
                getattr(cp, act)()
            else:
                pl.when(cond)(getattr(cp, act))

    @pl.when(step > 0)
    def _():
        run(out_copies(step - 1), 'wait')

    def square(g):
        return jnp.sum((g * g).reshape(g.shape[0] // 8, 8, g.shape[1]), axis=0)

    def weight_grads(r, carry):
        quarter = half_d // ROW_STEPS
        a = pl.multiple_of(r * quarter, quarter)
        b = pl.multiple_of(r * quarter + half_d, quarter)
        if last:
            total = ss_ref[...]
            for at in (a, b):
                rows = pl.ds(at, quarter)
                g = dot_nn(x_t[rows, :], dh[...])
                g1_st[rows, :] = g
                total = total + square(g)
                g = dot_nn(dz_t[rows, :], h[...])
                g2_st[rows, :] = g
                total = total + square(g)
        else:
            own = pl.multiple_of(r * quarter + x_pos * half_d, quarter)
            far = pl.multiple_of(r * quarter + (1 - x_pos) * half_d, quarter)
            rows = pl.ds(a, quarter)
            g = dot_nn(x_t[pl.ds(own, quarter), :], dh[...])
            g1k_st[rows, :] = g
            total = ss_ref[...] + square(g)
            g = dot_nn(x_t[pl.ds(far, quarter), :], dh[...])
            g1s_st[rows, :] = g.astype(BF16)
            total = total + square(g)
            for at in (a, b):
                rows = pl.ds(at, quarter)
                g = dot_nn(dz_t[rows, :], h[...])
                g2k_st[rows, :] = g
                g2s_st[rows, :] = g.astype(BF16)
                total = total + square(g)
        ss_ref[...] = total
        return carry

    lax.fori_loop(0, ROW_STEPS, weight_grads, 0)
    run(out_copies(step), 'start')

    @pl.when(step == n_steps - 1)
    def _():
        if not last:
            def dx_copy(c):
                rows = pl.ds(pl.multiple_of(c * IN_CHUNK, IN_CHUNK), IN_CHUNK)
                slot = lax.rem(c, IN_SLOTS)
                return pltpu.make_async_copy(x_st.at[slot], dx_hbm.at[rows, :], in_sem.at[0, slot])

            def put(c, carry):
                @pl.when(c >= IN_SLOTS)
                def _():
                    dx_copy(c - IN_SLOTS).wait()

                rows = pl.ds(pl.multiple_of(c * IN_CHUNK, IN_CHUNK), IN_CHUNK)
                x_st[lax.rem(c, IN_SLOTS)] = acc[rows, :].astype(BF16)
                dx_copy(c).start()
                return carry

            lax.fori_loop(0, n_in, put, 0)
            for c in range(n_in - IN_SLOTS, n_in):
                dx_copy(c).wait()
        run(out_copies(step), 'wait')
        if dzo_hbm is not None:
            pltpu.make_async_copy(dz, dzo_hbm, out_sem.at[4]).wait()


def run_layer(kind, place, layer, example, pre_act, w_in, w_out, block_in, dz, parts, token):
    first, last = kind == 'first', kind == 'last'
    n_tok, d_model, d_ff = block_in.shape[2], block_in.shape[3], pre_act.shape[3]
    n_steps = d_ff // F_BLOCK
    half_d, half_f = d_model // 2, d_ff // 2

    def f_at(j, sc):
        return j if last else lax.rem(j + (n_steps // 2) * (1 - sc[3]), n_steps)

    in_specs = [
        pl.BlockSpec((1, 1, n_tok, F_BLOCK), lambda j, sc: (sc[0], sc[1], 0, f_at(j, sc))),
        pl.BlockSpec((1, d_model, F_BLOCK), lambda j, sc: (sc[0], 0, f_at(j, sc))),
        pl.BlockSpec((1, F_BLOCK, d_model), lambda j, sc: (sc[0], f_at(j, sc), 0)),
    ]
    extra = [block_in, dz, *parts, token]
    in_specs += [pl.BlockSpec(memory_space=ANY)] * len(extra)
    sds = jax.ShapeDtypeStruct
    scratch = [
        pltpu.VMEM((d_model, n_tok), BF16),
        pltpu.VMEM((n_tok, d_model), BF16),
        pltpu.VMEM((d_model, n_tok), BF16),
        pltpu.VMEM((n_tok, F_BLOCK), BF16),
        pltpu.VMEM((n_tok, F_BLOCK), BF16),
        pltpu.VMEM((2, T_CHUNK, F_BLOCK), F32),
        pltpu.VMEM((IN_SLOTS, IN_CHUNK, d_model), BF16),
    ]
    if not first:
        scratch += [pltpu.VMEM((IN_SLOTS, IN_CHUNK, d_model), BF16)] * 2
    if last:
        outs = [sds((d_model, d_ff), F32), sds((d_model, d_ff), F32)]
        scratch += [pltpu.VMEM((d_model, F_BLOCK), F32)] * 2
    else:
        outs = [
            sds((half_d, d_ff), F32), sds((half_d, d_ff), BF16),
            sds((d_model, half_f), F32), sds((d_model, half_f), BF16),
            sds((n_tok, d_model), BF16),
        ]
        if not first:
            outs.append(sds((n_tok, d_model), BF16))
        scratch += [
            pltpu.VMEM((n_tok, d_model), F32),
            pltpu.VMEM((half_d, F_BLOCK), F32), pltpu.VMEM((half_d, F_BLOCK), BF16),
            pltpu.VMEM((d_model, F_BLOCK), F32), pltpu.VMEM((d_model, F_BLOCK), BF16),
        ]
    scratch += [pltpu.SemaphoreType.DMA((4, IN_SLOTS)), pltpu.SemaphoreType.DMA((5,))]
    out_specs = [pl.BlockSpec(memory_space=ANY)] * len(outs)
    outs.append(sds((8, F_BLOCK), F32))
    out_specs.append(pl.BlockSpec((8, F_BLOCK), lambda j, sc: (0, 0)))
    n_dots = 3 if last else 4
    return pl.pallas_call(
        functools.partial(layer_kernel, first, last, n_steps),
        out_shape=outs,
        grid_spec=pltpu.PrefetchScalarGridSpec(
            num_scalar_prefetch=1, grid=(n_steps,), in_specs=in_specs, out_specs=out_specs, scratch_shapes=scratch),
        compiler_params=pltpu.CompilerParams(dimension_semantics=('arbitrary',), vmem_limit_bytes=VMEM_LIMIT),
        cost_estimate=pl.CostEstimate(
            flops=2 * n_dots * n_tok * d_model * d_ff, bytes_accessed=80_000_000, transcendentals=2 * n_tok * d_ff),
    )(jnp.stack([jnp.int32(layer), jnp.int32(example), place[0], place[1]]), pre_act, w_in, w_out, *extra)


def put_in_kernel(sc_ref, coef_ref, piece_ref, noise_ref, *rest):
    out_ref = rest[-1]
    out_ref[0, 0] = (piece_ref[...].astype(F32) + coef_ref[0] * noise_ref[0, 0]) * coef_ref[1]


def put_out_kernel(sc_ref, coef_ref, piece_ref, noise_ref, *rest):
    out_ref = rest[-1]
    out_ref[0, 0] = (piece_ref[...].astype(F32).T + coef_ref[0] * noise_ref[0, 0]) * coef_ref[1]


def put_piece(transposed, total, layer, quarter, coef, piece, noise):
    if transposed:
        rows, width = piece.shape[1], piece.shape[0]
        block = 256
        piece_spec = pl.BlockSpec((width, block), lambda i, sc: (0, i))
    else:
        rows, width = piece.shape
        block = rows // 2
        piece_spec = pl.BlockSpec((block, width), lambda i, sc: (i, 0))
    big_spec = pl.BlockSpec((1, 1, block, width), lambda i, sc: (sc[0], sc[1], i, 0))
    args = [jnp.stack([jnp.int32(layer), quarter]), coef, piece, noise]
    in_specs = [pl.BlockSpec(memory_space=pltpu.SMEM), piece_spec, big_spec]
    aliases = {}
    if total is not None:
        args.append(total)
        in_specs.append(pl.BlockSpec(memory_space=ANY))
        aliases = {4: 0}
    return pl.pallas_call(
        put_out_kernel if transposed else put_in_kernel,
        out_shape=jax.ShapeDtypeStruct(noise.shape, F32),
        grid_spec=pltpu.PrefetchScalarGridSpec(
            num_scalar_prefetch=1, grid=(rows // block,), in_specs=in_specs, out_specs=big_spec),
        input_output_aliases=aliases,
        compiler_params=pltpu.CompilerParams(dimension_semantics=('arbitrary',), vmem_limit_bytes=40_000_000),
        cost_estimate=pl.CostEstimate(flops=4 * rows * width, bytes_accessed=10 * rows * width, transcendentals=0),
        name='put_out' if transposed else 'put_in',
    )(*args)


def solution(mesh):
    data_size = mesh.shape['dp']
    swap_x = [(i, i ^ 1) for i in range(data_size)]
    swap_y = [(i, i ^ 2) for i in range(data_size)]

    def local_step(block_in, pre_act, w_in, w_out, d_out, noise_in, noise_out, clip_norm, noise_mult):
        n_layers, local_batch, _, d_model = block_in.shape
        d_ff = pre_act.shape[3]
        batch_total = local_batch * data_size
        dp = lax.axis_index('dp')
        x_pos, y_pos = lax.rem(dp, 2), dp // 2
        place = (x_pos, y_pos)
        over_x = lambda v: lax.ppermute(v, 'dp', swap_x)
        over_y = lambda v: lax.ppermute(v, 'dp', swap_y)
        over_tp = lambda v: lax.ppermute(v, 'tp', [(0, 1), (1, 0)])

        token = jnp.zeros((8, F_BLOCK), F32)
        d_z = [d_out] * local_batch
        parts = [()] * local_batch
        grads = [[None] * local_batch for _ in range(n_layers)]
        far = [[None] * local_batch for _ in range(n_layers)]
        sums = [[] for _ in range(local_batch)]
        for layer in range(n_layers - 1, -1, -1):
            kind = 'first' if layer == n_layers - 1 else ('last' if layer == 0 else 'mid')
            for ex in range(local_batch):
                res = run_layer(kind, place, layer, ex, pre_act, w_in, w_out, block_in, d_z[ex], parts[ex], token)
                token = res[-1]
                sums[ex].append(jnp.sum(token))
                if kind == 'last':
                    grads[layer][ex] = res[:2]
                else:
                    g1k, g1s, g2k, g2s, dx_part = res[:5]
                    grads[layer][ex] = (g1k, g2k)
                    parts[ex] = (dx_part, over_tp(dx_part))
                    far_x = over_x(g1s)
                    far_y = over_y(g2s)
                    far[layer][ex] = (far_x, far_y)
                    if kind == 'mid':
                        d_z[ex] = res[5]

        part_sq = jnp.stack([sum(s) for s in sums])
        part_all = lax.dynamic_update_slice(jnp.zeros((batch_total,), F32), part_sq, (dp * local_batch,))
        sq_norm = lax.psum(part_all, ('dp', 'tp'))
        clip = jnp.minimum(1.0, clip_norm / jnp.sqrt(sq_norm))
        at = lambda d: [lax.dynamic_index_in_dim(clip, d * local_batch + k, keepdims=False) for k in range(local_batch)]
        c_own, c_x, c_y = at(dp), at(dp ^ 1), at(dp ^ 2)
        mix = lambda cs, vs: sum(c * v.astype(F32) for c, v in zip(cs, vs))
        coef = jnp.stack([noise_mult * clip_norm, jnp.float32(1.0 / batch_total)])

        cut = lambda v, axis, pos: lax.dynamic_slice_in_dim(v, pos * (v.shape[axis] // 2), v.shape[axis] // 2, axis)
        noise_in4 = noise_in.reshape(n_layers, 4, d_model // 4, d_ff)
        noise_out4 = noise_out.reshape(n_layers, 4, d_ff // 4, d_model)
        grad_in = grad_out = None

        def half(layer, which, axis, pos, c_far, far_parts, part_pos):
            own = [grads[layer][k][which] for k in range(local_batch)]
            if layer == 0:
                own = [cut(v, axis, pos) for v in own]
            vals = [cut(v, axis, part_pos) for v in own]
            res = mix(c_own, vals)
            fp = [cut(v, axis, part_pos) for v in far_parts]
            return res + (mix(c_far, fp) if layer else fp[0].astype(F32))

        order = [2, 1, 0]
        last_far = [
            (over_x(mix(c_own, [cut(grads[0][k][0], 0, 1 - x_pos) for k in range(local_batch)]).astype(BF16)),),
            (over_y(mix(c_own, [cut(grads[0][k][1], 1, 1 - y_pos) for k in range(local_batch)]).astype(BF16)),),
        ]
        for layer in order:
            far1 = [far[layer][k][0] for k in range(local_batch)] if layer else last_far[0]
            far2 = [far[layer][k][1] for k in range(local_batch)] if layer else last_far[1]
            send1 = half(layer, 0, 0, x_pos, c_x, far1, 1 - y_pos).astype(BF16)
            send2 = half(layer, 1, 1, y_pos, c_y, far2, 1 - x_pos).astype(BF16)
            got1, got2 = over_y(send1), over_x(send2)
            own1 = (half(layer, 0, 0, x_pos, c_x, far1, y_pos) + got1.astype(F32)).astype(BF16)
            own2 = (half(layer, 1, 1, y_pos, c_y, far2, x_pos) + got2.astype(F32)).astype(BF16)
            near1, near2 = over_y(own1), over_x(own2)
            side1, side2 = over_x(own1), over_y(own2)
            diag1, diag2 = over_x(near1), over_y(near2)
            q1 = lambda a, b: 2 * a + b
            for a, b, v in ((x_pos, y_pos, own1), (x_pos, 1 - y_pos, near1), (1 - x_pos, y_pos, side1), (1 - x_pos, 1 - y_pos, diag1)):
                grad_in = put_piece(False, grad_in, layer, q1(a, b), coef, v, noise_in4)
            for a, b, v in ((y_pos, x_pos, own2), (y_pos, 1 - x_pos, near2), (1 - y_pos, x_pos, side2), (1 - y_pos, 1 - x_pos, diag2)):
                grad_out = put_piece(True, grad_out, layer, q1(a, b), coef, v, noise_out4)
        return grad_in.reshape(n_layers, d_model, d_ff), grad_out.reshape(n_layers, d_ff, d_model)


    return jax.shard_map(
        local_step,
        mesh=mesh,
        in_specs=(P(None, 'dp', None, None), P(None, 'dp', None, 'tp'), P(None, None, 'tp'), P(None, 'tp', None),
                  P('dp', None, None), P(None, None, 'tp'), P(None, 'tp', None), P(), P()),
        out_specs=(P(None, None, 'tp'), P(None, 'tp', None)),
        check_vma=False,
    )
```

```python
import functools

import jax
import jax.numpy as jnp
from jax import lax
from jax.experimental import pallas as pl
from jax.experimental.pallas import tpu as pltpu
from jax.sharding import PartitionSpec as P


INV_SQRT2 = 0.7071067811865476
INV_SQRT_2PI = 0.3989422804014327
LOG2_E = 1.4426950408889634
F_BLOCK = 512
T_CHUNK = 256
IN_SLOTS = 4
ROW_STEPS = 2
VMEM_LIMIT = 66_500_000

F32 = jnp.float32
BF16 = jnp.bfloat16
ANY = pl.ANY


def dot_nn(a, b):
    return lax.dot_general(a, b, (((1,), (0,)), ((), ())), preferred_element_type=F32)


def dot_nt(a, b):
    return lax.dot_general(a, b, (((1,), (1,)), ((), ())), preferred_element_type=F32)


def layer_kernel(first, last, n_steps, sc_ref, u_ref, w1_ref, w2_ref, x_hbm, dz_hbm, *refs):
    refs = list(refs)
    p_hbm, q_hbm = (None, None) if first else (refs.pop(0), refs.pop(0))
    refs.pop(0)
    if last:
        g1_hbm, g2_hbm = refs.pop(0), refs.pop(0)
    else:
        g1k_hbm, g1s_hbm, g2k_hbm, g2s_hbm, dx_hbm = [refs.pop(0) for _ in range(5)]
    dzo_hbm = None if (first or last) else refs.pop(0)
    ss_ref = refs.pop(0)
    x_t, dz, dz_t, dh, h, x_st = [refs.pop(0) for _ in range(6)]
    p_st, q_st = (None, None) if first else (refs.pop(0), refs.pop(0))
    if last:
        g1_st, g2_st = refs.pop(0), refs.pop(0)
    else:
        acc, g1k_st, g1s_st, g2k_st, g2s_st = [refs.pop(0) for _ in range(5)]
    in_sem, out_sem, io_sem = refs.pop(0), refs.pop(0), refs.pop(0)

    step = pl.program_id(0)
    layer, example, x_pos, y_pos = sc_ref[0], sc_ref[1], sc_ref[2], sc_ref[3]
    n_tok, d_model = dz.shape
    half_d = d_model // 2
    n_t = n_tok // T_CHUNK

    def in_copies(c):
        slot = c % IN_SLOTS
        rows = pl.ds(c * T_CHUNK, T_CHUNK)
        dz_src = dz_hbm.at[rows, :] if last else dz_hbm.at[example, rows, :]
        pairs = [(dz_src, dz.at[rows, :])]
        if not first:
            pairs += [(p_hbm.at[rows, :], p_st.at[slot]), (q_hbm.at[rows, :], q_st.at[slot])]
        pairs += [(x_hbm.at[layer, example, rows, :], x_st.at[slot])]
        return [pltpu.make_async_copy(a, b, in_sem.at[k, slot]) for k, (a, b) in enumerate(pairs)]

    def front(load):
        for s in range(n_t + (0 if last else 1)):
            rows = pl.ds(s * T_CHUNK, T_CHUNK)
            if load and s < n_t:
                if s + IN_SLOTS - 1 < n_t:
                    for cp in in_copies(s + IN_SLOTS - 1):
                        cp.start()
                for cp in in_copies(s):
                    cp.wait()
                slot = s % IN_SLOTS
                z = dz[rows, :]
                if not first:
                    z = (z.astype(F32) + (p_st[slot].astype(F32) + q_st[slot].astype(F32))).astype(BF16)
                    dz[rows, :] = z
                dz_t[:, rows] = z.T
                x_t[:, rows] = x_st[slot].T
            if s < n_t:
                u = u_ref[0, 0, rows, :].astype(F32)
                t = u * INV_SQRT2
                cdf = 0.5 * lax.erf(t) + 0.5
                h[rows, :] = (u * cdf).astype(BF16)
                slope = cdf + (t * (INV_SQRT_2PI / INV_SQRT2)) * jnp.exp2((t * t) * -LOG2_E)
                dh[rows, :] = (slope * dot_nt(dz[rows, :], w2_ref[0])).astype(BF16)
            if s >= 1 and not last:
                rows = pl.ds((s - 1) * T_CHUNK, T_CHUNK)
                part = dot_nt(dh[rows, :], w1_ref[0])
                acc[rows, :] = part if load else acc[rows, :] + part

    @pl.when(step == 0)
    def _():
        for c in range(IN_SLOTS - 1):
            for cp in in_copies(c):
                cp.start()
        ss_ref[...] = jnp.zeros_like(ss_ref)
        front(True)
        if dzo_hbm is not None:
            pltpu.make_async_copy(dz, dzo_hbm, io_sem.at[0]).start()

    @pl.when(step > 0)
    def _():
        front(False)

    if not last:
        @pl.when(step == n_steps - 1)
        def _():
            if dzo_hbm is not None:
                pltpu.make_async_copy(dz, dzo_hbm, io_sem.at[0]).wait()

            def put(c, carry):
                rows = pl.ds(pl.multiple_of(c * T_CHUNK, T_CHUNK), T_CHUNK)
                dz[rows, :] = acc[rows, :].astype(BF16)
                return carry

            lax.fori_loop(0, n_t, put, 0)
            pltpu.make_async_copy(dz, dx_hbm, io_sem.at[1]).start()

    cols = lambda k: pl.ds(pl.multiple_of(k * F_BLOCK, F_BLOCK), F_BLOCK)
    n_half = n_steps // 2

    def out_copies(k, r):
        def at(size):
            return pl.ds(pl.multiple_of(r * size, 16), size)

        half_rows, part_rows = at(half_d), at(half_d // ROW_STEPS)
        if last:
            return [
                (pltpu.make_async_copy(g1_st.at[half_rows, :], g1_hbm.at[half_rows, cols(k)], out_sem.at[0, r]), None),
                (pltpu.make_async_copy(g2_st.at[half_rows, :], g2_hbm.at[half_rows, cols(k)], out_sem.at[1, r]), None),
            ]
        fb = lax.rem(k + n_half * (1 - y_pos), n_steps)
        return [
            (pltpu.make_async_copy(g1k_st.at[part_rows, :], g1k_hbm.at[part_rows, cols(fb)], out_sem.at[0, r]), None),
            (pltpu.make_async_copy(g1s_st.at[part_rows, :], g1s_hbm.at[part_rows, cols(fb)], out_sem.at[1, r]), None),
            (pltpu.make_async_copy(g2s_st.at[half_rows, :], g2s_hbm.at[half_rows, cols(k)], out_sem.at[2, r]), k < n_half),
            (pltpu.make_async_copy(g2k_st.at[half_rows, :], g2k_hbm.at[half_rows, cols(k - n_half)], out_sem.at[3, r]), k >= n_half),
        ]

    def run(copies, act):
        for cp, cond in copies:
            if cond is None:
                getattr(cp, act)()
            else:
                pl.when(cond)(getattr(cp, act))

    @pl.when(step > 0)
    def _():
        for r in range(ROW_STEPS):
            run(out_copies(step - 1, r), 'wait')

    def square(g):
        return jnp.sum((g * g).reshape(g.shape[0] // 8, 8, g.shape[1]), axis=0)

    def weight_grads(r, carry):
        part = half_d // ROW_STEPS
        total = ss_ref[...]
        if last:
            for at in range(ROW_STEPS):
                rows = pl.ds(pl.multiple_of(r * half_d + at * part, part), part)
                g = dot_nn(x_t[rows, :], dh[...])
                g1_st[rows, :] = g
                total = total + square(g)
                g = dot_nn(dz_t[rows, :], h[...])
                g2_st[rows, :] = g
                total = total + square(g)
        else:
            own = pl.multiple_of(r * part + x_pos * half_d, part)
            far = pl.multiple_of(r * part + (1 - x_pos) * half_d, part)
            rows = pl.ds(pl.multiple_of(r * part, part), part)
            g = dot_nn(x_t[pl.ds(own, part), :], dh[...])
            g1k_st[rows, :] = g
            total = total + square(g)
            g = dot_nn(x_t[pl.ds(far, part), :], dh[...])
            g1s_st[rows, :] = g.astype(BF16)
            total = total + square(g)
            for at in range(ROW_STEPS):
                rows = pl.ds(pl.multiple_of(r * half_d + at * part, part), part)
                g = dot_nn(dz_t[rows, :], h[...])
                g2k_st[rows, :] = g
                g2s_st[rows, :] = g.astype(BF16)
                total = total + square(g)
        ss_ref[...] = total
        run(out_copies(step, r), 'start')
        return carry

    lax.fori_loop(0, ROW_STEPS, weight_grads, 0)

    @pl.when(step == n_steps - 1)
    def _():
        for r in range(ROW_STEPS):
            run(out_copies(step, r), 'wait')
        if not last:
            pltpu.make_async_copy(dz, dx_hbm, io_sem.at[1]).wait()


def run_layer(kind, place, layer, example, pre_act, w_in, w_out, block_in, dz, parts, token):
    first, last = kind == 'first', kind == 'last'
    n_tok, d_model, d_ff = block_in.shape[2], block_in.shape[3], pre_act.shape[3]
    n_steps = d_ff // F_BLOCK
    half_d, half_f = d_model // 2, d_ff // 2

    def f_at(j, sc):
        return j if last else lax.rem(j + (n_steps // 2) * (1 - sc[3]), n_steps)

    in_specs = [
        pl.BlockSpec((1, 1, n_tok, F_BLOCK), lambda j, sc: (sc[0], sc[1], 0, f_at(j, sc))),
        pl.BlockSpec((1, d_model, F_BLOCK), lambda j, sc: (sc[0], 0, f_at(j, sc))),
        pl.BlockSpec((1, F_BLOCK, d_model), lambda j, sc: (sc[0], f_at(j, sc), 0)),
    ]
    extra = [block_in, dz, *parts, token]
    in_specs += [pl.BlockSpec(memory_space=ANY)] * len(extra)
    sds = jax.ShapeDtypeStruct
    scratch = [
        pltpu.VMEM((d_model, n_tok), BF16),
        pltpu.VMEM((n_tok, d_model), BF16),
        pltpu.VMEM((d_model, n_tok), BF16),
        pltpu.VMEM((n_tok, F_BLOCK), BF16),
        pltpu.VMEM((n_tok, F_BLOCK), BF16),
        pltpu.VMEM((IN_SLOTS, T_CHUNK, d_model), BF16),
    ]
    if not first:
        scratch += [pltpu.VMEM((IN_SLOTS, T_CHUNK, d_model), BF16)] * 2
    if last:
        outs = [sds((d_model, d_ff), F32), sds((d_model, d_ff), F32)]
        scratch += [pltpu.VMEM((d_model, F_BLOCK), F32)] * 2
    else:
        outs = [
            sds((half_d, d_ff), F32), sds((half_d, d_ff), BF16),
            sds((d_model, half_f), F32), sds((d_model, half_f), BF16),
            sds((n_tok, d_model), BF16),
        ]
        if not first:
            outs.append(sds((n_tok, d_model), BF16))
        scratch += [
            pltpu.VMEM((n_tok, d_model), F32),
            pltpu.VMEM((half_d, F_BLOCK), F32), pltpu.VMEM((half_d, F_BLOCK), BF16),
            pltpu.VMEM((d_model, F_BLOCK), F32), pltpu.VMEM((d_model, F_BLOCK), BF16),
        ]
    scratch += [
        pltpu.SemaphoreType.DMA((4, IN_SLOTS)), pltpu.SemaphoreType.DMA((4, ROW_STEPS)), pltpu.SemaphoreType.DMA((2,)),
    ]
    out_specs = [pl.BlockSpec(memory_space=ANY)] * len(outs)
    outs.append(sds((8, F_BLOCK), F32))
    out_specs.append(pl.BlockSpec((8, F_BLOCK), lambda j, sc: (0, 0)))
    n_dots = 3 if last else 4
    return pl.pallas_call(
        functools.partial(layer_kernel, first, last, n_steps),
        out_shape=outs,
        grid_spec=pltpu.PrefetchScalarGridSpec(
            num_scalar_prefetch=1, grid=(n_steps,), in_specs=in_specs, out_specs=out_specs, scratch_shapes=scratch),
        compiler_params=pltpu.CompilerParams(dimension_semantics=('arbitrary',), vmem_limit_bytes=VMEM_LIMIT),
        cost_estimate=pl.CostEstimate(
            flops=2 * n_dots * n_tok * d_model * d_ff, bytes_accessed=80_000_000, transcendentals=2 * n_tok * d_ff),
    )(jnp.stack([jnp.int32(layer), jnp.int32(example), place[0], place[1]]), pre_act, w_in, w_out, *extra)


def put_in_kernel(sc_ref, coef_ref, piece_ref, noise_ref, *rest):
    out_ref = rest[-1]
    out_ref[0, 0] = (piece_ref[...].astype(F32) + coef_ref[0] * noise_ref[0, 0]) * coef_ref[1]


def put_out_kernel(sc_ref, coef_ref, piece_ref, noise_ref, *rest):
    out_ref = rest[-1]
    out_ref[0, 0] = (piece_ref[...].astype(F32).T + coef_ref[0] * noise_ref[0, 0]) * coef_ref[1]


def put_piece(transposed, total, layer, quarter, coef, piece, noise):
    if transposed:
        rows, width = piece.shape[1], piece.shape[0]
        block = 256
        piece_spec = pl.BlockSpec((width, block), lambda i, sc: (0, i))
    else:
        rows, width = piece.shape
        block = rows // 2
        piece_spec = pl.BlockSpec((block, width), lambda i, sc: (i, 0))
    big_spec = pl.BlockSpec((1, 1, block, width), lambda i, sc: (sc[0], sc[1], i, 0))
    args = [jnp.stack([jnp.int32(layer), quarter]), coef, piece, noise]
    in_specs = [pl.BlockSpec(memory_space=pltpu.SMEM), piece_spec, big_spec]
    aliases = {}
    if total is not None:
        args.append(total)
        in_specs.append(pl.BlockSpec(memory_space=ANY))
        aliases = {4: 0}
    return pl.pallas_call(
        put_out_kernel if transposed else put_in_kernel,
        out_shape=jax.ShapeDtypeStruct(noise.shape, F32),
        grid_spec=pltpu.PrefetchScalarGridSpec(
            num_scalar_prefetch=1, grid=(rows // block,), in_specs=in_specs, out_specs=big_spec),
        input_output_aliases=aliases,
        compiler_params=pltpu.CompilerParams(dimension_semantics=('arbitrary',), vmem_limit_bytes=40_000_000),
        cost_estimate=pl.CostEstimate(flops=4 * rows * width, bytes_accessed=10 * rows * width, transcendentals=0),
        name='put_out' if transposed else 'put_in',
    )(*args)


def solution(mesh):
    data_size = mesh.shape['dp']
    swap_x = [(i, i ^ 1) for i in range(data_size)]
    swap_y = [(i, i ^ 2) for i in range(data_size)]

    def local_step(block_in, pre_act, w_in, w_out, d_out, noise_in, noise_out, clip_norm, noise_mult):
        n_layers, local_batch, _, d_model = block_in.shape
        d_ff = pre_act.shape[3]
        batch_total = local_batch * data_size
        dp = lax.axis_index('dp')
        x_pos, y_pos = lax.rem(dp, 2), dp // 2
        place = (x_pos, y_pos)
        over_x = lambda v: lax.ppermute(v, 'dp', swap_x)
        over_y = lambda v: lax.ppermute(v, 'dp', swap_y)
        over_tp = lambda v: lax.ppermute(v, 'tp', [(0, 1), (1, 0)])

        token = jnp.zeros((8, F_BLOCK), F32)
        d_z = [d_out] * local_batch
        parts = [()] * local_batch
        grads = [[None] * local_batch for _ in range(n_layers)]
        far = [[None] * local_batch for _ in range(n_layers)]
        sums = [[] for _ in range(local_batch)]
        for layer in range(n_layers - 1, -1, -1):
            kind = 'first' if layer == n_layers - 1 else ('last' if layer == 0 else 'mid')
            for ex in range(local_batch):
                res = run_layer(kind, place, layer, ex, pre_act, w_in, w_out, block_in, d_z[ex], parts[ex], token)
                token = res[-1]
                sums[ex].append(jnp.sum(token))
                if kind == 'last':
                    grads[layer][ex] = res[:2]
                else:
                    g1k, g1s, g2k, g2s, dx_part = res[:5]
                    grads[layer][ex] = (g1k, g2k)
                    parts[ex] = (dx_part, over_tp(dx_part))
                    far_x = over_x(g1s)
                    far_y = over_y(g2s)
                    far[layer][ex] = (far_x, far_y)
                    if kind == 'mid':
                        d_z[ex] = res[5]

        part_sq = jnp.stack([sum(s) for s in sums])
        clip = jnp.minimum(1.0, clip_norm / jnp.sqrt(lax.psum(part_sq, 'tp')))
        clip_x, clip_y = over_x(clip), over_y(clip)
        c_own, c_x, c_y = [[v[k] for k in range(local_batch)] for v in (clip, clip_x, clip_y)]
        mix = lambda cs, vs: sum(c * v.astype(F32) for c, v in zip(cs, vs))
        coef = jnp.stack([noise_mult * clip_norm, jnp.float32(1.0 / batch_total)])

        cut = lambda v, axis, pos: lax.dynamic_slice_in_dim(v, pos * (v.shape[axis] // 2), v.shape[axis] // 2, axis)
        noise_in4 = noise_in.reshape(n_layers, 4, d_model // 4, d_ff)
        noise_out4 = noise_out.reshape(n_layers, 4, d_ff // 4, d_model)
        grad_in = grad_out = None

        def quarter(layer, which, half_pos, pos):
            vals = [grads[layer][k][which] for k in range(local_batch)]
            if layer == 0:
                vals = [cut(v, which, half_pos) for v in vals]
            return mix(c_own, [cut(v, which, pos) for v in vals])

        far_last = {}
        for first_send in (True, False):
            for which, over, half_pos, pos in ((0, over_x, 1 - x_pos, y_pos), (1, over_y, 1 - y_pos, x_pos)):
                at = 1 - pos if first_send else pos
                far_last[which, first_send] = over(quarter(0, which, half_pos, at).astype(BF16))

        def pair_sum(layer, which, half_pos, pos, to_send):
            at = 1 - pos if to_send else pos
            res = quarter(layer, which, half_pos, at)
            if layer == 0:
                return res + far_last[which, to_send].astype(F32)
            return res + mix(c_y if which else c_x, [cut(far[layer][k][which], which, at) for k in range(local_batch)])

        for layer in range(n_layers - 1, -1, -1):
            got1 = over_y(pair_sum(layer, 0, x_pos, y_pos, True).astype(BF16))
            got2 = over_x(pair_sum(layer, 1, y_pos, x_pos, True).astype(BF16))
            own1 = (pair_sum(layer, 0, x_pos, y_pos, False) + got1.astype(F32)).astype(BF16)
            own2 = (pair_sum(layer, 1, y_pos, x_pos, False) + got2.astype(F32)).astype(BF16)
            near1, near2 = over_y(own1), over_x(own2)
            side1, side2 = over_x(own1), over_y(own2)
            diag1, diag2 = over_x(near1), over_y(near2)
            q1 = lambda a, b: 2 * a + b
            for a, b, v in ((x_pos, y_pos, own1), (x_pos, 1 - y_pos, near1), (1 - x_pos, y_pos, side1), (1 - x_pos, 1 - y_pos, diag1)):
                grad_in = put_piece(False, grad_in, layer, q1(a, b), coef, v, noise_in4)
            for a, b, v in ((y_pos, x_pos, own2), (y_pos, 1 - x_pos, near2), (1 - y_pos, x_pos, side2), (1 - y_pos, 1 - x_pos, diag2)):
                grad_out = put_piece(True, grad_out, layer, q1(a, b), coef, v, noise_out4)
        return grad_in.reshape(n_layers, d_model, d_ff), grad_out.reshape(n_layers, d_ff, d_model)


    return jax.shard_map(
        local_step,
        mesh=mesh,
        in_specs=(P(None, 'dp', None, None), P(None, 'dp', None, 'tp'), P(None, None, 'tp'), P(None, 'tp', None),
                  P('dp', None, None), P(None, None, 'tp'), P(None, 'tp', None), P(), P()),
        out_specs=(P(None, None, 'tp'), P(None, 'tp', None)),
        check_vma=False,
    )
```

```python
import functools

import jax
import jax.numpy as jnp
from jax import lax
from jax.experimental import pallas as pl
from jax.experimental.pallas import tpu as pltpu
from jax.sharding import PartitionSpec as P

INV_SQRT2 = 0.7071067811865476
INV_SQRT_2PI = 0.3989422804014327
LOG2_E = 1.4426950408889634
F_BLOCK = 512
T_CHUNK = 256
IN_SLOTS = 3
ROW_STEPS = 2
VMEM_LIMIT = 66_500_000

F32 = jnp.float32
BF16 = jnp.bfloat16
ANY = pl.ANY
MESH = pl.DeviceIdType.MESH


def dot_nn(a, b):
    return lax.dot_general(a, b, (((1,), (0,)), ((), ())), preferred_element_type=F32)


def dot_nt(a, b):
    return lax.dot_general(a, b, (((1,), (1,)), ((), ())), preferred_element_type=F32)


def stack_kernel(n_layers, n_ex, n_steps, u_ref, w1_ref, w2_ref, x_hbm, dout_hbm,
                 p_hbm, q_hbm, dzo_hbm, g1k_hbm, g1s_hbm, g1r_hbm, g2k_hbm, g2s_hbm, g2r_hbm, g1l_hbm, g2l_hbm, ss_ref,
                 x_t, dz, dz_t, dh, h, acc, x_st, z_st, p_st, q_st, g1_st, g1s_st, g2_st, g2s_st,
                 in_sem, out_sem, io_sem, tp_send, tp_recv, far_send, far_recv):
    task, step = pl.program_id(0), pl.program_id(1)
    n_early = (n_layers - 1) * n_ex
    dp = lax.axis_index('dp')
    x_pos, y_pos = lax.rem(dp, 2), dp // 2
    x_far = {'dp': dp + 1 - 2 * x_pos}
    y_far = {'dp': dp + 2 - 4 * y_pos}
    tp_far = {'tp': 1 - lax.axis_index('tp')}
    n_tok, d_model = dz.shape
    half_d = d_model // 2
    n_half = n_steps // 2
    n_t = n_tok // T_CHUNK
    example = lax.rem(task, n_ex)
    cols = lambda k: pl.ds(pl.multiple_of(k * F_BLOCK, F_BLOCK), F_BLOCK)

    def in_start(t, c):
        slot, rows, ex = c % IN_SLOTS, pl.ds(c * T_CHUNK, T_CHUNK), lax.rem(t, n_ex)
        copy = lambda k, src, dst: pltpu.make_async_copy(src, dst.at[slot], in_sem.at[k, slot]).start()
        copy(0, x_hbm.at[n_layers - 1 - t // n_ex, ex, rows, :], x_st)

        @pl.when(t < n_early)
        def _():
            copy(1, dout_hbm.at[ex, rows, :], z_st)

        @pl.when(t >= n_early)
        def _():
            copy(1, dzo_hbm.at[ex, rows, :], z_st)

        @pl.when(t >= n_ex)
        def _():
            copy(2, p_hbm.at[t - n_ex, rows, :], p_st)
            copy(3, q_hbm.at[t - n_ex, rows, :], q_st)

    def in_wait(c):
        slot, rows = c % IN_SLOTS, pl.ds(c * T_CHUNK, T_CHUNK)
        wait = lambda k, dst: pltpu.make_async_copy(dout_hbm.at[0, rows, :], dst.at[slot], in_sem.at[k, slot]).wait()
        wait(0, x_st)
        wait(1, z_st)

        @pl.when(task >= n_ex)
        def _():
            wait(2, p_st)
            wait(3, q_st)

    def tp_copy(t):
        return pltpu.make_async_remote_copy(
            src_ref=p_hbm.at[t], dst_ref=q_hbm.at[t], send_sem=tp_send.at[t], recv_sem=tp_recv.at[t],
            device_id=tp_far, device_id_type=MESH)

    def front(load, to_dx):
        for s in range(n_t + (1 if to_dx else 0)):
            rows = pl.ds(s * T_CHUNK, T_CHUNK)
            if load and s < n_t:
                if s + IN_SLOTS - 1 < n_t:
                    in_start(task, s + IN_SLOTS - 1)
                in_wait(s)
                slot = s % IN_SLOTS
                z = z_st[slot]
                moved = (z.astype(F32) + (p_st[slot].astype(F32) + q_st[slot].astype(F32))).astype(BF16)
                z = jnp.where(task >= n_ex, moved, z) if to_dx else moved
                dz[rows, :] = z
                dz_t[:, rows] = z.T
                x_t[:, rows] = x_st[slot].T
            if s < n_t:
                u = u_ref[0, 0, rows, :].astype(F32)
                t = u * INV_SQRT2
                cdf = 0.5 * lax.erf(t) + 0.5
                h[rows, :] = (u * cdf).astype(BF16)
                slope = cdf + (t * (INV_SQRT_2PI / INV_SQRT2)) * jnp.exp2((t * t) * -LOG2_E)
                dh[rows, :] = (slope * dot_nt(dz[rows, :], w2_ref[0])).astype(BF16)
            if s >= 1 and to_dx:
                rows = pl.ds((s - 1) * T_CHUNK, T_CHUNK)
                part = dot_nt(dh[rows, :], w1_ref[0])
                acc[rows, :] = part if load else acc[rows, :] + part

    @pl.when((task == 0) & (step == 0))
    def _():
        ss_ref[...] = jnp.zeros_like(ss_ref)
        for c in range(IN_SLOTS - 1):
            in_start(task, c)

    for load in (True, False):
        for to_dx in (True, False):
            @pl.when(((step == 0) if load else (step > 0)) & ((task < n_early) if to_dx else (task >= n_early)))
            def _():
                front(load, to_dx)

    dz_keep = pltpu.make_async_copy(dz, dzo_hbm.at[example], io_sem.at[0])
    is_mid = (task >= n_ex) & (task < n_early)
    pl.when(is_mid & (step == 0))(dz_keep.start)
    ends_early = (step == n_steps - 1) & (task < n_early)
    dx_out = pltpu.make_async_copy(dz, p_hbm.at[task], io_sem.at[1])

    @pl.when(ends_early)
    def _():
        pl.when(is_mid)(dz_keep.wait)

        def put(c, carry):
            rows = pl.ds(pl.multiple_of(c * T_CHUNK, T_CHUNK), T_CHUNK)
            dz[rows, :] = acc[rows, :].astype(BF16)
            return carry

        lax.fori_loop(0, n_t, put, 0)
        dx_out.start()

    def out_copies(t, k, r):
        half_rows = pl.ds(pl.multiple_of(r * half_d, 16), half_d)
        part_rows = pl.ds(pl.multiple_of(r * (half_d // ROW_STEPS), 16), half_d // ROW_STEPS)
        early, k_half, k_col = t < n_early, k // n_half, lax.rem(k, n_half)
        copy = lambda n, src, dst: pltpu.make_async_copy(src, dst, out_sem.at[n, r])
        t_e, t_l = jnp.minimum(t, n_early - 1), jnp.maximum(t - n_early, 0)
        return [
            (early, copy(0, g1_st.at[part_rows, :], g1k_hbm.at[t_e, part_rows, cols(k)])),
            (early, copy(1, g1s_st.at[part_rows, :], g1s_hbm.at[t_e, part_rows, cols(k)])),
            (early & (k_half != y_pos), copy(2, g2s_st.at[half_rows, :], g2s_hbm.at[t_e, half_rows, cols(k_col)])),
            (early & (k_half == y_pos), copy(3, g2_st.at[half_rows, :], g2k_hbm.at[t_e, half_rows, cols(k_col)])),
            (~early, copy(0, g1_st.at[half_rows, :], g1l_hbm.at[t_l, half_rows, cols(k)])),
            (~early, copy(3, g2_st.at[half_rows, :], g2l_hbm.at[t_l, half_rows, cols(k)])),
        ]

    def far_x(src, dst):
        return pltpu.make_async_remote_copy(
            src_ref=src, dst_ref=dst, send_sem=far_send.at[0], recv_sem=far_recv.at[0], device_id=x_far, device_id_type=MESH)

    def far_y(src, dst):
        return pltpu.make_async_remote_copy(
            src_ref=src, dst_ref=dst, send_sem=far_send.at[1], recv_sem=far_recv.at[1], device_id=y_far, device_id_type=MESH)

    @pl.when((task > 0) | (step > 0))
    def _():
        t = jnp.where(step > 0, task, task - 1)
        k = jnp.where(step > 0, step - 1, n_steps - 1)
        for r in range(ROW_STEPS):
            for cond, cp in out_copies(t, k, r):
                pl.when(cond)(cp.wait)

        @pl.when(t < n_early)
        def _():
            far_x(g1s_hbm.at[t, :, cols(k)], g1r_hbm.at[t, :, cols(k)]).start()

        @pl.when((t < n_early) & (k // n_half != y_pos))
        def _():
            k_col = cols(lax.rem(k, n_half))
            far_y(g2s_hbm.at[t, :, k_col], g2r_hbm.at[t, :, k_col]).start()

    def square(g):
        return jnp.sum((g * g).reshape(g.shape[0] // 8, 8, g.shape[1]), axis=0)

    def weight_grads(early, r, carry):
        part = half_d // ROW_STEPS
        total = ss_ref[example]
        if early:
            own = pl.multiple_of(r * part + x_pos * half_d, part)
            far = pl.multiple_of(r * part + (1 - x_pos) * half_d, part)
            rows = pl.ds(pl.multiple_of(r * part, part), part)
            g = dot_nn(x_t[pl.ds(own, part), :], dh[...])
            g1_st[rows, :] = g
            total = total + square(g)
            g = dot_nn(x_t[pl.ds(far, part), :], dh[...])
            g1s_st[rows, :] = g.astype(BF16)
            total = total + square(g)
        for at in range(ROW_STEPS):
            rows = pl.ds(pl.multiple_of(r * half_d + at * part, part), part)
            if not early:
                g = dot_nn(x_t[rows, :], dh[...])
                g1_st[rows, :] = g
                total = total + square(g)
            g = dot_nn(dz_t[rows, :], h[...])
            g2_st[rows, :] = g
            if early:
                g2s_st[rows, :] = g.astype(BF16)
            total = total + square(g)
        ss_ref[example] = total
        for cond, cp in out_copies(task, step, r):
            pl.when(cond)(cp.start)
        return carry

    @pl.when(task < n_early)
    def _():
        lax.fori_loop(0, ROW_STEPS, functools.partial(weight_grads, True), 0)

    @pl.when(task >= n_early)
    def _():
        lax.fori_loop(0, ROW_STEPS, functools.partial(weight_grads, False), 0)

    @pl.when(ends_early)
    def _():
        dx_out.wait()
        tp_copy(task).start()

    @pl.when((step == n_steps - 1) & (task < n_early + n_ex - 1))
    def _():
        nxt = task + 1

        @pl.when(nxt >= n_ex)
        def _():
            tp_copy(nxt - n_ex).wait()

        for c in range(IN_SLOTS - 1):
            in_start(nxt, c)

    @pl.when((step == n_steps - 1) & (task == n_early + n_ex - 1))
    def _():
        for r in range(ROW_STEPS):
            for cond, cp in out_copies(task, step, r):
                pl.when(cond)(cp.wait)
        far_x(g1s_hbm, g1r_hbm).wait()
        far_y(g2s_hbm, g2r_hbm).wait()


def run_stack(pre_act, w_in, w_out, block_in, d_out):
    n_layers, n_ex, n_tok, d_model = block_in.shape
    d_ff = pre_act.shape[3]
    n_steps = d_ff // F_BLOCK
    half_d, half_f = d_model // 2, d_ff // 2
    n_early = (n_layers - 1) * n_ex
    top = n_layers - 1
    in_specs = [
        pl.BlockSpec((1, 1, n_tok, F_BLOCK), lambda t, j: (top - t // n_ex, lax.rem(t, n_ex), 0, j)),
        pl.BlockSpec((1, d_model, F_BLOCK),
                     lambda t, j: (jnp.maximum(top - t // n_ex, 1), 0, jnp.minimum(j + n_steps * (t // n_early), n_steps - 1))),
        pl.BlockSpec((1, F_BLOCK, d_model), lambda t, j: (top - t // n_ex, j, 0)),
        pl.BlockSpec(memory_space=ANY),
        pl.BlockSpec(memory_space=ANY),
    ]
    sds = jax.ShapeDtypeStruct
    outs = [
        sds((n_early, n_tok, d_model), BF16), sds((n_early, n_tok, d_model), BF16), sds((n_ex, n_tok, d_model), BF16),
        sds((n_early, half_d, d_ff), F32), sds((n_early, half_d, d_ff), BF16), sds((n_early, half_d, d_ff), BF16),
        sds((n_early, d_model, half_f), F32), sds((n_early, d_model, half_f), BF16), sds((n_early, d_model, half_f), BF16),
        sds((n_ex, d_model, d_ff), F32), sds((n_ex, d_model, d_ff), F32),
        sds((n_ex, 8, F_BLOCK), F32),
    ]
    out_specs = [pl.BlockSpec(memory_space=ANY)] * (len(outs) - 1) + [pl.BlockSpec((n_ex, 8, F_BLOCK), lambda t, j: (0, 0, 0))]
    vm = pltpu.VMEM
    scratch = [
        vm((d_model, n_tok), BF16), vm((n_tok, d_model), BF16), vm((d_model, n_tok), BF16),
        vm((n_tok, F_BLOCK), BF16), vm((n_tok, F_BLOCK), BF16), vm((n_tok, d_model), F32),
        *[vm((IN_SLOTS, T_CHUNK, d_model), BF16)] * 4,
        vm((d_model, F_BLOCK), F32), vm((half_d, F_BLOCK), BF16), vm((d_model, F_BLOCK), F32), vm((d_model, F_BLOCK), BF16),
        pltpu.SemaphoreType.DMA((4, IN_SLOTS)), pltpu.SemaphoreType.DMA((4, ROW_STEPS)), pltpu.SemaphoreType.DMA((2,)),
        pltpu.SemaphoreType.DMA((n_early,)), pltpu.SemaphoreType.DMA((n_early,)),
        pltpu.SemaphoreType.DMA((2,)), pltpu.SemaphoreType.DMA((2,)),
    ]
    n_dots = 4 * n_early + 3 * n_ex
    return pl.pallas_call(
        functools.partial(stack_kernel, n_layers, n_ex, n_steps),
        out_shape=outs,
        grid_spec=pltpu.PrefetchScalarGridSpec(
            num_scalar_prefetch=0, grid=(n_early + n_ex, n_steps), in_specs=in_specs, out_specs=out_specs, scratch_shapes=scratch),
        compiler_params=pltpu.CompilerParams(
            dimension_semantics=('arbitrary', 'arbitrary'), vmem_limit_bytes=VMEM_LIMIT, has_side_effects=True),
        cost_estimate=pl.CostEstimate(
            flops=2 * n_dots * n_tok * d_model * d_ff, bytes_accessed=500_000_000, transcendentals=2 * n_tok * d_ff),
        name='stack',
    )(pre_act, w_in, w_out, block_in, d_out)


def mix_kernel(sc_ref, coef_ref, *refs):
    total = refs[0][0].astype(F32) * coef_ref[0]
    for k, ref in enumerate(refs[1:-1]):
        total = total + ref[0].astype(F32) * coef_ref[k + 1]
    refs[-1][...] = total.astype(BF16)


def mix(which, shape, terms, coefs):
    rows, width = shape
    block = (rows // 2, width) if which == 0 else (rows // 4, width)

    def spec(k, lead):
        if which == 0:
            return pl.BlockSpec((1, *block), lambda i, sc: (lead, 2 * sc[k] + i, 0))
        return pl.BlockSpec((1, *block), lambda i, sc: (lead, i, sc[k]))

    out_map = lambda i, sc: (i, 0)
    places = jnp.stack([jnp.asarray(p, jnp.int32) for _, _, p in terms])
    return pl.pallas_call(
        mix_kernel,
        out_shape=jax.ShapeDtypeStruct((rows, width), BF16),
        grid_spec=pltpu.PrefetchScalarGridSpec(
            num_scalar_prefetch=1, grid=(rows // block[0],),
            in_specs=[pl.BlockSpec(memory_space=pltpu.SMEM)] + [spec(k, lead) for k, (_, lead, _) in enumerate(terms)],
            out_specs=pl.BlockSpec(block, out_map)),
        compiler_params=pltpu.CompilerParams(dimension_semantics=('arbitrary',), vmem_limit_bytes=40_000_000),
        cost_estimate=pl.CostEstimate(flops=2 * len(terms) * rows * width, bytes_accessed=14 * rows * width, transcendentals=0),
        name='mix',
    )(places, jnp.stack([jnp.asarray(c, F32) for c in coefs]), *[v for v, _, _ in terms])


def put_in_kernel(sc_ref, coef_ref, piece_ref, noise_ref, *rest):
    out_ref = rest[-1]
    out_ref[0, 0] = (piece_ref[...].astype(F32) + coef_ref[0] * noise_ref[0, 0]) * coef_ref[1]


def put_out_kernel(sc_ref, coef_ref, piece_ref, noise_ref, *rest):
    out_ref = rest[-1]
    out_ref[0, 0] = (piece_ref[...].astype(F32).T + coef_ref[0] * noise_ref[0, 0]) * coef_ref[1]


def put_piece(transposed, total, layer, quarter, coef, piece, noise):
    if transposed:
        rows, width = piece.shape[1], piece.shape[0]
        block = 256
        piece_spec = pl.BlockSpec((width, block), lambda i, sc: (0, i))
    else:
        rows, width = piece.shape
        block = rows // 2
        piece_spec = pl.BlockSpec((block, width), lambda i, sc: (i, 0))
    big_spec = pl.BlockSpec((1, 1, block, width), lambda i, sc: (sc[0], sc[1], i, 0))
    args = [jnp.stack([jnp.int32(layer), quarter]), coef, piece, noise]
    in_specs = [pl.BlockSpec(memory_space=pltpu.SMEM), piece_spec, big_spec]
    aliases = {}
    if total is not None:
        args.append(total)
        in_specs.append(pl.BlockSpec(memory_space=ANY))
        aliases = {4: 0}
    return pl.pallas_call(
        put_out_kernel if transposed else put_in_kernel,
        out_shape=jax.ShapeDtypeStruct(noise.shape, F32),
        grid_spec=pltpu.PrefetchScalarGridSpec(
            num_scalar_prefetch=1, grid=(rows // block,), in_specs=in_specs, out_specs=big_spec),
        input_output_aliases=aliases,
        compiler_params=pltpu.CompilerParams(dimension_semantics=('arbitrary',), vmem_limit_bytes=40_000_000),
        cost_estimate=pl.CostEstimate(flops=4 * rows * width, bytes_accessed=10 * rows * width, transcendentals=0),
        name='put_out' if transposed else 'put_in',
    )(*args)


def solution(mesh):
    data_size = mesh.shape['dp']
    swap_x = [(i, i ^ 1) for i in range(data_size)]
    swap_y = [(i, i ^ 2) for i in range(data_size)]

    def local_step(block_in, pre_act, w_in, w_out, d_out, noise_in, noise_out, clip_norm, noise_mult):
        n_layers, local_batch, _, d_model = block_in.shape
        d_ff = pre_act.shape[3]
        batch_total = local_batch * data_size
        dp = lax.axis_index('dp')
        x_pos, y_pos = lax.rem(dp, 2), dp // 2
        over_x = lambda v: lax.ppermute(v, 'dp', swap_x)
        over_y = lambda v: lax.ppermute(v, 'dp', swap_y)
        res = run_stack(pre_act, w_in, w_out, block_in, d_out)
        g1k, _, g1r, g2k, _, g2r, g1l, g2l, squares = res[3:]
        part_sq = jnp.sum(squares, axis=(1, 2))
        clip = jnp.minimum(1.0, clip_norm / jnp.sqrt(lax.psum(part_sq, 'tp')))
        clip_x, clip_y = over_x(clip), over_y(clip)
        c_own, c_x, c_y = [[v[k] for k in range(local_batch)] for v in (clip, clip_x, clip_y)]
        coef = jnp.stack([noise_mult * clip_norm, jnp.float32(1.0 / batch_total)])

        noise_in4 = noise_in.reshape(n_layers, 4, d_model // 4, d_ff)
        noise_out4 = noise_out.reshape(n_layers, 4, d_ff // 4, d_model)
        grad_in = grad_out = None

        shapes = ((d_model // 4, d_ff), (d_model, d_ff // 4))
        at_half, at_side = (x_pos, y_pos), (y_pos, x_pos)
        over_half, over_side = (over_x, over_y), (over_y, over_x)
        early, early_far, late = (g1k, g2k), (g1r, g2r), (g1l, g2l)

        def own_terms(layer, which, half_pos, pos):
            if layer == 0:
                return [(late[which], k, 2 * half_pos + pos) for k in range(local_batch)]
            first = (n_layers - 1 - layer) * local_batch
            return [(early[which], first + k, pos) for k in range(local_batch)]

        far_last = {}
        for to_send in (True, False):
            for which in (0, 1):
                pos = 1 - at_side[which] if to_send else at_side[which]
                piece = mix(which, shapes[which], own_terms(0, which, 1 - at_half[which], pos), c_own)
                far_last[which, to_send] = over_half[which](piece)

        def pair_sum(layer, which, to_send, *more):
            pos = 1 - at_side[which] if to_send else at_side[which]
            terms, coefs = own_terms(layer, which, at_half[which], pos), list(c_own)
            if layer == 0:
                more = (far_last[which, to_send], *more)
            else:
                first = (n_layers - 1 - layer) * local_batch
                terms += [(early_far[which], first + k, pos) for k in range(local_batch)]
                coefs += c_y if which else c_x
            terms += [(v[None], 0, 0) for v in more]
            return mix(which, shapes[which], terms, coefs + [1.0] * len(more))

        for layer in range(n_layers - 1, -1, -1):
            got = [over_side[which](pair_sum(layer, which, True)) for which in (0, 1)]
            own1, own2 = [pair_sum(layer, which, False, got[which]) for which in (0, 1)]
            near1, near2 = over_y(own1), over_x(own2)
            side1, side2 = over_x(own1), over_y(own2)
            diag1, diag2 = over_x(near1), over_y(near2)
            q1 = lambda a, b: 2 * a + b
            for a, b, v in ((x_pos, y_pos, own1), (x_pos, 1 - y_pos, near1), (1 - x_pos, y_pos, side1), (1 - x_pos, 1 - y_pos, diag1)):
                grad_in = put_piece(False, grad_in, layer, q1(a, b), coef, v, noise_in4)
            for a, b, v in ((y_pos, x_pos, own2), (y_pos, 1 - x_pos, near2), (1 - y_pos, x_pos, side2), (1 - y_pos, 1 - x_pos, diag2)):
                grad_out = put_piece(True, grad_out, layer, q1(a, b), coef, v, noise_out4)
        return grad_in.reshape(n_layers, d_model, d_ff), grad_out.reshape(n_layers, d_ff, d_model)

    return jax.shard_map(
        local_step,
        mesh=mesh,
        in_specs=(P(None, 'dp', None, None), P(None, 'dp', None, 'tp'), P(None, None, 'tp'), P(None, 'tp', None),
                  P('dp', None, None), P(None, None, 'tp'), P(None, 'tp', None), P(), P()),
        out_specs=(P(None, None, 'tp'), P(None, 'tp', None)),
        check_vma=False,
    )
```

```python
import functools

import jax
import jax.numpy as jnp
from jax import lax
from jax.experimental import pallas as pl
from jax.experimental.pallas import tpu as pltpu
from jax.sharding import PartitionSpec as P

INV_SQRT2 = 0.7071067811865476
INV_SQRT_2PI = 0.3989422804014327
LOG2_E = 1.4426950408889634
F_BLOCK = 512
T_CHUNK = 256
IN_SLOTS = 4
ROW_STEPS = 2
VMEM_LIMIT = 66_500_000

F32 = jnp.float32
BF16 = jnp.bfloat16
ANY = pl.ANY
MESH = pl.DeviceIdType.MESH


def dot_nn(a, b):
    return lax.dot_general(a, b, (((1,), (0,)), ((), ())), preferred_element_type=F32)


def dot_nt(a, b):
    return lax.dot_general(a, b, (((1,), (1,)), ((), ())), preferred_element_type=F32)


def stack_kernel(n_layers, n_ex, n_steps, u_ref, w1_ref, w2_ref, x_hbm, dout_hbm,
                 p_hbm, q_hbm, dzo_hbm, g1k_hbm, g1s_hbm, g1r_hbm, g2k_hbm, g2s_hbm, g2r_hbm, g1l_hbm, g2l_hbm, ss_ref,
                 x_t, dz, dz_t, dh, h, acc, x_st, z_st, p_st, q_st, g1_st, g1s_st, g2_st, g2s_st,
                 in_sem, out_sem, io_sem, tp_send, tp_recv, far_send, far_recv):
    task, step = pl.program_id(0), pl.program_id(1)
    n_early = (n_layers - 1) * n_ex
    dp = lax.axis_index('dp')
    x_pos, y_pos = lax.rem(dp, 2), dp // 2
    x_far = {'dp': dp + 1 - 2 * x_pos}
    y_far = {'dp': dp + 2 - 4 * y_pos}
    tp_far = {'tp': 1 - lax.axis_index('tp')}
    n_tok, d_model = dz.shape
    half_d = d_model // 2
    n_half = n_steps // 2
    n_t = n_tok // T_CHUNK
    example = lax.rem(task, n_ex)
    cols = lambda k: pl.ds(pl.multiple_of(k * F_BLOCK, F_BLOCK), F_BLOCK)

    def in_start(t, c):
        slot, rows, ex = c % IN_SLOTS, pl.ds(c * T_CHUNK, T_CHUNK), lax.rem(t, n_ex)
        copy = lambda k, src, dst: pltpu.make_async_copy(src, dst.at[slot], in_sem.at[k, slot]).start()
        copy(0, x_hbm.at[n_layers - 1 - t // n_ex, ex, rows, :], x_st)

        @pl.when(t < n_early)
        def _():
            copy(1, dout_hbm.at[ex, rows, :], z_st)

        @pl.when(t >= n_early)
        def _():
            copy(1, dzo_hbm.at[ex, rows, :], z_st)

        @pl.when(t >= n_ex)
        def _():
            copy(2, p_hbm.at[t - n_ex, rows, :], p_st)
            copy(3, q_hbm.at[t - n_ex, rows, :], q_st)

    def in_wait(c):
        slot, rows = c % IN_SLOTS, pl.ds(c * T_CHUNK, T_CHUNK)
        wait = lambda k, dst: pltpu.make_async_copy(dout_hbm.at[0, rows, :], dst.at[slot], in_sem.at[k, slot]).wait()
        wait(0, x_st)
        wait(1, z_st)

        @pl.when(task >= n_ex)
        def _():
            wait(2, p_st)
            wait(3, q_st)

    def tp_copy(t):
        return pltpu.make_async_remote_copy(
            src_ref=p_hbm.at[t], dst_ref=q_hbm.at[t], send_sem=tp_send.at[t], recv_sem=tp_recv.at[t],
            device_id=tp_far, device_id_type=MESH)

    def front(load, to_dx):
        for s in range(n_t + (1 if to_dx else 0)):
            rows = pl.ds(s * T_CHUNK, T_CHUNK)
            if load and s < n_t:
                if s + IN_SLOTS - 1 < n_t:
                    in_start(task, s + IN_SLOTS - 1)
                in_wait(s)
                slot = s % IN_SLOTS
                z = z_st[slot]
                moved = (z.astype(F32) + (p_st[slot].astype(F32) + q_st[slot].astype(F32))).astype(BF16)
                z = jnp.where(task >= n_ex, moved, z) if to_dx else moved
                dz[rows, :] = z
                dz_t[:, rows] = z.T
                x_t[:, rows] = x_st[slot].T
            if s < n_t:
                u = u_ref[0, 0, rows, :].astype(F32)
                t = u * INV_SQRT2
                cdf = 0.5 * lax.erf(t) + 0.5
                h[rows, :] = (u * cdf).astype(BF16)
                slope = cdf + (t * (INV_SQRT_2PI / INV_SQRT2)) * jnp.exp2((t * t) * -LOG2_E)
                dh[rows, :] = (slope * dot_nt(dz[rows, :], w2_ref[0])).astype(BF16)
            if s >= 1 and to_dx:
                rows = pl.ds((s - 1) * T_CHUNK, T_CHUNK)
                part = dot_nt(dh[rows, :], w1_ref[0])
                acc[rows, :] = part if load else acc[rows, :] + part

    @pl.when((task == 0) & (step == 0))
    def _():
        ss_ref[...] = jnp.zeros_like(ss_ref)
        for c in range(IN_SLOTS - 1):
            in_start(task, c)

    for load in (True, False):
        for to_dx in (True, False):
            @pl.when(((step == 0) if load else (step > 0)) & ((task < n_early) if to_dx else (task >= n_early)))
            def _():
                front(load, to_dx)

    dz_keep = pltpu.make_async_copy(dz, dzo_hbm.at[example], io_sem.at[0])
    is_mid = (task >= n_ex) & (task < n_early)
    pl.when(is_mid & (step == 0))(dz_keep.start)
    ends_early = (step == n_steps - 1) & (task < n_early)
    dx_out = pltpu.make_async_copy(dz, p_hbm.at[task], io_sem.at[1])

    @pl.when(ends_early)
    def _():
        pl.when(is_mid)(dz_keep.wait)

        def put(c, carry):
            rows = pl.ds(pl.multiple_of(c * T_CHUNK, T_CHUNK), T_CHUNK)
            dz[rows, :] = acc[rows, :].astype(BF16)
            return carry

        lax.fori_loop(0, n_t, put, 0)
        dx_out.start()

    def out_copies(t, k, r):
        half_rows = pl.ds(pl.multiple_of(r * half_d, 16), half_d)
        part_rows = pl.ds(pl.multiple_of(r * (half_d // ROW_STEPS), 16), half_d // ROW_STEPS)
        early, k_half, k_col = t < n_early, k // n_half, lax.rem(k, n_half)
        copy = lambda n, src, dst: pltpu.make_async_copy(src, dst, out_sem.at[n, r])
        t_e, t_l = jnp.minimum(t, n_early - 1), jnp.maximum(t - n_early, 0)
        return [
            (early, copy(0, g1_st.at[part_rows, :], g1k_hbm.at[t_e, part_rows, cols(k)])),
            (early, copy(1, g1s_st.at[part_rows, :], g1s_hbm.at[t_e, part_rows, cols(k)])),
            (early & (k_half != y_pos), copy(2, g2s_st.at[half_rows, :], g2s_hbm.at[t_e, half_rows, cols(k_col)])),
            (early & (k_half == y_pos), copy(3, g2_st.at[half_rows, :], g2k_hbm.at[t_e, half_rows, cols(k_col)])),
            (~early, copy(0, g1_st.at[half_rows, :], g1l_hbm.at[t_l, half_rows, cols(k)])),
            (~early, copy(3, g2_st.at[half_rows, :], g2l_hbm.at[t_l, half_rows, cols(k)])),
        ]

    def far_x(src, dst):
        return pltpu.make_async_remote_copy(
            src_ref=src, dst_ref=dst, send_sem=far_send.at[0], recv_sem=far_recv.at[0], device_id=x_far, device_id_type=MESH)

    def far_y(src, dst):
        return pltpu.make_async_remote_copy(
            src_ref=src, dst_ref=dst, send_sem=far_send.at[1], recv_sem=far_recv.at[1], device_id=y_far, device_id_type=MESH)

    @pl.when((task > 0) | (step > 0))
    def _():
        t = jnp.where(step > 0, task, task - 1)
        k = jnp.where(step > 0, step - 1, n_steps - 1)
        for r in range(ROW_STEPS):
            for cond, cp in out_copies(t, k, r):
                pl.when(cond)(cp.wait)

        @pl.when(t < n_early)
        def _():
            far_x(g1s_hbm.at[t, :, cols(k)], g1r_hbm.at[t, :, cols(k)]).start()

        @pl.when((t < n_early) & (k // n_half != y_pos))
        def _():
            k_col = cols(lax.rem(k, n_half))
            far_y(g2s_hbm.at[t, :, k_col], g2r_hbm.at[t, :, k_col]).start()

    def square(g):
        return jnp.sum((g * g).reshape(g.shape[0] // 8, 8, g.shape[1]), axis=0)

    def weight_grads(early, r, carry):
        part = half_d // ROW_STEPS
        total = ss_ref[example]
        if early:
            own = pl.multiple_of(r * part + x_pos * half_d, part)
            far = pl.multiple_of(r * part + (1 - x_pos) * half_d, part)
            rows = pl.ds(pl.multiple_of(r * part, part), part)
            g = dot_nn(x_t[pl.ds(own, part), :], dh[...])
            g1_st[rows, :] = g
            total = total + square(g)
            g = dot_nn(x_t[pl.ds(far, part), :], dh[...])
            g1s_st[rows, :] = g.astype(BF16)
            total = total + square(g)
        for at in range(ROW_STEPS):
            rows = pl.ds(pl.multiple_of(r * half_d + at * part, part), part)
            if not early:
                g = dot_nn(x_t[rows, :], dh[...])
                g1_st[rows, :] = g
                total = total + square(g)
            g = dot_nn(dz_t[rows, :], h[...])
            g2_st[rows, :] = g
            if early:
                g2s_st[rows, :] = g.astype(BF16)
            total = total + square(g)
        ss_ref[example] = total
        for cond, cp in out_copies(task, step, r):
            pl.when(cond)(cp.start)
        return carry

    @pl.when(task < n_early)
    def _():
        lax.fori_loop(0, ROW_STEPS, functools.partial(weight_grads, True), 0, unroll=True)

    @pl.when(task >= n_early)
    def _():
        lax.fori_loop(0, ROW_STEPS, functools.partial(weight_grads, False), 0, unroll=True)

    @pl.when(ends_early)
    def _():
        dx_out.wait()
        tp_copy(task).start()

    @pl.when((step == n_steps - 1) & (task < n_early + n_ex - 1))
    def _():
        nxt = task + 1

        @pl.when(nxt >= n_ex)
        def _():
            tp_copy(nxt - n_ex).wait()

        for c in range(IN_SLOTS - 1):
            in_start(nxt, c)

    @pl.when((step == n_steps - 1) & (task == n_early + n_ex - 1))
    def _():
        for r in range(ROW_STEPS):
            for cond, cp in out_copies(task, step, r):
                pl.when(cond)(cp.wait)
        far_x(g1s_hbm, g1r_hbm).wait()
        far_y(g2s_hbm, g2r_hbm).wait()


def run_stack(pre_act, w_in, w_out, block_in, d_out):
    n_layers, n_ex, n_tok, d_model = block_in.shape
    d_ff = pre_act.shape[3]
    n_steps = d_ff // F_BLOCK
    half_d, half_f = d_model // 2, d_ff // 2
    n_early = (n_layers - 1) * n_ex
    top = n_layers - 1
    in_specs = [
        pl.BlockSpec((1, 1, n_tok, F_BLOCK), lambda t, j: (top - t // n_ex, lax.rem(t, n_ex), 0, j)),
        pl.BlockSpec((1, d_model, F_BLOCK),
                     lambda t, j: (jnp.maximum(top - t // n_ex, 1), 0, jnp.minimum(j + n_steps * (t // n_early), n_steps - 1))),
        pl.BlockSpec((1, F_BLOCK, d_model), lambda t, j: (top - t // n_ex, j, 0)),
        pl.BlockSpec(memory_space=ANY),
        pl.BlockSpec(memory_space=ANY),
    ]
    sds = jax.ShapeDtypeStruct
    outs = [
        sds((n_early, n_tok, d_model), BF16), sds((n_early, n_tok, d_model), BF16), sds((n_ex, n_tok, d_model), BF16),
        sds((n_early, half_d, d_ff), F32), sds((n_early, half_d, d_ff), BF16), sds((n_early, half_d, d_ff), BF16),
        sds((n_early, d_model, half_f), F32), sds((n_early, d_model, half_f), BF16), sds((n_early, d_model, half_f), BF16),
        sds((n_ex, d_model, d_ff), F32), sds((n_ex, d_model, d_ff), F32),
        sds((n_ex, 8, F_BLOCK), F32),
    ]
    out_specs = [pl.BlockSpec(memory_space=ANY)] * (len(outs) - 1) + [pl.BlockSpec((n_ex, 8, F_BLOCK), lambda t, j: (0, 0, 0))]
    vm = pltpu.VMEM
    scratch = [
        vm((d_model, n_tok), BF16), vm((n_tok, d_model), BF16), vm((d_model, n_tok), BF16),
        vm((n_tok, F_BLOCK), BF16), vm((n_tok, F_BLOCK), BF16), vm((n_tok, d_model), F32),
        *[vm((IN_SLOTS, T_CHUNK, d_model), BF16)] * 4,
        vm((d_model, F_BLOCK), F32), vm((half_d, F_BLOCK), BF16), vm((d_model, F_BLOCK), F32), vm((d_model, F_BLOCK), BF16),
        pltpu.SemaphoreType.DMA((4, IN_SLOTS)), pltpu.SemaphoreType.DMA((4, ROW_STEPS)), pltpu.SemaphoreType.DMA((2,)),
        pltpu.SemaphoreType.DMA((n_early,)), pltpu.SemaphoreType.DMA((n_early,)),
        pltpu.SemaphoreType.DMA((2,)), pltpu.SemaphoreType.DMA((2,)),
    ]
    n_dots = 4 * n_early + 3 * n_ex
    return pl.pallas_call(
        functools.partial(stack_kernel, n_layers, n_ex, n_steps),
        out_shape=outs,
        grid_spec=pltpu.PrefetchScalarGridSpec(
            num_scalar_prefetch=0, grid=(n_early + n_ex, n_steps), in_specs=in_specs, out_specs=out_specs, scratch_shapes=scratch),
        compiler_params=pltpu.CompilerParams(
            dimension_semantics=('arbitrary', 'arbitrary'), vmem_limit_bytes=VMEM_LIMIT, has_side_effects=True),
        cost_estimate=pl.CostEstimate(
            flops=2 * n_dots * n_tok * d_model * d_ff, bytes_accessed=500_000_000, transcendentals=2 * n_tok * d_ff),
        name='stack',
    )(pre_act, w_in, w_out, block_in, d_out)


def mix_kernel(sc_ref, coef_ref, *refs):
    total = refs[0][0].astype(F32) * coef_ref[0]
    for k, ref in enumerate(refs[1:-1]):
        total = total + ref[0].astype(F32) * coef_ref[k + 1]
    refs[-1][...] = total.astype(BF16)


def mix(which, shape, terms, coefs):
    rows, width = shape
    block = (rows // 2, width) if which == 0 else (rows // 4, width)

    def spec(k, lead):
        if which == 0:
            return pl.BlockSpec((1, *block), lambda i, sc: (lead, 2 * sc[k] + i, 0))
        return pl.BlockSpec((1, *block), lambda i, sc: (lead, i, sc[k]))

    out_map = lambda i, sc: (i, 0)
    places = jnp.stack([jnp.asarray(p, jnp.int32) for _, _, p in terms])
    return pl.pallas_call(
        mix_kernel,
        out_shape=jax.ShapeDtypeStruct((rows, width), BF16),
        grid_spec=pltpu.PrefetchScalarGridSpec(
            num_scalar_prefetch=1, grid=(rows // block[0],),
            in_specs=[pl.BlockSpec(memory_space=pltpu.SMEM)] + [spec(k, lead) for k, (_, lead, _) in enumerate(terms)],
            out_specs=pl.BlockSpec(block, out_map)),
        compiler_params=pltpu.CompilerParams(dimension_semantics=('arbitrary',), vmem_limit_bytes=40_000_000),
        cost_estimate=pl.CostEstimate(flops=2 * len(terms) * rows * width, bytes_accessed=14 * rows * width, transcendentals=0),
        name='mix',
    )(places, jnp.stack([jnp.asarray(c, F32) for c in coefs]), *[v for v, _, _ in terms])


def put_in_kernel(sc_ref, coef_ref, piece_ref, noise_ref, *rest):
    out_ref = rest[-1]
    out_ref[0, 0] = (piece_ref[...].astype(F32) + coef_ref[0] * noise_ref[0, 0]) * coef_ref[1]


def put_out_kernel(sc_ref, coef_ref, piece_ref, noise_ref, *rest):
    out_ref = rest[-1]
    out_ref[0, 0] = (piece_ref[...].astype(F32).T + coef_ref[0] * noise_ref[0, 0]) * coef_ref[1]


def put_piece(transposed, total, layer, quarter, coef, piece, noise):
    if transposed:
        rows, width = piece.shape[1], piece.shape[0]
        block = 256
        piece_spec = pl.BlockSpec((width, block), lambda i, sc: (0, i))
    else:
        rows, width = piece.shape
        block = rows // 2
        piece_spec = pl.BlockSpec((block, width), lambda i, sc: (i, 0))
    big_spec = pl.BlockSpec((1, 1, block, width), lambda i, sc: (sc[0], sc[1], i, 0))
    args = [jnp.stack([jnp.int32(layer), quarter]), coef, piece, noise]
    in_specs = [pl.BlockSpec(memory_space=pltpu.SMEM), piece_spec, big_spec]
    aliases = {}
    if total is not None:
        args.append(total)
        in_specs.append(pl.BlockSpec(memory_space=ANY))
        aliases = {4: 0}
    return pl.pallas_call(
        put_out_kernel if transposed else put_in_kernel,
        out_shape=jax.ShapeDtypeStruct(noise.shape, F32),
        grid_spec=pltpu.PrefetchScalarGridSpec(
            num_scalar_prefetch=1, grid=(rows // block,), in_specs=in_specs, out_specs=big_spec),
        input_output_aliases=aliases,
        compiler_params=pltpu.CompilerParams(dimension_semantics=('arbitrary',), vmem_limit_bytes=40_000_000),
        cost_estimate=pl.CostEstimate(flops=4 * rows * width, bytes_accessed=10 * rows * width, transcendentals=0),
        name='put_out' if transposed else 'put_in',
    )(*args)


def solution(mesh):
    data_size = mesh.shape['dp']
    swap_x = [(i, i ^ 1) for i in range(data_size)]
    swap_y = [(i, i ^ 2) for i in range(data_size)]

    def local_step(block_in, pre_act, w_in, w_out, d_out, noise_in, noise_out, clip_norm, noise_mult):
        n_layers, local_batch, _, d_model = block_in.shape
        d_ff = pre_act.shape[3]
        batch_total = local_batch * data_size
        dp = lax.axis_index('dp')
        x_pos, y_pos = lax.rem(dp, 2), dp // 2
        over_x = lambda v: lax.ppermute(v, 'dp', swap_x)
        over_y = lambda v: lax.ppermute(v, 'dp', swap_y)
        res = run_stack(pre_act, w_in, w_out, block_in, d_out)
        g1k, _, g1r, g2k, _, g2r, g1l, g2l, squares = res[3:]
        part_sq = jnp.sum(squares, axis=(1, 2))
        clip = jnp.minimum(1.0, clip_norm / jnp.sqrt(lax.psum(part_sq, 'tp')))
        clip_x, clip_y = over_x(clip), over_y(clip)
        c_own, c_x, c_y = [[v[k] for k in range(local_batch)] for v in (clip, clip_x, clip_y)]
        coef = jnp.stack([noise_mult * clip_norm, jnp.float32(1.0 / batch_total)])

        noise_in4 = noise_in.reshape(n_layers, 4, d_model // 4, d_ff)
        noise_out4 = noise_out.reshape(n_layers, 4, d_ff // 4, d_model)

        shapes = ((d_model // 4, d_ff), (d_model, d_ff // 4))
        at_half, at_side = (x_pos, y_pos), (y_pos, x_pos)
        over_half, over_side = (over_x, over_y), (over_y, over_x)
        early, early_far, late = (g1k, g2k), (g1r, g2r), (g1l, g2l)

        def own_terms(layer, which, half_pos, pos):
            if layer == 0:
                return [(late[which], k, 2 * half_pos + pos) for k in range(local_batch)]
            first = (n_layers - 1 - layer) * local_batch
            return [(early[which], first + k, pos) for k in range(local_batch)]

        far_last = {}
        for to_send in (True, False):
            for which in (0, 1):
                pos = 1 - at_side[which] if to_send else at_side[which]
                piece = mix(which, shapes[which], own_terms(0, which, 1 - at_half[which], pos), c_own)
                far_last[which, to_send] = over_half[which](piece)

        def pair_sum(layer, which, to_send, *more):
            pos = 1 - at_side[which] if to_send else at_side[which]
            terms, coefs = own_terms(layer, which, at_half[which], pos), list(c_own)
            if layer == 0:
                more = (far_last[which, to_send], *more)
            else:
                first = (n_layers - 1 - layer) * local_batch
                terms += [(early_far[which], first + k, pos) for k in range(local_batch)]
                coefs += c_y if which else c_x
            terms += [(v[None], 0, 0) for v in more]
            return mix(which, shapes[which], terms, coefs + [1.0] * len(more))

        places = {}
        for layer in range(n_layers - 1, -1, -1):
            got = [over_side[which](pair_sum(layer, which, True)) for which in (0, 1)]
            for which in (0, 1):
                half_pos, pos = at_half[which], at_side[which]
                own = pair_sum(layer, which, False, got[which])
                near, side = over_side[which](own), over_half[which](own)
                diag = over_half[which](near)
                places[layer, which] = (
                    (2 * half_pos + pos, own), (2 * half_pos + 1 - pos, near),
                    (2 * (1 - half_pos) + pos, side), (2 * (1 - half_pos) + 1 - pos, diag))
        grads, noises = [None, None], (noise_in4, noise_out4)
        for kind in range(4):
            for layer in range(n_layers - 1, -1, -1):
                for which in (0, 1):
                    at, piece = places[layer, which][kind]
                    grads[which] = put_piece(which == 1, grads[which], layer, at, coef, piece, noises[which])
        grad_in, grad_out = grads
        return grad_in.reshape(n_layers, d_model, d_ff), grad_out.reshape(n_layers, d_ff, d_model)

    return jax.shard_map(
        local_step,
        mesh=mesh,
        in_specs=(P(None, 'dp', None, None), P(None, 'dp', None, 'tp'), P(None, None, 'tp'), P(None, 'tp', None),
                  P('dp', None, None), P(None, None, 'tp'), P(None, 'tp', None), P(), P()),
        out_specs=(P(None, None, 'tp'), P(None, 'tp', None)),
        check_vma=False,
    )
```

```python
import functools

import jax
import jax.numpy as jnp
from jax import lax
from jax.experimental import pallas as pl
from jax.experimental.pallas import tpu as pltpu
from jax.sharding import PartitionSpec as P


INV_SQRT2 = 0.7071067811865476
INV_SQRT_2PI = 0.3989422804014327
LOG2_E = 1.4426950408889634
F_BLOCK = 512
T_CHUNK = 256
IN_SLOTS = 4
LOAD_CHUNKS = 2
VMEM_LIMIT = 66_500_000

F32 = jnp.float32
BF16 = jnp.bfloat16
ANY = pl.ANY
MESH = pl.DeviceIdType.MESH


def dot_nn(a, b):
    return lax.dot_general(a, b, (((1,), (0,)), ((), ())), preferred_element_type=F32)


def dot_nt(a, b):
    return lax.dot_general(a, b, (((1,), (1,)), ((), ())), preferred_element_type=F32)


def block_at(j, n_half, x_pos, y_pos):
    far = n_half * (1 - y_pos) + x_pos * j + (1 - x_pos) * (n_half - 1 - j)
    own = n_half * y_pos + j - n_half
    is_far = 1 - j // n_half
    return is_far * far + (1 - is_far) * own


def stack_kernel(n_layers, n_ex, n_steps, u_ref, w1_ref, w2_ref, x_hbm, dout_hbm,
                 p_hbm, q_hbm, dzo_hbm, g1k_hbm, g1s_hbm, g1r_hbm, g2k_hbm, g2s_hbm, g2r_hbm,
                 g1l_hbm, g2l_hbm, g1e_hbm, g1er_hbm, g2e_hbm, g2er_hbm, ss_ref,
                 x_t, dz, dz_t, dh, h, acc, x_st, z_st, p_st, q_st, g1_st, g1s_st, g2_st, g2s_st,
                 in_sem, out_sem, io_sem, tp_send, tp_recv, far_send, far_recv):
    task, step = pl.program_id(0), pl.program_id(1)
    n_early = (n_layers - 1) * n_ex
    n_task = n_early + n_ex
    dp = lax.axis_index('dp')
    x_pos, y_pos = lax.rem(dp, 2), dp // 2
    x_far = {'dp': dp + 1 - 2 * x_pos}
    y_far = {'dp': dp + 2 - 4 * y_pos}
    tp_far = {'tp': 1 - lax.axis_index('tp')}
    n_tok, d_model = dz.shape
    half_d, quarter_d = d_model // 2, d_model // 4
    n_half = n_steps // 2
    half_b = F_BLOCK // 2
    n_t = n_tok // T_CHUNK
    example = lax.rem(task, n_ex)
    cols = lambda k: pl.ds(pl.multiple_of(k * F_BLOCK, F_BLOCK), F_BLOCK)
    chunk = lambda c: pl.ds(c * T_CHUNK if isinstance(c, int) else pl.multiple_of(c * T_CHUNK, T_CHUNK), T_CHUNK)

    def in_start(t, c):
        slot, rows, ex = lax.rem(c, IN_SLOTS), chunk(c), lax.rem(t, n_ex)
        copy = lambda k, src, dst: pltpu.make_async_copy(src, dst.at[slot], in_sem.at[k, slot]).start()
        copy(0, x_hbm.at[n_layers - 1 - t // n_ex, ex, rows, :], x_st)

        @pl.when(t < n_early)
        def _():
            copy(1, dout_hbm.at[ex, rows, :], z_st)

        @pl.when(t >= n_early)
        def _():
            copy(1, dzo_hbm.at[ex, rows, :], z_st)

        @pl.when(t >= n_ex)
        def _():
            copy(2, p_hbm.at[t - n_ex, rows, :], p_st)
            copy(3, q_hbm.at[t - n_ex, rows, :], q_st)

    def in_wait(c):
        slot, rows = lax.rem(c, IN_SLOTS), chunk(c)
        wait = lambda k, dst: pltpu.make_async_copy(dout_hbm.at[0, rows, :], dst.at[slot], in_sem.at[k, slot]).wait()
        wait(0, x_st)
        wait(1, z_st)

        @pl.when(task >= n_ex)
        def _():
            wait(2, p_st)
            wait(3, q_st)

    def tp_copy(t):
        return pltpu.make_async_remote_copy(
            src_ref=p_hbm.at[t], dst_ref=q_hbm.at[t], send_sem=tp_send.at[t], recv_sem=tp_recv.at[t],
            device_id=tp_far, device_id_type=MESH)

    def front(load, to_dx):
        n_in = LOAD_CHUNKS if load else (n_t if to_dx else n_t // 2)

        def trip(i, carry):
            def dx_part(rows):
                part = dot_nt(dh[rows, :], w1_ref[0])
                acc[rows, :] = part if load else acc[rows, :] + part

            for s in range(n_in):
                c = i * n_in + s
                rows = chunk(c)
                if load:
                    @pl.when(c + IN_SLOTS - 1 < n_t)
                    def _():
                        in_start(task, c + IN_SLOTS - 1)

                    in_wait(c)
                    slot = lax.rem(c, IN_SLOTS)
                    z = z_st[slot]
                    moved = (z.astype(F32) + (p_st[slot].astype(F32) + q_st[slot].astype(F32))).astype(BF16)
                    z = jnp.where(task >= n_ex, moved, z) if to_dx else moved
                    dz[rows, :] = z
                    dz_t[:, rows] = z.T
                    x_t[:, rows] = x_st[slot].T
                u = u_ref[0, 0, rows, :].astype(F32)
                t = u * INV_SQRT2
                cdf = 0.5 * lax.erf(t) + 0.5
                h[rows, :] = (u * cdf).astype(BF16)
                slope = cdf + (t * (INV_SQRT_2PI / INV_SQRT2)) * jnp.exp2((t * t) * -LOG2_E)
                dh[rows, :] = (slope * dot_nt(dz[rows, :], w2_ref[0])).astype(BF16)
                if to_dx and s:
                    dx_part(chunk(c - 1))
            if to_dx:
                dx_part(chunk(i * n_in + n_in - 1))
            return carry

        if n_in == n_t:
            trip(0, 0)
        else:
            lax.fori_loop(0, n_t // n_in, trip, 0)

    @pl.when((task == 0) & (step == 0))
    def _():
        ss_ref[...] = jnp.zeros_like(ss_ref)
        for c in range(IN_SLOTS - 1):
            in_start(task, c)

    for load in (True, False):
        for to_dx in (True, False):
            @pl.when(((step == 0) if load else (step > 0)) & ((task < n_early) if to_dx else (task >= n_early)))
            def _():
                front(load, to_dx)

    dz_keep = pltpu.make_async_copy(dz, dzo_hbm.at[example], io_sem.at[0])
    is_mid = (task >= n_ex) & (task < n_early)
    pl.when(is_mid & (step == 0))(dz_keep.start)
    ends_early = (step == n_steps - 1) & (task < n_early)
    dx_out = pltpu.make_async_copy(dz, p_hbm.at[task], io_sem.at[1])

    @pl.when(ends_early)
    def _():
        pl.when(is_mid)(dz_keep.wait)

        def put(c, carry):
            dz[chunk(c), :] = acc[chunk(c), :].astype(BF16)
            return carry

        lax.fori_loop(0, n_t, put, 0)
        dx_out.start()

    def out_copies(t, j):
        early, is_far, fb = t < n_early, j < n_half, block_at(j, n_half, x_pos, y_pos)
        copy = lambda n, src, dst: pltpu.make_async_copy(src, dst, out_sem.at[n])
        t_e, t_l = jnp.minimum(t, n_early - 1), jnp.maximum(t - n_early, 0)
        own_rows = pl.ds(pl.multiple_of(x_pos * half_d, 16), half_d)
        pass_rows = pl.ds(pl.multiple_of((1 - y_pos) * quarter_d, 16), quarter_d)
        in_half = cols(lax.rem(fb, n_half))
        src_half = pl.ds(pl.multiple_of((1 - x_pos) * half_b, half_b), half_b)
        dst_half = pl.ds(pl.multiple_of(x_pos * F_BLOCK, half_b), half_b)
        dst_full = pl.ds(pl.multiple_of((1 - x_pos) * half_b, half_b), F_BLOCK)
        return [
            (early, copy(0, g1_st.at[own_rows, :], g1k_hbm.at[t_e, :, cols(fb)])),
            (early, copy(1, g1s_st, g1s_hbm.at[t_e, :, cols(fb)])),
            (early & is_far, copy(2, g2s_st, g2s_hbm.at[t_e, :, in_half])),
            (early & ~is_far, copy(3, g2_st, g2k_hbm.at[t_e, :, in_half])),
            (~early, copy(0, g1_st, g1l_hbm.at[t_l, :, cols(fb)])),
            (~early, copy(1, g1s_st.at[pass_rows, :], g1e_hbm.at[t_l, :, cols(fb)])),
            (~early & (j == 0), copy(2, g2s_st, g2e_hbm.at[t_l, :, dst_full])),
            (~early & (j == 1), copy(2, g2s_st.at[:, src_half], g2e_hbm.at[t_l, :, dst_half])),
            (~early, copy(3, g2_st, g2l_hbm.at[t_l, :, cols(fb)])),
        ]

    def far_copy(axis, src, dst):
        return pltpu.make_async_remote_copy(
            src_ref=src, dst_ref=dst, send_sem=far_send.at[axis], recv_sem=far_recv.at[axis],
            device_id=y_far if axis % 2 else x_far, device_id_type=MESH)

    def send_far(t, j):
        early, is_far, fb = t < n_early, j < n_half, block_at(j, n_half, x_pos, y_pos)
        t_l = jnp.maximum(t - n_early, 0)
        in_half = cols(lax.rem(fb, n_half))
        half = pl.ds(pl.multiple_of(x_pos * F_BLOCK, half_b), half_b)
        full = pl.ds(pl.multiple_of((1 - x_pos) * half_b, half_b), F_BLOCK)

        @pl.when(early)
        def _():
            far_copy(0, g1s_hbm.at[t, :, cols(fb)], g1r_hbm.at[t, :, cols(fb)]).start()

        @pl.when(early & is_far)
        def _():
            far_copy(1, g2s_hbm.at[t, :, in_half], g2r_hbm.at[t, :, in_half]).start()

        @pl.when(~early)
        def _():
            far_copy(2, g1e_hbm.at[t_l, :, cols(fb)], g1er_hbm.at[t_l, :, cols(fb)]).start()

        @pl.when(~early & (j == 0))
        def _():
            far_copy(3, g2e_hbm.at[t_l, :, full], g2er_hbm.at[t_l, :, full]).start()

        @pl.when(~early & (j == 1))
        def _():
            far_copy(3, g2e_hbm.at[t_l, :, half], g2er_hbm.at[t_l, :, half]).start()

    def finish_block(t, j):
        for cond, cp in out_copies(t, j):
            pl.when(cond)(cp.wait)
        send_far(t, j)

    @pl.when((task > 0) | (step > 0))
    def _():
        finish_block(jnp.where(step > 0, task, task - 1), jnp.where(step > 0, step - 1, n_steps - 1))

    def square(g):
        return jnp.sum((g * g).reshape(g.shape[0] // 8, 8, g.shape[1]), axis=0)

    total = ss_ref[example]
    for r in range(2):
        part = pl.ds(r * quarter_d, quarter_d)
        own = pl.ds(pl.multiple_of(r * quarter_d + x_pos * half_d, 16), quarter_d)
        far = pl.ds(pl.multiple_of(r * quarter_d + (1 - x_pos) * half_d, 16), quarter_d)
        g = dot_nn(x_t[own, :], dh[...])
        g1_st[own, :] = g
        total = total + square(g)
        g = dot_nn(x_t[far, :], dh[...])
        g1_st[far, :] = g
        g1s_st[part, :] = g.astype(BF16)
        total = total + square(g)
        for at in (part, pl.ds(r * quarter_d + half_d, quarter_d)):
            g = dot_nn(dz_t[at, :], h[...])
            g2_st[at, :] = g
            g2s_st[at, :] = g.astype(BF16)
            total = total + square(g)
    ss_ref[example] = total
    for cond, cp in out_copies(task, step):
        pl.when(cond)(cp.start)

    @pl.when(ends_early)
    def _():
        dx_out.wait()
        tp_copy(task).start()

    @pl.when((step == n_steps - 1) & (task < n_task - 1))
    def _():
        nxt = task + 1

        @pl.when(nxt >= n_ex)
        def _():
            tp_copy(nxt - n_ex).wait()

        for c in range(IN_SLOTS - 1):
            in_start(nxt, c)

    @pl.when((step == n_steps - 1) & (task == n_task - 1))
    def _():
        finish_block(task, step)
        far_copy(0, g1s_hbm, g1r_hbm).wait()
        far_copy(1, g2s_hbm, g2r_hbm).wait()
        far_copy(2, g1e_hbm, g1er_hbm).wait()
        far_copy(3, g2e_hbm, g2er_hbm).wait()


def run_stack(pre_act, w_in, w_out, block_in, d_out):
    n_layers, n_ex, n_tok, d_model = block_in.shape
    d_ff = pre_act.shape[3]
    n_steps = d_ff // F_BLOCK
    half_d, half_f = d_model // 2, d_ff // 2
    n_early = (n_layers - 1) * n_ex
    top = n_layers - 1

    def fb(j):
        dp = lax.axis_index('dp')
        return block_at(j, n_steps // 2, lax.rem(dp, 2), dp // 2)

    def w1_at(t, j):
        is_last = t // n_early
        return jnp.maximum(top - t // n_ex, 1), 0, fb((1 - is_last) * j + is_last * (n_steps - 1))

    in_specs = [
        pl.BlockSpec((1, 1, n_tok, F_BLOCK), lambda t, j: (top - t // n_ex, lax.rem(t, n_ex), 0, fb(j))),
        pl.BlockSpec((1, d_model, F_BLOCK), w1_at),
        pl.BlockSpec((1, F_BLOCK, d_model), lambda t, j: (top - t // n_ex, fb(j), 0)),
        pl.BlockSpec(memory_space=ANY),
        pl.BlockSpec(memory_space=ANY),
    ]
    sds = jax.ShapeDtypeStruct
    outs = [
        sds((n_early, n_tok, d_model), BF16), sds((n_early, n_tok, d_model), BF16), sds((n_ex, n_tok, d_model), BF16),
        sds((n_early, half_d, d_ff), F32), sds((n_early, half_d, d_ff), BF16), sds((n_early, half_d, d_ff), BF16),
        sds((n_early, d_model, half_f), F32), sds((n_early, d_model, half_f), BF16), sds((n_early, d_model, half_f), BF16),
        sds((n_ex, d_model, d_ff), F32), sds((n_ex, d_model, d_ff), F32),
        sds((n_ex, d_model // 4, d_ff), BF16), sds((n_ex, d_model // 4, d_ff), BF16),
        sds((n_ex, d_model, d_ff // 4), BF16), sds((n_ex, d_model, d_ff // 4), BF16),
        sds((n_ex, 8, F_BLOCK), F32),
    ]
    out_specs = [pl.BlockSpec(memory_space=ANY)] * (len(outs) - 1) + [pl.BlockSpec((n_ex, 8, F_BLOCK), lambda t, j: (0, 0, 0))]
    vm = pltpu.VMEM
    scratch = [
        vm((d_model, n_tok), BF16), vm((n_tok, d_model), BF16), vm((d_model, n_tok), BF16),
        vm((n_tok, F_BLOCK), BF16), vm((n_tok, F_BLOCK), BF16), vm((n_tok, d_model), F32),
        *[vm((IN_SLOTS, T_CHUNK, d_model), BF16)] * 4,
        vm((d_model, F_BLOCK), F32), vm((half_d, F_BLOCK), BF16), vm((d_model, F_BLOCK), F32), vm((d_model, F_BLOCK), BF16),
        pltpu.SemaphoreType.DMA((4, IN_SLOTS)), pltpu.SemaphoreType.DMA((4,)), pltpu.SemaphoreType.DMA((2,)),
        pltpu.SemaphoreType.DMA((n_early,)), pltpu.SemaphoreType.DMA((n_early,)),
        pltpu.SemaphoreType.DMA((4,)), pltpu.SemaphoreType.DMA((4,)),
    ]
    n_dots = 4 * n_early + 3 * n_ex
    return pl.pallas_call(
        functools.partial(stack_kernel, n_layers, n_ex, n_steps),
        out_shape=outs,
        grid_spec=pltpu.PrefetchScalarGridSpec(
            num_scalar_prefetch=0, grid=(n_early + n_ex, n_steps), in_specs=in_specs, out_specs=out_specs, scratch_shapes=scratch),
        compiler_params=pltpu.CompilerParams(
            dimension_semantics=('arbitrary', 'arbitrary'), vmem_limit_bytes=VMEM_LIMIT, has_side_effects=True),
        cost_estimate=pl.CostEstimate(
            flops=2 * n_dots * n_tok * d_model * d_ff, bytes_accessed=500_000_000, transcendentals=2 * n_tok * d_ff),
        name='stack',
    )(pre_act, w_in, w_out, block_in, d_out)


def mix_kernel(sc_ref, coef_ref, *refs):
    total = refs[0][0].astype(F32) * coef_ref[0]
    for k, ref in enumerate(refs[1:-1]):
        total = total + ref[0].astype(F32) * coef_ref[k + 1]
    refs[-1][...] = total.astype(BF16)


def mix(which, shape, terms, coefs):
    rows, width = shape
    block = (32, width) if which == 0 else (rows // 8, width)

    def spec(k, lead):
        if which == 0:
            return pl.BlockSpec((1, *block), lambda i, sc: (lead, (rows // block[0]) * sc[k] + i, 0))
        return pl.BlockSpec((1, *block), lambda i, sc: (lead, i, sc[k]))

    out_map = lambda i, sc: (i, 0)
    places = jnp.stack([jnp.asarray(p, jnp.int32) for _, _, p in terms])
    return pl.pallas_call(
        mix_kernel,
        out_shape=jax.ShapeDtypeStruct((rows, width), BF16),
        grid_spec=pltpu.PrefetchScalarGridSpec(
            num_scalar_prefetch=1, grid=(rows // block[0],),
            in_specs=[pl.BlockSpec(memory_space=pltpu.SMEM)] + [spec(k, lead) for k, (_, lead, _) in enumerate(terms)],
            out_specs=pl.BlockSpec(block, out_map)),
        compiler_params=pltpu.CompilerParams(dimension_semantics=('arbitrary',), vmem_limit_bytes=40_000_000),
        cost_estimate=pl.CostEstimate(flops=2 * len(terms) * rows * width, bytes_accessed=14 * rows * width, transcendentals=0),
        name='mix',
    )(places, coefs, *[v for v, _, _ in terms])


def put_in_kernel(sc_ref, coef_ref, piece_ref, noise_ref, *rest):
    out_ref = rest[-1]
    out_ref[0, 0] = (piece_ref[...].astype(F32) + coef_ref[0] * noise_ref[0, 0]) * coef_ref[1]


def put_out_kernel(sc_ref, coef_ref, piece_ref, noise_ref, *rest):
    out_ref = rest[-1]
    out_ref[0, 0] = (piece_ref[...].astype(F32).T + coef_ref[0] * noise_ref[0, 0]) * coef_ref[1]


def put_piece(transposed, total, layer, quarter, coef, piece, noise):
    if transposed:
        rows, width = piece.shape[1], piece.shape[0]
        block = 256
        piece_spec = pl.BlockSpec((width, block), lambda i, sc: (0, i))
    else:
        rows, width = piece.shape
        block = rows // 2
        piece_spec = pl.BlockSpec((block, width), lambda i, sc: (i, 0))
    big_spec = pl.BlockSpec((1, 1, block, width), lambda i, sc: (sc[0], sc[1], i, 0))
    args = [jnp.stack([jnp.int32(layer), quarter]), coef, piece, noise]
    in_specs = [pl.BlockSpec(memory_space=pltpu.SMEM), piece_spec, big_spec]
    aliases = {}
    if total is not None:
        args.append(total)
        in_specs.append(pl.BlockSpec(memory_space=ANY))
        aliases = {4: 0}
    return pl.pallas_call(
        put_out_kernel if transposed else put_in_kernel,
        out_shape=jax.ShapeDtypeStruct(noise.shape, F32),
        grid_spec=pltpu.PrefetchScalarGridSpec(
            num_scalar_prefetch=1, grid=(rows // block,), in_specs=in_specs, out_specs=big_spec),
        input_output_aliases=aliases,
        compiler_params=pltpu.CompilerParams(dimension_semantics=('arbitrary',), vmem_limit_bytes=40_000_000),
        cost_estimate=pl.CostEstimate(flops=4 * rows * width, bytes_accessed=10 * rows * width, transcendentals=0),
        name='put_out' if transposed else 'put_in',
    )(*args)


def solution(mesh):
    data_size = mesh.shape['dp']
    swap_x = [(i, i ^ 1) for i in range(data_size)]
    swap_y = [(i, i ^ 2) for i in range(data_size)]

    def local_step(block_in, pre_act, w_in, w_out, d_out, noise_in, noise_out, clip_norm, noise_mult):
        n_layers, local_batch, _, d_model = block_in.shape
        d_ff = pre_act.shape[3]
        batch_total = local_batch * data_size
        dp = lax.axis_index('dp')
        x_pos, y_pos = lax.rem(dp, 2), dp // 2
        over_x = lambda v: lax.ppermute(v, 'dp', swap_x)
        over_y = lambda v: lax.ppermute(v, 'dp', swap_y)
        res = run_stack(pre_act, w_in, w_out, block_in, d_out)
        g1k, _, g1r, g2k, _, g2r, g1l, g2l, _, g1er, _, g2er, squares = res[3:]
        part_sq = jnp.sum(squares, axis=(1, 2))
        clip = jnp.minimum(1.0, clip_norm / jnp.sqrt(lax.psum(part_sq, 'tp')))
        clip, clip_x, clip_y = lax.optimization_barrier((clip, over_x(clip), over_y(clip)))
        c_own, c_x, c_y = [[v[k] for k in range(local_batch)] for v in (clip, clip_x, clip_y)]
        coef = jnp.stack([noise_mult * clip_norm, jnp.float32(1.0 / batch_total)])

        noise_in4 = noise_in.reshape(n_layers, 4, d_model // 4, d_ff)
        noise_out4 = noise_out.reshape(n_layers, 4, d_ff // 4, d_model)

        shapes = ((d_model // 4, d_ff), (d_model, d_ff // 4))
        at_half, at_side = (x_pos, y_pos), (y_pos, x_pos)
        over_half, over_side = (over_x, over_y), (over_y, over_x)
        early, early_far, late = (g1k, g2k), (g1r, g2r), (g1l, g2l)

        def own_terms(layer, which, half_pos, pos):
            if layer == 0:
                return [(late[which], k, 2 * half_pos + pos) for k in range(local_batch)]
            first = (n_layers - 1 - layer) * local_batch
            return [(early[which], first + k, pos) for k in range(local_batch)]

        def mixed(which, terms, coefs):
            return mix(which, shapes[which], terms, jnp.stack([jnp.asarray(c, F32) for c in coefs]))

        made = []

        def send(which, terms, coefs, over):
            coefs = jnp.stack([jnp.asarray(c, F32) for c in coefs])
            if made:
                coefs, _ = lax.optimization_barrier((coefs, made[-1]))
            made.append(mix(which, shapes[which], terms, coefs))
            return over(made[-1])

        def pair_terms(layer, which, to_send, *more):
            pos = 1 - at_side[which] if to_send else at_side[which]
            terms, coefs = own_terms(layer, which, at_half[which], pos), list(c_own)
            if layer == 0 and not to_send:
                more = (far_last[which], *more)
            else:
                if layer == 0:
                    terms += [((g1er, g2er)[which], k, 0) for k in range(local_batch)]
                else:
                    first = (n_layers - 1 - layer) * local_batch
                    terms += [(early_far[which], first + k, pos) for k in range(local_batch)]
                coefs += c_y if which else c_x
            terms += [(v[None], 0, 0) for v in more]
            return terms, coefs + [1.0] * len(more)

        got = {}
        for layer in range(n_layers - 1, 0, -1):
            for which in (0, 1):
                got[layer, which] = send(which, *pair_terms(layer, which, True), over_side[which])
        far_last = [
            send(which, own_terms(0, which, 1 - at_half[which], at_side[which]), c_own, over_half[which]) for which in (0, 1)]
        for which in (0, 1):
            got[0, which] = send(which, *pair_terms(0, which, True), over_side[which])

        places = {}
        for layer in range(n_layers - 1, -1, -1):
            for which in (0, 1):
                half_pos, pos = at_half[which], at_side[which]
                own = mixed(which, *pair_terms(layer, which, False, got[layer, which]))
                near, side = over_side[which](own), over_half[which](own)
                diag = over_half[which](near)
                places[layer, which] = (
                    (2 * half_pos + pos, own), (2 * half_pos + 1 - pos, near),
                    (2 * (1 - half_pos) + pos, side), (2 * (1 - half_pos) + 1 - pos, diag))
        grads, noises = [None, None], (noise_in4, noise_out4)
        for kind in range(4):
            for layer in range(n_layers - 1, -1, -1):
                for which in (0, 1):
                    at, piece = places[layer, which][kind]
                    grads[which] = put_piece(which == 1, grads[which], layer, at, coef, piece, noises[which])
        grad_in, grad_out = grads
        return grad_in.reshape(n_layers, d_model, d_ff), grad_out.reshape(n_layers, d_ff, d_model)

    return jax.shard_map(
        local_step,
        mesh=mesh,
        in_specs=(P(None, 'dp', None, None), P(None, 'dp', None, 'tp'), P(None, None, 'tp'), P(None, 'tp', None),
                  P('dp', None, None), P(None, None, 'tp'), P(None, 'tp', None), P(), P()),
        out_specs=(P(None, None, 'tp'), P(None, 'tp', None)),
        check_vma=False,
    )
```

```python
import functools

import jax
import jax.numpy as jnp
from jax import lax
from jax.experimental import pallas as pl
from jax.experimental.pallas import tpu as pltpu
from jax.sharding import PartitionSpec as P


INV_SQRT2 = 0.7071067811865476
INV_SQRT_2PI = 0.3989422804014327
LOG2_E = 1.4426950408889634
F_BLOCK = 512
T_CHUNK = 256
IN_SLOTS = 4
LOAD_CHUNKS = 2
MIX_ROWS = 32
VMEM_LIMIT = 66_500_000

F32 = jnp.float32
BF16 = jnp.bfloat16
ANY = pl.ANY
MESH = pl.DeviceIdType.MESH


def dot_nn(a, b):
    return lax.dot_general(a, b, (((1,), (0,)), ((), ())), preferred_element_type=F32)


def dot_nt(a, b):
    return lax.dot_general(a, b, (((1,), (1,)), ((), ())), preferred_element_type=F32)


def block_at(j, n_half, x_pos, y_pos):
    far = n_half * (1 - y_pos) + x_pos * j + (1 - x_pos) * (n_half - 1 - j)
    own = n_half * y_pos + j - n_half
    is_far = 1 - j // n_half
    return is_far * far + (1 - is_far) * own


def stack_kernel(n_layers, n_ex, n_steps, u_ref, w1_ref, w2_ref, x_hbm, dout_hbm,
                 p_hbm, q_hbm, dzo_hbm, g1k_hbm, g1s_hbm, g1r_hbm, g2k_hbm, g2s_hbm, g2r_hbm,
                 g1l_hbm, g2l_hbm, g1e_hbm, g1er_hbm, g2e_hbm, g2er_hbm, ss_ref,
                 x_t, dz, dz_t, dh, h, acc, x_st, z_st, p_st, q_st, g1_st, g1s_st, g2_st, g2s_st,
                 in_sem, out_sem, io_sem, tp_send, tp_recv, far_send, far_recv):
    task, step = pl.program_id(0), pl.program_id(1)
    n_early = (n_layers - 1) * n_ex
    n_task = n_early + n_ex
    dp = lax.axis_index('dp')
    x_pos, y_pos = lax.rem(dp, 2), dp // 2
    x_far = {'dp': dp + 1 - 2 * x_pos}
    y_far = {'dp': dp + 2 - 4 * y_pos}
    tp_far = {'tp': 1 - lax.axis_index('tp')}
    n_tok, d_model = dz.shape
    half_d, quarter_d = d_model // 2, d_model // 4
    n_half = n_steps // 2
    half_b = F_BLOCK // 2
    n_t = n_tok // T_CHUNK
    example = lax.rem(task, n_ex)
    cols = lambda k: pl.ds(pl.multiple_of(k * F_BLOCK, F_BLOCK), F_BLOCK)
    chunk = lambda c: pl.ds(c * T_CHUNK if isinstance(c, int) else pl.multiple_of(c * T_CHUNK, T_CHUNK), T_CHUNK)

    def in_start(t, c):
        slot, rows, ex = lax.rem(c, IN_SLOTS), chunk(c), lax.rem(t, n_ex)
        copy = lambda k, src, dst: pltpu.make_async_copy(src, dst.at[slot], in_sem.at[k, slot]).start()
        copy(0, x_hbm.at[n_layers - 1 - t // n_ex, ex, rows, :], x_st)

        @pl.when(t < n_early)
        def _():
            copy(1, dout_hbm.at[ex, rows, :], z_st)

        @pl.when(t >= n_early)
        def _():
            copy(1, dzo_hbm.at[ex, rows, :], z_st)

        @pl.when(t >= n_ex)
        def _():
            copy(2, p_hbm.at[t - n_ex, rows, :], p_st)
            copy(3, q_hbm.at[t - n_ex, rows, :], q_st)

    def in_wait(c):
        slot, rows = lax.rem(c, IN_SLOTS), chunk(c)
        wait = lambda k, dst: pltpu.make_async_copy(dout_hbm.at[0, rows, :], dst.at[slot], in_sem.at[k, slot]).wait()
        wait(0, x_st)
        wait(1, z_st)

        @pl.when(task >= n_ex)
        def _():
            wait(2, p_st)
            wait(3, q_st)

    def tp_copy(t):
        return pltpu.make_async_remote_copy(
            src_ref=p_hbm.at[t], dst_ref=q_hbm.at[t], send_sem=tp_send.at[t], recv_sem=tp_recv.at[t],
            device_id=tp_far, device_id_type=MESH)

    def front(load, to_dx):
        n_in = (2 if to_dx else 1) * LOAD_CHUNKS if load else n_t

        def trip(i, carry):
            def dx_part(rows):
                part = dot_nt(dh[rows, :], w1_ref[0])
                acc[rows, :] = part if load else acc[rows, :] + part

            for s in range(n_in):
                c = i * n_in + s
                rows = chunk(c)
                if load:
                    @pl.when(c + IN_SLOTS - 1 < n_t)
                    def _():
                        in_start(task, c + IN_SLOTS - 1)

                    in_wait(c)
                    slot = lax.rem(c, IN_SLOTS)
                    z = z_st[slot]
                    moved = (z.astype(F32) + (p_st[slot].astype(F32) + q_st[slot].astype(F32))).astype(BF16)
                    z = jnp.where(task >= n_ex, moved, z) if to_dx else moved
                    dz[rows, :] = z
                    dz_t[:, rows] = z.T
                    x_t[:, rows] = x_st[slot].T
                u = u_ref[0, 0, rows, :].astype(F32)
                t = u * INV_SQRT2
                cdf = 0.5 * lax.erf(t) + 0.5
                h[rows, :] = (u * cdf).astype(BF16)
                slope = cdf + (t * (INV_SQRT_2PI / INV_SQRT2)) * jnp.exp2((t * t) * -LOG2_E)
                dh[rows, :] = (slope * dot_nt(dz[rows, :], w2_ref[0])).astype(BF16)
                if to_dx and s:
                    dx_part(chunk(c - 1))
            if to_dx:
                dx_part(chunk(i * n_in + n_in - 1))
            return carry

        if n_in == n_t:
            trip(0, 0)
        else:
            lax.fori_loop(0, n_t // n_in, trip, 0)

    @pl.when((task == 0) & (step == 0))
    def _():
        ss_ref[...] = jnp.zeros_like(ss_ref)
        for c in range(IN_SLOTS - 1):
            in_start(task, c)

    for load in (True, False):
        for to_dx in (True, False):
            @pl.when(((step == 0) if load else (step > 0)) & ((task < n_early) if to_dx else (task >= n_early)))
            def _():
                front(load, to_dx)

    dz_keep = pltpu.make_async_copy(dz, dzo_hbm.at[example], io_sem.at[0])
    is_mid = (task >= n_ex) & (task < n_early)
    pl.when(is_mid & (step == 0))(dz_keep.start)
    ends_early = (step == n_steps - 1) & (task < n_early)
    dx_out = pltpu.make_async_copy(dz, p_hbm.at[task], io_sem.at[1])

    @pl.when(ends_early)
    def _():
        pl.when(is_mid)(dz_keep.wait)

        def put(c, carry):
            dz[chunk(c), :] = acc[chunk(c), :].astype(BF16)
            return carry

        lax.fori_loop(0, n_t, put, 0)
        dx_out.start()

    def out_copies(t, j):
        early, is_far, fb = t < n_early, j < n_half, block_at(j, n_half, x_pos, y_pos)
        copy = lambda n, src, dst: pltpu.make_async_copy(src, dst, out_sem.at[n])
        t_e, t_l = jnp.minimum(t, n_early - 1), jnp.maximum(t - n_early, 0)
        own_rows = pl.ds(pl.multiple_of(x_pos * half_d, 16), half_d)
        pass_rows = pl.ds(pl.multiple_of((1 - y_pos) * quarter_d, 16), quarter_d)
        in_half = cols(lax.rem(fb, n_half))
        src_half = pl.ds(pl.multiple_of((1 - x_pos) * half_b, half_b), half_b)
        dst_half = pl.ds(pl.multiple_of(x_pos * F_BLOCK, half_b), half_b)
        dst_full = pl.ds(pl.multiple_of((1 - x_pos) * half_b, half_b), F_BLOCK)
        return [
            (early, copy(0, g1_st.at[own_rows, :], g1k_hbm.at[t_e, :, cols(fb)])),
            (early, copy(1, g1s_st, g1s_hbm.at[t_e, :, cols(fb)])),
            (early & is_far, copy(2, g2s_st, g2s_hbm.at[t_e, :, in_half])),
            (early & ~is_far, copy(3, g2_st, g2k_hbm.at[t_e, :, in_half])),
            (~early, copy(0, g1_st, g1l_hbm.at[t_l, :, cols(fb)])),
            (~early, copy(1, g1s_st.at[pass_rows, :], g1e_hbm.at[t_l, :, cols(fb)])),
            (~early & (j == 0), copy(2, g2s_st, g2e_hbm.at[t_l, :, dst_full])),
            (~early & (j == 1), copy(2, g2s_st.at[:, src_half], g2e_hbm.at[t_l, :, dst_half])),
            (~early, copy(3, g2_st, g2l_hbm.at[t_l, :, cols(fb)])),
        ]

    def far_copy(axis, src, dst):
        return pltpu.make_async_remote_copy(
            src_ref=src, dst_ref=dst, send_sem=far_send.at[axis], recv_sem=far_recv.at[axis],
            device_id=y_far if axis % 2 else x_far, device_id_type=MESH)

    def send_far(t, j):
        early, is_far, fb = t < n_early, j < n_half, block_at(j, n_half, x_pos, y_pos)
        t_l = jnp.maximum(t - n_early, 0)
        in_half = cols(lax.rem(fb, n_half))
        half = pl.ds(pl.multiple_of(x_pos * F_BLOCK, half_b), half_b)
        full = pl.ds(pl.multiple_of((1 - x_pos) * half_b, half_b), F_BLOCK)

        @pl.when(early)
        def _():
            far_copy(0, g1s_hbm.at[t, :, cols(fb)], g1r_hbm.at[t, :, cols(fb)]).start()

        @pl.when(early & is_far)
        def _():
            far_copy(1, g2s_hbm.at[t, :, in_half], g2r_hbm.at[t, :, in_half]).start()

        @pl.when(~early)
        def _():
            far_copy(2, g1e_hbm.at[t_l, :, cols(fb)], g1er_hbm.at[t_l, :, cols(fb)]).start()

        @pl.when(~early & (j == 0))
        def _():
            far_copy(3, g2e_hbm.at[t_l, :, full], g2er_hbm.at[t_l, :, full]).start()

        @pl.when(~early & (j == 1))
        def _():
            far_copy(3, g2e_hbm.at[t_l, :, half], g2er_hbm.at[t_l, :, half]).start()

    def finish_block(t, j):
        for cond, cp in out_copies(t, j):
            pl.when(cond)(cp.wait)
        send_far(t, j)

    @pl.when((task > 0) | (step > 0))
    def _():
        finish_block(jnp.where(step > 0, task, task - 1), jnp.where(step > 0, step - 1, n_steps - 1))

    def square(g):
        return jnp.sum((g * g).reshape(g.shape[0] // 8, 8, g.shape[1]), axis=0)

    total = ss_ref[example]
    for r in range(2):
        part = pl.ds(r * quarter_d, quarter_d)
        own = pl.ds(pl.multiple_of(r * quarter_d + x_pos * half_d, 16), quarter_d)
        far = pl.ds(pl.multiple_of(r * quarter_d + (1 - x_pos) * half_d, 16), quarter_d)
        g = dot_nn(x_t[own, :], dh[...])
        g1_st[own, :] = g
        total = total + square(g)
        g = dot_nn(x_t[far, :], dh[...])
        g1_st[far, :] = g
        g1s_st[part, :] = g.astype(BF16)
        total = total + square(g)
        for at in (part, pl.ds(r * quarter_d + half_d, quarter_d)):
            g = dot_nn(dz_t[at, :], h[...])
            g2_st[at, :] = g
            g2s_st[at, :] = g.astype(BF16)
            total = total + square(g)
    ss_ref[example] = total
    for cond, cp in out_copies(task, step):
        pl.when(cond)(cp.start)

    @pl.when(ends_early)
    def _():
        dx_out.wait()
        tp_copy(task).start()

    @pl.when((step == n_steps - 1) & (task < n_task - 1))
    def _():
        nxt = task + 1

        @pl.when(nxt >= n_ex)
        def _():
            tp_copy(nxt - n_ex).wait()

        for c in range(IN_SLOTS - 1):
            in_start(nxt, c)

    @pl.when((step == n_steps - 1) & (task == n_task - 1))
    def _():
        finish_block(task, step)
        far_copy(0, g1s_hbm, g1r_hbm).wait()
        far_copy(1, g2s_hbm, g2r_hbm).wait()
        far_copy(2, g1e_hbm, g1er_hbm).wait()
        far_copy(3, g2e_hbm, g2er_hbm).wait()


def run_stack(pre_act, w_in, w_out, block_in, d_out):
    n_layers, n_ex, n_tok, d_model = block_in.shape
    d_ff = pre_act.shape[3]
    n_steps = d_ff // F_BLOCK
    half_d, half_f = d_model // 2, d_ff // 2
    n_early = (n_layers - 1) * n_ex
    top = n_layers - 1

    def fb(j):
        dp = lax.axis_index('dp')
        return block_at(j, n_steps // 2, lax.rem(dp, 2), dp // 2)

    def w1_at(t, j):
        is_last = t // n_early
        return jnp.maximum(top - t // n_ex, 1), 0, fb((1 - is_last) * j + is_last * (n_steps - 1))

    in_specs = [
        pl.BlockSpec((1, 1, n_tok, F_BLOCK), lambda t, j: (top - t // n_ex, lax.rem(t, n_ex), 0, fb(j))),
        pl.BlockSpec((1, d_model, F_BLOCK), w1_at),
        pl.BlockSpec((1, F_BLOCK, d_model), lambda t, j: (top - t // n_ex, fb(j), 0)),
        pl.BlockSpec(memory_space=ANY),
        pl.BlockSpec(memory_space=ANY),
    ]
    sds = jax.ShapeDtypeStruct
    outs = [
        sds((n_early, n_tok, d_model), BF16), sds((n_early, n_tok, d_model), BF16), sds((n_ex, n_tok, d_model), BF16),
        sds((n_early, half_d, d_ff), F32), sds((n_early, half_d, d_ff), BF16), sds((n_early, half_d, d_ff), BF16),
        sds((n_early, d_model, half_f), F32), sds((n_early, d_model, half_f), BF16), sds((n_early, d_model, half_f), BF16),
        sds((n_ex, d_model, d_ff), F32), sds((n_ex, d_model, d_ff), F32),
        sds((n_ex, d_model // 4, d_ff), BF16), sds((n_ex, d_model // 4, d_ff), BF16),
        sds((n_ex, d_model, d_ff // 4), BF16), sds((n_ex, d_model, d_ff // 4), BF16),
        sds((n_ex, 8, F_BLOCK), F32),
    ]
    out_specs = [pl.BlockSpec(memory_space=ANY)] * (len(outs) - 1) + [pl.BlockSpec((n_ex, 8, F_BLOCK), lambda t, j: (0, 0, 0))]
    vm = pltpu.VMEM
    scratch = [
        vm((d_model, n_tok), BF16), vm((n_tok, d_model), BF16), vm((d_model, n_tok), BF16),
        vm((n_tok, F_BLOCK), BF16), vm((n_tok, F_BLOCK), BF16), vm((n_tok, d_model), F32),
        *[vm((IN_SLOTS, T_CHUNK, d_model), BF16)] * 4,
        vm((d_model, F_BLOCK), F32), vm((half_d, F_BLOCK), BF16), vm((d_model, F_BLOCK), F32), vm((d_model, F_BLOCK), BF16),
        pltpu.SemaphoreType.DMA((4, IN_SLOTS)), pltpu.SemaphoreType.DMA((4,)), pltpu.SemaphoreType.DMA((2,)),
        pltpu.SemaphoreType.DMA((n_early,)), pltpu.SemaphoreType.DMA((n_early,)),
        pltpu.SemaphoreType.DMA((4,)), pltpu.SemaphoreType.DMA((4,)),
    ]
    n_dots = 4 * n_early + 3 * n_ex
    return pl.pallas_call(
        functools.partial(stack_kernel, n_layers, n_ex, n_steps),
        out_shape=outs,
        grid_spec=pltpu.PrefetchScalarGridSpec(
            num_scalar_prefetch=0, grid=(n_early + n_ex, n_steps), in_specs=in_specs, out_specs=out_specs, scratch_shapes=scratch),
        compiler_params=pltpu.CompilerParams(
            dimension_semantics=('arbitrary', 'arbitrary'), vmem_limit_bytes=VMEM_LIMIT, has_side_effects=True),
        cost_estimate=pl.CostEstimate(
            flops=2 * n_dots * n_tok * d_model * d_ff, bytes_accessed=500_000_000, transcendentals=2 * n_tok * d_ff),
        name='stack',
    )(pre_act, w_in, w_out, block_in, d_out)


def mix_kernel(sc_ref, coef_ref, *refs):
    def group(r, carry):
        rows = pl.ds(pl.multiple_of(r * MIX_ROWS, MIX_ROWS), MIX_ROWS)
        total = refs[0][0, rows, :].astype(F32) * coef_ref[0]
        for k, ref in enumerate(refs[1:-1]):
            total = total + ref[0, rows, :].astype(F32) * coef_ref[k + 1]
        refs[-1][rows, :] = total.astype(BF16)
        return carry

    lax.fori_loop(0, refs[-1].shape[0] // MIX_ROWS, group, 0)


def mix(which, shape, terms, coefs):
    rows, width = shape
    block = (rows, width // 4) if which == 0 else (rows // 4, width)

    def spec(k, lead):
        if which == 0:
            return pl.BlockSpec((1, *block), lambda i, sc: (lead, sc[k], i))
        return pl.BlockSpec((1, *block), lambda i, sc: (lead, i, sc[k]))

    out_map = (lambda i, sc: (0, i)) if which == 0 else (lambda i, sc: (i, 0))
    places = jnp.stack([jnp.asarray(p, jnp.int32) for _, _, p in terms])
    return pl.pallas_call(
        mix_kernel,
        out_shape=jax.ShapeDtypeStruct((rows, width), BF16),
        grid_spec=pltpu.PrefetchScalarGridSpec(
            num_scalar_prefetch=1, grid=(4,),
            in_specs=[pl.BlockSpec(memory_space=pltpu.SMEM)] + [spec(k, lead) for k, (_, lead, _) in enumerate(terms)],
            out_specs=pl.BlockSpec(block, out_map)),
        compiler_params=pltpu.CompilerParams(dimension_semantics=('arbitrary',), vmem_limit_bytes=40_000_000),
        cost_estimate=pl.CostEstimate(flops=2 * len(terms) * rows * width, bytes_accessed=14 * rows * width, transcendentals=0),
        name='mix',
    )(places, coefs, *[v for v, _, _ in terms])


def put_in_kernel(sc_ref, coef_ref, piece_ref, noise_ref, *rest):
    out_ref = rest[-1]
    out_ref[0, 0] = (piece_ref[...].astype(F32) + coef_ref[0] * noise_ref[0, 0]) * coef_ref[1]


def put_out_kernel(sc_ref, coef_ref, piece_ref, noise_ref, *rest):
    out_ref = rest[-1]
    out_ref[0, 0] = (piece_ref[...].astype(F32).T + coef_ref[0] * noise_ref[0, 0]) * coef_ref[1]


def put_piece(transposed, total, layer, quarter, coef, piece, noise):
    if transposed:
        rows, width = piece.shape[1], piece.shape[0]
        block = 256
        piece_spec = pl.BlockSpec((width, block), lambda i, sc: (0, i))
    else:
        rows, width = piece.shape
        block = rows // 2
        piece_spec = pl.BlockSpec((block, width), lambda i, sc: (i, 0))
    big_spec = pl.BlockSpec((1, 1, block, width), lambda i, sc: (sc[0], sc[1], i, 0))
    args = [jnp.stack([jnp.int32(layer), quarter]), coef, piece, noise]
    in_specs = [pl.BlockSpec(memory_space=pltpu.SMEM), piece_spec, big_spec]
    aliases = {}
    if total is not None:
        args.append(total)
        in_specs.append(pl.BlockSpec(memory_space=ANY))
        aliases = {4: 0}
    return pl.pallas_call(
        put_out_kernel if transposed else put_in_kernel,
        out_shape=jax.ShapeDtypeStruct(noise.shape, F32),
        grid_spec=pltpu.PrefetchScalarGridSpec(
            num_scalar_prefetch=1, grid=(rows // block,), in_specs=in_specs, out_specs=big_spec),
        input_output_aliases=aliases,
        compiler_params=pltpu.CompilerParams(dimension_semantics=('arbitrary',), vmem_limit_bytes=40_000_000),
        cost_estimate=pl.CostEstimate(flops=4 * rows * width, bytes_accessed=10 * rows * width, transcendentals=0),
        name='put_out' if transposed else 'put_in',
    )(*args)


def solution(mesh):
    data_size = mesh.shape['dp']
    swap_x = [(i, i ^ 1) for i in range(data_size)]
    swap_y = [(i, i ^ 2) for i in range(data_size)]

    def local_step(block_in, pre_act, w_in, w_out, d_out, noise_in, noise_out, clip_norm, noise_mult):
        n_layers, local_batch, _, d_model = block_in.shape
        d_ff = pre_act.shape[3]
        batch_total = local_batch * data_size
        dp = lax.axis_index('dp')
        x_pos, y_pos = lax.rem(dp, 2), dp // 2
        over_x = lambda v: lax.ppermute(v, 'dp', swap_x)
        over_y = lambda v: lax.ppermute(v, 'dp', swap_y)
        res = run_stack(pre_act, w_in, w_out, block_in, d_out)
        g1k, _, g1r, g2k, _, g2r, g1l, g2l, _, g1er, _, g2er, squares = res[3:]
        part_sq = jnp.sum(squares, axis=(1, 2))
        clip = jnp.minimum(1.0, clip_norm / jnp.sqrt(lax.psum(part_sq, 'tp')))
        clip_x = over_x(clip)
        clip_y = over_y(clip)
        c_own, c_x, c_y = [[v[k] for k in range(local_batch)] for v in (clip, clip_x, clip_y)]
        coef = jnp.stack([noise_mult * clip_norm, jnp.float32(1.0 / batch_total)])

        noise_in4 = noise_in.reshape(n_layers, 4, d_model // 4, d_ff)
        noise_out4 = noise_out.reshape(n_layers, 4, d_ff // 4, d_model)

        shapes = ((d_model // 4, d_ff), (d_model, d_ff // 4))
        at_half, at_side = (x_pos, y_pos), (y_pos, x_pos)
        over_half, over_side = (over_x, over_y), (over_y, over_x)
        early, early_far, late = (g1k, g2k), (g1r, g2r), (g1l, g2l)

        def own_terms(layer, which, half_pos, pos):
            if layer == 0:
                return [(late[which], k, 2 * half_pos + pos) for k in range(local_batch)]
            first = (n_layers - 1 - layer) * local_batch
            return [(early[which], first + k, pos) for k in range(local_batch)]

        made = []

        def mixed(which, terms, coefs):
            coefs = jnp.stack([jnp.asarray(c, F32) for c in coefs])
            if made:
                coefs, _ = lax.optimization_barrier((coefs, made[-1]))
            made.append(mix(which, shapes[which], terms, coefs))
            return made[-1]

        def pair_terms(layer, which, to_send, *more):
            pos = 1 - at_side[which] if to_send else at_side[which]
            terms, coefs = own_terms(layer, which, at_half[which], pos), list(c_own)
            if layer == 0 and not to_send:
                more = (far_last[which], *more)
            else:
                if layer == 0:
                    terms += [((g1er, g2er)[which], k, 0) for k in range(local_batch)]
                else:
                    first = (n_layers - 1 - layer) * local_batch
                    terms += [(early_far[which], first + k, pos) for k in range(local_batch)]
                coefs += c_y if which else c_x
            terms += [(v[None], 0, 0) for v in more]
            return terms, coefs + [1.0] * len(more)

        got, far_last, places = {}, {}, {}
        for which in (0, 1):
            far_last[which] = over_half[which](
                mixed(which, own_terms(0, which, 1 - at_half[which], at_side[which]), c_own))
        for layer in range(n_layers - 1, -1, -1):
            for which in (0, 1):
                got[layer, which] = over_side[which](mixed(which, *pair_terms(layer, which, True)))
        for layer in range(n_layers - 1, -1, -1):
            for which in (0, 1):
                half_pos, pos = at_half[which], at_side[which]
                own = mixed(which, *pair_terms(layer, which, False, got[layer, which]))
                near = over_side[which](own)
                side = over_half[which](own)
                diag = over_half[which](near)
                places[layer, which] = (
                    (2 * half_pos + pos, own), (2 * half_pos + 1 - pos, near),
                    (2 * (1 - half_pos) + pos, side), (2 * (1 - half_pos) + 1 - pos, diag))
        grads, noises = [None, None], (noise_in4, noise_out4)
        for kind in range(4):
            for layer in range(n_layers - 1, -1, -1):
                for which in (0, 1):
                    at, piece = places[layer, which][kind]
                    grads[which] = put_piece(which == 1, grads[which], layer, at, coef, piece, noises[which])
        grad_in, grad_out = grads
        return grad_in.reshape(n_layers, d_model, d_ff), grad_out.reshape(n_layers, d_ff, d_model)

    return jax.shard_map(
        local_step,
        mesh=mesh,
        in_specs=(P(None, 'dp', None, None), P(None, 'dp', None, 'tp'), P(None, None, 'tp'), P(None, 'tp', None),
                  P('dp', None, None), P(None, None, 'tp'), P(None, 'tp', None), P(), P()),
        out_specs=(P(None, None, 'tp'), P(None, 'tp', None)),
        check_vma=False,
    )
```

```python
import functools

import jax
import jax.numpy as jnp
from jax import lax
from jax.experimental import pallas as pl
from jax.experimental.pallas import tpu as pltpu
from jax.sharding import PartitionSpec as P


INV_SQRT2 = 0.7071067811865476
INV_SQRT_2PI = 0.3989422804014327
LOG2_E = 1.4426950408889634
F_BLOCK = 512
T_CHUNK = 256
IN_SLOTS = 4
LOAD_CHUNKS = 2
MIX_ROWS = 32
N_SUM, N_FIRST, N_PUT = 20, 12, 32
VMEM_LIMIT = 67_000_000

F32 = jnp.float32
BF16 = jnp.bfloat16
ANY = pl.ANY
MESH = pl.DeviceIdType.MESH


def dot_nn(a, b):
    return lax.dot_general(a, b, (((1,), (0,)), ((), ())), preferred_element_type=F32)


def dot_nt(a, b):
    return lax.dot_general(a, b, (((1,), (1,)), ((), ())), preferred_element_type=F32)


def block_at(j, n_half, x_pos, y_pos):
    far = n_half * (1 - y_pos) + x_pos * j + (1 - x_pos) * (n_half - 1 - j)
    own = n_half * y_pos + j - n_half
    is_far = 1 - j // n_half
    return is_far * far + (1 - is_far) * own


def stack_kernel(n_layers, n_ex, n_steps, u_hbm, w1_hbm, w2_hbm, x_hbm, dout_hbm,
                 p_hbm, q_hbm, dzo_hbm, g1k_hbm, g1s_hbm, g1r_hbm, g2k_hbm, g2s_hbm, g2r_hbm,
                 g1l_hbm, g2l_hbm, g1e_hbm, g1er_hbm, g2e_hbm, g2er_hbm, ss_ref,
                 u_buf, w1_buf, w2_buf, x_t, dz, dz_t, dh, h, acc, x_st, z_st, p_st, q_st, g1_st, g1s_st, g2_st, g2s_st,
                 block_sem, in_sem, out_sem, io_sem, tp_send, tp_recv, far_send, far_recv):
    task, step = pl.program_id(0), pl.program_id(1)
    n_early = (n_layers - 1) * n_ex
    n_task = n_early + n_ex
    dp = lax.axis_index('dp')
    x_pos, y_pos = lax.rem(dp, 2), dp // 2
    x_far = {'dp': dp + 1 - 2 * x_pos}
    y_far = {'dp': dp + 2 - 4 * y_pos}
    tp_far = {'tp': 1 - lax.axis_index('tp')}
    n_tok, d_model = dz.shape
    half_d, quarter_d = d_model // 2, d_model // 4
    n_half = n_steps // 2
    half_b = F_BLOCK // 2
    n_t = n_tok // T_CHUNK
    example = lax.rem(task, n_ex)
    cols = lambda k: pl.ds(pl.multiple_of(k * F_BLOCK, F_BLOCK), F_BLOCK)
    chunk = lambda c: pl.ds(c * T_CHUNK if isinstance(c, int) else pl.multiple_of(c * T_CHUNK, T_CHUNK), T_CHUNK)

    def fetch(act, t, j, slot):
        layer, at = n_layers - 1 - t // n_ex, cols(block_at(j, n_half, x_pos, y_pos))

        def one(k, src, dst):
            getattr(pltpu.make_async_copy(src, dst.at[slot], block_sem.at[k, slot]), act)()

        one(0, u_hbm.at[layer, lax.rem(t, n_ex), :, at], u_buf)
        one(1, w2_hbm.at[layer, at, :], w2_buf)
        pl.when(t < n_early)(lambda: one(2, w1_hbm.at[layer, :, at], w1_buf))

    ends = (step + 1) // n_steps
    now = lax.rem(task * n_steps + step, 2)

    def rarely(cond, body, n=1):
        def trip(i, carry):
            body(i)
            return carry

        lax.fori_loop(0, jnp.where(cond, n, 0), trip, 0)

    is_first = (task == 0) & (step == 0)
    rarely(is_first, lambda i: fetch('start', task, step, now))
    pl.when(task + ends < n_task)(lambda: fetch('start', task + ends, step + 1 - n_steps * ends, 1 - now))

    def in_start(t, c):
        slot, rows, ex = lax.rem(c, IN_SLOTS), chunk(c), lax.rem(t, n_ex)
        copy = lambda k, src, dst: pltpu.make_async_copy(src, dst.at[slot], in_sem.at[k, slot]).start()
        copy(0, x_hbm.at[n_layers - 1 - t // n_ex, ex, rows, :], x_st)

        @pl.when(t < n_early)
        def _():
            copy(1, dout_hbm.at[ex, rows, :], z_st)

        @pl.when(t >= n_early)
        def _():
            copy(1, dzo_hbm.at[ex, rows, :], z_st)

        @pl.when(t >= n_ex)
        def _():
            copy(2, p_hbm.at[t - n_ex, rows, :], p_st)
            copy(3, q_hbm.at[t - n_ex, rows, :], q_st)

    def in_wait(c):
        slot, rows = lax.rem(c, IN_SLOTS), chunk(c)
        wait = lambda k, dst: pltpu.make_async_copy(dout_hbm.at[0, rows, :], dst.at[slot], in_sem.at[k, slot]).wait()
        wait(0, x_st)
        wait(1, z_st)

        @pl.when(task >= n_ex)
        def _():
            wait(2, p_st)
            wait(3, q_st)

    def tp_copy(t):
        return pltpu.make_async_remote_copy(
            src_ref=p_hbm.at[t], dst_ref=q_hbm.at[t], send_sem=tp_send.at[t], recv_sem=tp_recv.at[t],
            device_id=tp_far, device_id_type=MESH)

    def front(load, to_dx):
        n_in = (2 if to_dx else 1) * LOAD_CHUNKS if load else n_t

        def trip(i, carry):
            def dx_part(rows):
                part = dot_nt(dh[rows, :], w1_buf[now])
                acc[rows, :] = part if load else acc[rows, :] + part

            for s in range(n_in):
                c = i * n_in + s
                rows = chunk(c)
                if load:
                    @pl.when(c + IN_SLOTS - 1 < n_t)
                    def _():
                        in_start(task, c + IN_SLOTS - 1)

                    in_wait(c)
                    slot = lax.rem(c, IN_SLOTS)
                    z = z_st[slot]
                    moved = (z.astype(F32) + (p_st[slot].astype(F32) + q_st[slot].astype(F32))).astype(BF16)
                    z = jnp.where(task >= n_ex, moved, z) if to_dx else moved
                    dz[rows, :] = z
                    dz_t[:, rows] = z.T
                    x_t[:, rows] = x_st[slot].T
                u = u_buf[now, rows, :].astype(F32)
                t = u * INV_SQRT2
                cdf = 0.5 * lax.erf(t) + 0.5
                h[rows, :] = (u * cdf).astype(BF16)
                slope = cdf + (t * (INV_SQRT_2PI / INV_SQRT2)) * jnp.exp2((t * t) * -LOG2_E)
                dh[rows, :] = (slope * dot_nt(dz[rows, :], w2_buf[now])).astype(BF16)
                if to_dx and s:
                    dx_part(chunk(c - 1))
            if to_dx:
                dx_part(chunk(i * n_in + n_in - 1))
            return carry

        if n_in == n_t:
            trip(0, 0)
        else:
            lax.fori_loop(0, n_t // n_in, trip, 0)

    def begin(c):
        ss_ref[...] = jnp.zeros_like(ss_ref)
        in_start(task, c)

    rarely(is_first, begin, IN_SLOTS - 1)

    fetch('wait', task, step, now)
    for load in (True, False):
        for to_dx in (True, False):
            @pl.when(((step == 0) if load else (step > 0)) & ((task < n_early) if to_dx else (task >= n_early)))
            def _():
                front(load, to_dx)

    dz_keep = pltpu.make_async_copy(dz, dzo_hbm.at[example], io_sem.at[0])
    is_mid = (task >= n_ex) & (task < n_early)
    pl.when(is_mid & (step == 0))(dz_keep.start)
    ends_early = (step == n_steps - 1) & (task < n_early)
    dx_out = pltpu.make_async_copy(dz, p_hbm.at[task], io_sem.at[1])

    @pl.when(ends_early)
    def _():
        pl.when(is_mid)(dz_keep.wait)

        def put(c, carry):
            dz[chunk(c), :] = acc[chunk(c), :].astype(BF16)
            return carry

        lax.fori_loop(0, n_t, put, 0)
        dx_out.start()

    def far_copy(axis, src, dst):
        return pltpu.make_async_remote_copy(
            src_ref=src, dst_ref=dst, send_sem=far_send.at[axis], recv_sem=far_recv.at[axis],
            device_id=y_far if axis % 2 else x_far, device_id_type=MESH)

    own_rows = pl.ds(pl.multiple_of(x_pos * half_d, 16), half_d)
    pass_rows = pl.ds(pl.multiple_of((1 - y_pos) * quarter_d, 16), quarter_d)
    cut_half = pl.ds(pl.multiple_of((1 - x_pos) * half_b, half_b), half_b)
    to_half = pl.ds(pl.multiple_of(x_pos * F_BLOCK, half_b), half_b)
    to_full = pl.ds(pl.multiple_of((1 - x_pos) * half_b, half_b), F_BLOCK)

    def block(act, t, j):
        far_k = x_pos * j + (1 - x_pos) * (n_half - 1 - j)
        far_at, own_at = cols(far_k), cols(j - n_half)
        fb_at = cols(block_at(j, n_half, x_pos, y_pos))

        def local(n, src, dst):
            cp = pltpu.make_async_copy(src, dst, out_sem.at[n])
            (cp.start if act == 'start' else cp.wait)()

        def far(axis, src, dst):
            if act == 'end':
                far_copy(axis, src, dst).start()

        @pl.when(t < n_early)
        def _():
            local(0, g1_st.at[own_rows, :], g1k_hbm.at[t, :, fb_at])
            local(1, g1s_st, g1s_hbm.at[t, :, fb_at])
            far(0, g1s_hbm.at[t, :, fb_at], g1r_hbm.at[t, :, fb_at])

            @pl.when(j < n_half)
            def _():
                local(2, g2s_st, g2s_hbm.at[t, :, far_at])
                far(1, g2s_hbm.at[t, :, far_at], g2r_hbm.at[t, :, far_at])

            @pl.when(j >= n_half)
            def _():
                local(3, g2_st, g2k_hbm.at[t, :, own_at])

        @pl.when(t >= n_early)
        def _():
            ex = t - n_early
            local(1, g1s_st.at[pass_rows, :], g1e_hbm.at[ex, :, fb_at])
            far(2, g1e_hbm.at[ex, :, fb_at], g1er_hbm.at[ex, :, fb_at])
            local(0, g1_st, g1l_hbm.at[ex, :, fb_at])
            local(3, g2_st, g2l_hbm.at[ex, :, fb_at])

            @pl.when(j == 0)
            def _():
                local(2, g2s_st, g2e_hbm.at[ex, :, to_full])
                far(3, g2e_hbm.at[ex, :, to_full], g2er_hbm.at[ex, :, to_full])

            @pl.when(j == 1)
            def _():
                local(2, g2s_st.at[:, cut_half], g2e_hbm.at[ex, :, to_half])
                far(3, g2e_hbm.at[ex, :, to_half], g2er_hbm.at[ex, :, to_half])

    @pl.when((task > 0) | (step > 0))
    def _():
        block('end', jnp.where(step > 0, task, task - 1), jnp.where(step > 0, step - 1, n_steps - 1))

    def square(g):
        return jnp.sum((g * g).reshape(g.shape[0] // 8, 8, g.shape[1]), axis=0)

    total = ss_ref[example]
    for r in range(2):
        part = pl.ds(r * quarter_d, quarter_d)
        own = pl.ds(pl.multiple_of(r * quarter_d + x_pos * half_d, 16), quarter_d)
        far = pl.ds(pl.multiple_of(r * quarter_d + (1 - x_pos) * half_d, 16), quarter_d)
        g = dot_nn(x_t[own, :], dh[...])
        g1_st[own, :] = g
        total = total + square(g)
        g = dot_nn(x_t[far, :], dh[...])
        g1_st[far, :] = g
        g1s_st[part, :] = g.astype(BF16)
        total = total + square(g)
        for at in (part, pl.ds(r * quarter_d + half_d, quarter_d)):
            g = dot_nn(dz_t[at, :], h[...])
            g2_st[at, :] = g
            g2s_st[at, :] = g.astype(BF16)
            total = total + square(g)
    ss_ref[example] = total
    block('start', task, step)

    @pl.when(ends_early)
    def _():
        dx_out.wait()
        tp_copy(task).start()

    ends_task, ends_all = (step == n_steps - 1) & (task < n_task - 1), (step == n_steps - 1) & (task == n_task - 1)
    rarely(ends_task & (task + 1 >= n_ex), lambda i: tp_copy(task + 1 - n_ex).wait())
    rarely(ends_task, lambda c: in_start(task + 1, c), IN_SLOTS - 1)

    def finish(i):
        block('end', task, step)
        far_copy(0, g1s_hbm, g1r_hbm).wait()
        far_copy(1, g2s_hbm, g2r_hbm).wait()
        far_copy(2, g1e_hbm, g1er_hbm).wait()
        far_copy(3, g2e_hbm, g2er_hbm).wait()

    rarely(ends_all, finish)


def run_stack(pre_act, w_in, w_out, block_in, d_out):
    n_layers, n_ex, n_tok, d_model = block_in.shape
    d_ff = pre_act.shape[3]
    n_steps = d_ff // F_BLOCK
    half_d, half_f = d_model // 2, d_ff // 2
    n_early = (n_layers - 1) * n_ex
    sds = jax.ShapeDtypeStruct
    outs = [
        sds((n_early, n_tok, d_model), BF16), sds((n_early, n_tok, d_model), BF16), sds((n_ex, n_tok, d_model), BF16),
        sds((n_early, half_d, d_ff), F32), sds((n_early, half_d, d_ff), BF16), sds((n_early, half_d, d_ff), BF16),
        sds((n_early, d_model, half_f), F32), sds((n_early, d_model, half_f), BF16), sds((n_early, d_model, half_f), BF16),
        sds((n_ex, d_model, d_ff), F32), sds((n_ex, d_model, d_ff), F32),
        sds((n_ex, d_model // 4, d_ff), BF16), sds((n_ex, d_model // 4, d_ff), BF16),
        sds((n_ex, d_model, d_ff // 4), BF16), sds((n_ex, d_model, d_ff // 4), BF16),
        sds((n_ex, 8, F_BLOCK), F32),
    ]
    out_specs = [pl.BlockSpec(memory_space=ANY)] * (len(outs) - 1) + [pl.BlockSpec((n_ex, 8, F_BLOCK), lambda t, j: (0, 0, 0))]
    vm = pltpu.VMEM
    scratch = [
        vm((2, n_tok, F_BLOCK), BF16), vm((2, d_model, F_BLOCK), BF16), vm((2, F_BLOCK, d_model), BF16),
        vm((d_model, n_tok), BF16), vm((n_tok, d_model), BF16), vm((d_model, n_tok), BF16),
        vm((n_tok, F_BLOCK), BF16), vm((n_tok, F_BLOCK), BF16), vm((n_tok, d_model), F32),
        *[vm((IN_SLOTS, T_CHUNK, d_model), BF16)] * 4,
        vm((d_model, F_BLOCK), F32), vm((half_d, F_BLOCK), BF16), vm((d_model, F_BLOCK), F32), vm((d_model, F_BLOCK), BF16),
        pltpu.SemaphoreType.DMA((3, 2)),
        pltpu.SemaphoreType.DMA((4, IN_SLOTS)), pltpu.SemaphoreType.DMA((4,)), pltpu.SemaphoreType.DMA((2,)),
        pltpu.SemaphoreType.DMA((n_early,)), pltpu.SemaphoreType.DMA((n_early,)),
        pltpu.SemaphoreType.DMA((4,)), pltpu.SemaphoreType.DMA((4,)),
    ]
    n_dots = 4 * n_early + 3 * n_ex
    return pl.pallas_call(
        functools.partial(stack_kernel, n_layers, n_ex, n_steps),
        out_shape=outs,
        grid_spec=pltpu.PrefetchScalarGridSpec(
            num_scalar_prefetch=0, grid=(n_early + n_ex, n_steps), in_specs=[pl.BlockSpec(memory_space=ANY)] * 5, out_specs=out_specs, scratch_shapes=scratch),
        compiler_params=pltpu.CompilerParams(
            dimension_semantics=('arbitrary', 'arbitrary'), vmem_limit_bytes=VMEM_LIMIT, has_side_effects=True),
        cost_estimate=pl.CostEstimate(
            flops=2 * n_dots * n_tok * d_model * d_ff, bytes_accessed=500_000_000, transcendentals=2 * n_tok * d_ff),
        name='stack',
    )(pre_act, w_in, w_out, block_in, d_out)


def mix_kernel(sc_ref, coef_ref, *refs):
    def group(r, carry):
        rows = pl.ds(pl.multiple_of(r * MIX_ROWS, MIX_ROWS), MIX_ROWS)
        total = refs[0][0, rows, :].astype(F32) * coef_ref[0]
        for k, ref in enumerate(refs[1:-1]):
            total = total + ref[0, rows, :].astype(F32) * coef_ref[k + 1]
        refs[-1][rows, :] = total.astype(BF16)
        return carry

    lax.fori_loop(0, refs[-1].shape[0] // MIX_ROWS, group, 0)


def mix(which, shape, terms, coefs, part, n_parts):
    rows, width = shape
    part_width = width // n_parts
    block = (rows, width // 4) if which == 0 else (rows // 4, part_width)
    n_blocks = 4 // n_parts if which == 0 else 4

    def spec(k, v, lead):
        off = part * n_blocks if which == 0 and v.shape[2] > part_width else 0
        if which == 0:
            return pl.BlockSpec((1, *block), lambda i, sc: (lead, sc[k], i + off))
        return pl.BlockSpec((1, *block), lambda i, sc: (lead, i, sc[k]))

    def place(v, p):
        return p * n_parts + part if which == 1 and v.shape[2] > part_width else p

    out_map = (lambda i, sc: (0, i)) if which == 0 else (lambda i, sc: (i, 0))
    places = jnp.stack([jnp.asarray(place(v, p), jnp.int32) for v, _, p in terms])
    return pl.pallas_call(
        mix_kernel,
        out_shape=jax.ShapeDtypeStruct((rows, part_width), BF16),
        grid_spec=pltpu.PrefetchScalarGridSpec(
            num_scalar_prefetch=1, grid=(n_blocks,),
            in_specs=[pl.BlockSpec(memory_space=pltpu.SMEM)] + [spec(k, v, lead) for k, (v, lead, _) in enumerate(terms)],
            out_specs=pl.BlockSpec(block, out_map)),
        compiler_params=pltpu.CompilerParams(dimension_semantics=('arbitrary',), vmem_limit_bytes=40_000_000),
        cost_estimate=pl.CostEstimate(
            flops=2 * len(terms) * rows * part_width, bytes_accessed=14 * rows * part_width, transcendentals=0),
        name='mix',
    )(places, coefs, *[v for v, _, _ in terms])


def put_in_kernel(sc_ref, coef_ref, piece_ref, noise_ref, *rest):
    out_ref = rest[-1]
    out_ref[0, 0] = (piece_ref[...].astype(F32) + coef_ref[0] * noise_ref[0, 0]) * coef_ref[1]


def put_out_kernel(sc_ref, coef_ref, piece_ref, noise_ref, *rest):
    out_ref = rest[-1]
    out_ref[0, 0] = (piece_ref[...].astype(F32).T + coef_ref[0] * noise_ref[0, 0]) * coef_ref[1]


def put_piece(transposed, total, layer, quarter, part, coef, piece, noise):
    if transposed:
        rows, width = piece.shape[1], piece.shape[0]
        block = 256 if rows % 256 == 0 else 128
        first = part * (rows // block)
        piece_spec = pl.BlockSpec((width, block), lambda i, sc: (0, i))
        big_spec = pl.BlockSpec((1, 1, block, width), lambda i, sc: (sc[0], sc[1], first + i, 0))
    else:
        rows, width = piece.shape
        block = rows // 2
        piece_spec = pl.BlockSpec((block, width), lambda i, sc: (i, 0))
        big_spec = pl.BlockSpec((1, 1, block, width), lambda i, sc: (sc[0], sc[1], i, part))
    args = [jnp.stack([jnp.int32(layer), quarter]), coef, piece, noise]
    in_specs = [pl.BlockSpec(memory_space=pltpu.SMEM), piece_spec, big_spec]
    aliases = {}
    if total is not None:
        args.append(total)
        in_specs.append(pl.BlockSpec(memory_space=ANY))
        aliases = {4: 0}
    return pl.pallas_call(
        put_out_kernel if transposed else put_in_kernel,
        out_shape=jax.ShapeDtypeStruct(noise.shape, F32),
        grid_spec=pltpu.PrefetchScalarGridSpec(
            num_scalar_prefetch=1, grid=(rows // block,), in_specs=in_specs, out_specs=big_spec),
        input_output_aliases=aliases,
        compiler_params=pltpu.CompilerParams(dimension_semantics=('arbitrary',), vmem_limit_bytes=40_000_000),
        cost_estimate=pl.CostEstimate(flops=4 * rows * width, bytes_accessed=10 * rows * width, transcendentals=0),
        name='put_out' if transposed else 'put_in',
    )(*args)


def solution(mesh):
    data_size = mesh.shape['dp']
    swap_x = [(i, i ^ 1) for i in range(data_size)]
    swap_y = [(i, i ^ 2) for i in range(data_size)]

    def local_step(block_in, pre_act, w_in, w_out, d_out, noise_in, noise_out, clip_norm, noise_mult):
        n_layers, local_batch, _, d_model = block_in.shape
        d_ff = pre_act.shape[3]
        batch_total = local_batch * data_size
        dp = lax.axis_index('dp')
        x_pos, y_pos = lax.rem(dp, 2), dp // 2
        over_x = lambda v: lax.ppermute(v, 'dp', swap_x)
        over_y = lambda v: lax.ppermute(v, 'dp', swap_y)
        res = run_stack(pre_act, w_in, w_out, block_in, d_out)
        g1k, _, g1r, g2k, _, g2r, g1l, g2l, _, g1er, _, g2er, squares = res[3:]
        part_sq = jnp.sum(squares, axis=(1, 2))
        clip = jnp.minimum(1.0, clip_norm / jnp.sqrt(lax.psum(part_sq, 'tp')))
        clip_x = over_x(clip)
        clip_y = over_y(clip)
        c_own, c_x, c_y = [[v[k] for k in range(local_batch)] for v in (clip, clip_x, clip_y)]
        coef = jnp.stack([noise_mult * clip_norm, jnp.float32(1.0 / batch_total)])

        noise_in4 = noise_in.reshape(n_layers, 4, d_model // 4, d_ff)
        noise_out4 = noise_out.reshape(n_layers, 4, d_ff // 4, d_model)

        shapes = ((d_model // 4, d_ff), (d_model, d_ff // 4))
        at_half, at_side = (x_pos, y_pos), (y_pos, x_pos)
        over_half, over_side = (over_x, over_y), (over_y, over_x)
        early, early_far, late = (g1k, g2k), (g1r, g2r), (g1l, g2l)

        def own_terms(layer, which, half_pos, pos):
            if layer == 0:
                return [(late[which], k, 2 * half_pos + pos) for k in range(local_batch)]
            first = (n_layers - 1 - layer) * local_batch
            return [(early[which], first + k, pos) for k in range(local_batch)]

        made = []

        def mixed(which, terms, coefs, part, n_parts):
            coefs = jnp.stack([jnp.asarray(c, F32) for c in coefs])
            if made:
                coefs, _ = lax.optimization_barrier((coefs, made[-1]))
            made.append(mix(which, shapes[which], terms, coefs, part, n_parts))
            return made[-1]

        def pair_terms(layer, which, part, to_send, *more):
            pos = 1 - at_side[which] if to_send else at_side[which]
            terms, coefs = own_terms(layer, which, at_half[which], pos), list(c_own)
            if layer == 0 and not to_send:
                more = (far_last[part, which], *more)
            else:
                if layer == 0:
                    terms += [((g1er, g2er)[which], k, 0) for k in range(local_batch)]
                else:
                    first = (n_layers - 1 - layer) * local_batch
                    terms += [(early_far[which], first + k, pos) for k in range(local_batch)]
                coefs += c_y if which else c_x
            terms += [(v[None], 0, 0) for v in more]
            return terms, coefs + [1.0] * len(more)

        last = [(0, part, 2) for part in range(2)]
        turns = [(layer, 0, 1) for layer in range(n_layers - 1, 0, -1)] + last
        got, far_last, places = {}, {}, {}
        for _, part, n_parts in last:
            for which in (0, 1):
                terms = own_terms(0, which, 1 - at_half[which], at_side[which])
                far_last[part, which] = over_half[which](mixed(which, terms, c_own, part, n_parts))
        for layer, part, n_parts in turns:
            for which in (0, 1):
                value = mixed(which, *pair_terms(layer, which, part, True), part, n_parts)
                got[layer, part, which] = over_side[which](value)
        n_first = len(made)
        for layer, part, n_parts in turns:
            for which in (0, 1):
                half_pos, pos = at_half[which], at_side[which]
                own = mixed(which, *pair_terms(layer, which, part, False, got[layer, part, which]), part, n_parts)
                near = over_side[which](own)
                side = over_half[which](own)
                diag = over_half[which](near)
                places[layer, part, which] = (
                    (2 * half_pos + pos, own), (2 * half_pos + 1 - pos, near),
                    (2 * (1 - half_pos) + pos, side), (2 * (1 - half_pos) + 1 - pos, diag))
        grads, noises, n_put = [None, None], (noise_in4, noise_out4), 0
        for kind in range(4):
            for layer, part, _ in turns:
                for which in (0, 1):
                    at, piece = places[layer, part, which][kind]
                    grads[which] = put_piece(which == 1, grads[which], layer, at, part, coef, piece, noises[which])
                    n_put += 1
        grad_in, grad_out = grads
        assert (len(made), n_first, n_put) == (N_SUM, N_FIRST, N_PUT)
        return grad_in.reshape(n_layers, d_model, d_ff), grad_out.reshape(n_layers, d_ff, d_model)

    return jax.shard_map(
        local_step,
        mesh=mesh,
        in_specs=(P(None, 'dp', None, None), P(None, 'dp', None, 'tp'), P(None, None, 'tp'), P(None, 'tp', None),
                  P('dp', None, None), P(None, None, 'tp'), P(None, 'tp', None), P(), P()),
        out_specs=(P(None, None, 'tp'), P(None, 'tp', None)),
        check_vma=False,
    )
```

```python
import functools

import jax
import jax.numpy as jnp
from jax import lax
from jax.experimental import pallas as pl
from jax.experimental.pallas import tpu as pltpu
from jax.sharding import PartitionSpec as P


INV_SQRT2 = 0.7071067811865476
INV_SQRT_2PI = 0.3989422804014327
LOG2_E = 1.4426950408889634
F_BLOCK = 512
T_CHUNK = 256
IN_SLOTS = 4
LOAD_CHUNKS = 2
MIX_ROWS = 32
N_SUM, N_FIRST, N_PUT = 20, 12, 32
VMEM_LIMIT = 67_000_000

F32 = jnp.float32
BF16 = jnp.bfloat16
ANY = pl.ANY
MESH = pl.DeviceIdType.MESH


def dot_nn(a, b):
    return lax.dot_general(a, b, (((1,), (0,)), ((), ())), preferred_element_type=F32)


def dot_nt(a, b):
    return lax.dot_general(a, b, (((1,), (1,)), ((), ())), preferred_element_type=F32)


def block_at(j, n_half, x_pos, y_pos):
    far = n_half * (1 - y_pos) + x_pos * j + (1 - x_pos) * (n_half - 1 - j)
    own = n_half * y_pos + j - n_half
    is_far = 1 - j // n_half
    return is_far * far + (1 - is_far) * own


def stack_kernel(n_layers, n_ex, n_steps, u_hbm, w1_hbm, w2_hbm, x_hbm, dout_hbm,
                 p_hbm, q_hbm, dzo_hbm, g1k_hbm, g1s_hbm, g1r_hbm, g2k_hbm, g2s_hbm, g2r_hbm,
                 g1l_hbm, g2l_hbm, g1e_hbm, g1er_hbm, g2e_hbm, g2er_hbm, ss_hbm, ss_ref,
                 u_buf, w1_buf, w2_buf, x_t, dz, dz_t, dh, h, acc, x_st, z_st, p_st, q_st, g1_st, g1s_st, g2_st, g2s_st,
                 block_sem, in_sem, out_sem, io_sem, tp_send, tp_recv, far_send, far_recv, ss_send, ss_recv):
    task, step = pl.program_id(0), pl.program_id(1)
    n_early = (n_layers - 1) * n_ex
    n_task = n_early + n_ex
    dp = lax.axis_index('dp')
    x_pos, y_pos = lax.rem(dp, 2), dp // 2
    x_far = {'dp': dp + 1 - 2 * x_pos}
    y_far = {'dp': dp + 2 - 4 * y_pos}
    tp_far = {'tp': 1 - lax.axis_index('tp')}
    n_tok, d_model = dz.shape
    half_d, quarter_d = d_model // 2, d_model // 4
    n_half = n_steps // 2
    half_b = F_BLOCK // 2
    n_t = n_tok // T_CHUNK
    example = lax.rem(task, n_ex)
    cols = lambda k: pl.ds(pl.multiple_of(k * F_BLOCK, F_BLOCK), F_BLOCK)
    chunk = lambda c: pl.ds(c * T_CHUNK if isinstance(c, int) else pl.multiple_of(c * T_CHUNK, T_CHUNK), T_CHUNK)

    def fetch(act, t, j, slot):
        layer, at = n_layers - 1 - t // n_ex, cols(block_at(j, n_half, x_pos, y_pos))

        def one(k, src, dst):
            getattr(pltpu.make_async_copy(src, dst.at[slot], block_sem.at[k, slot]), act)()

        one(0, u_hbm.at[layer, lax.rem(t, n_ex), :, at], u_buf)
        one(1, w2_hbm.at[layer, at, :], w2_buf)
        pl.when(t < n_early)(lambda: one(2, w1_hbm.at[layer, :, at], w1_buf))

    ends = (step + 1) // n_steps
    now = lax.rem(task * n_steps + step, 2)

    def rarely(cond, body, n=1):
        def trip(i, carry):
            body(i)
            return carry

        lax.fori_loop(0, jnp.where(cond, n, 0), trip, 0)

    is_first = (task == 0) & (step == 0)
    rarely(is_first, lambda i: fetch('start', task, step, now))
    pl.when(task + ends < n_task)(lambda: fetch('start', task + ends, step + 1 - n_steps * ends, 1 - now))

    def in_start(t, c):
        slot, rows, ex = lax.rem(c, IN_SLOTS), chunk(c), lax.rem(t, n_ex)
        copy = lambda k, src, dst: pltpu.make_async_copy(src, dst.at[slot], in_sem.at[k, slot]).start()
        copy(0, x_hbm.at[n_layers - 1 - t // n_ex, ex, rows, :], x_st)

        @pl.when(t < n_early)
        def _():
            copy(1, dout_hbm.at[ex, rows, :], z_st)

        @pl.when(t >= n_early)
        def _():
            copy(1, dzo_hbm.at[ex, rows, :], z_st)

        @pl.when(t >= n_ex)
        def _():
            copy(2, p_hbm.at[t - n_ex, rows, :], p_st)
            copy(3, q_hbm.at[t - n_ex, rows, :], q_st)

    def in_wait(c):
        slot, rows = lax.rem(c, IN_SLOTS), chunk(c)
        wait = lambda k, dst: pltpu.make_async_copy(dout_hbm.at[0, rows, :], dst.at[slot], in_sem.at[k, slot]).wait()
        wait(0, x_st)
        wait(1, z_st)

        @pl.when(task >= n_ex)
        def _():
            wait(2, p_st)
            wait(3, q_st)

    def tp_copy(t):
        return pltpu.make_async_remote_copy(
            src_ref=p_hbm.at[t], dst_ref=q_hbm.at[t], send_sem=tp_send.at[t], recv_sem=tp_recv.at[t],
            device_id=tp_far, device_id_type=MESH)

    def front(load, to_dx):
        n_in = LOAD_CHUNKS if load and not to_dx else n_t

        def trip(i, carry):
            def dx_part(rows):
                part = dot_nt(dh[rows, :], w1_buf[now])
                acc[rows, :] = part if load else acc[rows, :] + part

            for s in range(n_in):
                c = i * n_in + s
                rows = chunk(c)
                if load:
                    @pl.when(c + IN_SLOTS - 1 < n_t)
                    def _():
                        in_start(task, c + IN_SLOTS - 1)

                    in_wait(c)
                    slot = lax.rem(c, IN_SLOTS)
                    z = z_st[slot]
                    moved = (z.astype(F32) + (p_st[slot].astype(F32) + q_st[slot].astype(F32))).astype(BF16)
                    z = jnp.where(task >= n_ex, moved, z) if to_dx else moved
                    dz[rows, :] = z
                    dz_t[:, rows] = z.T
                    x_t[:, rows] = x_st[slot].T
                u = u_buf[now, rows, :].astype(F32)
                t = u * INV_SQRT2
                cdf = 0.5 * lax.erf(t) + 0.5
                h[rows, :] = (u * cdf).astype(BF16)
                slope = cdf + (t * (INV_SQRT_2PI / INV_SQRT2)) * jnp.exp2((t * t) * -LOG2_E)
                dh[rows, :] = (slope * dot_nt(dz[rows, :], w2_buf[now])).astype(BF16)
                if to_dx and s:
                    dx_part(chunk(c - 1))
            if to_dx:
                dx_part(chunk(i * n_in + n_in - 1))
            return carry

        if n_in == n_t:
            trip(0, 0)
        else:
            lax.fori_loop(0, n_t // n_in, trip, 0)

    def begin(c):
        ss_ref[...] = jnp.zeros_like(ss_ref)
        in_start(task, c)

    rarely(is_first, begin, IN_SLOTS - 1)

    fetch('wait', task, step, now)
    for load in (True, False):
        for to_dx in (True, False):
            @pl.when(((step == 0) if load else (step > 0)) & ((task < n_early) if to_dx else (task >= n_early)))
            def _():
                front(load, to_dx)

    dz_keep = pltpu.make_async_copy(dz, dzo_hbm.at[example], io_sem.at[0])
    is_mid = (task >= n_ex) & (task < n_early)
    pl.when(is_mid & (step == 0))(dz_keep.start)
    ends_early = (step == n_steps - 1) & (task < n_early)
    dx_out = pltpu.make_async_copy(dz, p_hbm.at[task], io_sem.at[1])

    @pl.when(ends_early)
    def _():
        pl.when(is_mid)(dz_keep.wait)

        def put(c, carry):
            dz[chunk(c), :] = acc[chunk(c), :].astype(BF16)
            return carry

        lax.fori_loop(0, n_t, put, 0)
        dx_out.start()

    def far_copy(axis, src, dst):
        return pltpu.make_async_remote_copy(
            src_ref=src, dst_ref=dst, send_sem=far_send.at[axis], recv_sem=far_recv.at[axis],
            device_id=y_far if axis % 2 else x_far, device_id_type=MESH)

    own_rows = pl.ds(pl.multiple_of(x_pos * half_d, 16), half_d)
    pass_rows = pl.ds(pl.multiple_of((1 - y_pos) * quarter_d, 16), quarter_d)
    cut_half = pl.ds(pl.multiple_of((1 - x_pos) * half_b, half_b), half_b)
    to_half = pl.ds(pl.multiple_of(x_pos * F_BLOCK, half_b), half_b)
    to_full = pl.ds(pl.multiple_of((1 - x_pos) * half_b, half_b), F_BLOCK)

    def block(act, t, j):
        far_k = x_pos * j + (1 - x_pos) * (n_half - 1 - j)
        far_at, own_at = cols(far_k), cols(j - n_half)
        fb_at = cols(block_at(j, n_half, x_pos, y_pos))

        def local(n, src, dst):
            cp = pltpu.make_async_copy(src, dst, out_sem.at[n])
            (cp.start if act == 'start' else cp.wait)()

        def far(axis, src, dst):
            if act == 'end':
                far_copy(axis, src, dst).start()

        @pl.when(t < n_early)
        def _():
            local(0, g1_st.at[own_rows, :], g1k_hbm.at[t, :, fb_at])
            local(1, g1s_st, g1s_hbm.at[t, :, fb_at])
            far(0, g1s_hbm.at[t, :, fb_at], g1r_hbm.at[t, :, fb_at])

            @pl.when(j < n_half)
            def _():
                local(2, g2s_st, g2s_hbm.at[t, :, far_at])
                far(1, g2s_hbm.at[t, :, far_at], g2r_hbm.at[t, :, far_at])

            @pl.when(j >= n_half)
            def _():
                local(3, g2_st, g2k_hbm.at[t, :, own_at])

        @pl.when(t >= n_early)
        def _():
            ex = t - n_early
            local(1, g1s_st.at[pass_rows, :], g1e_hbm.at[ex, :, fb_at])
            pl.when((t < n_task - 1) | (j < n_steps - 1))(lambda: far(2, g1e_hbm.at[ex, :, fb_at], g1er_hbm.at[ex, :, fb_at]))
            local(0, g1_st, g1l_hbm.at[ex, :, fb_at])
            local(3, g2_st, g2l_hbm.at[ex, :, fb_at])

            @pl.when(j == 0)
            def _():
                local(2, g2s_st, g2e_hbm.at[ex, :, to_full])
                far(3, g2e_hbm.at[ex, :, to_full], g2er_hbm.at[ex, :, to_full])

            @pl.when(j == 1)
            def _():
                local(2, g2s_st.at[:, cut_half], g2e_hbm.at[ex, :, to_half])
                far(3, g2e_hbm.at[ex, :, to_half], g2er_hbm.at[ex, :, to_half])

    @pl.when((task > 0) | (step > 0))
    def _():
        block('end', jnp.where(step > 0, task, task - 1), jnp.where(step > 0, step - 1, n_steps - 1))

    def square(g):
        return jnp.sum((g * g).reshape(g.shape[0] // 8, 8, g.shape[1]), axis=0)

    total = ss_ref[example]
    for r in range(2):
        part = pl.ds(r * quarter_d, quarter_d)
        own = pl.ds(pl.multiple_of(r * quarter_d + x_pos * half_d, 16), quarter_d)
        far = pl.ds(pl.multiple_of(r * quarter_d + (1 - x_pos) * half_d, 16), quarter_d)
        g = dot_nn(x_t[own, :], dh[...])
        g1_st[own, :] = g
        total = total + square(g)
        g = dot_nn(x_t[far, :], dh[...])
        g1_st[far, :] = g
        g1s_st[part, :] = g.astype(BF16)
        total = total + square(g)
        for at in (part, pl.ds(r * quarter_d + half_d, quarter_d)):
            g = dot_nn(dz_t[at, :], h[...])
            g2_st[at, :] = g
            g2s_st[at, :] = g.astype(BF16)
            total = total + square(g)
    ss_ref[example] = total
    block('start', task, step)
    ends_all = (step == n_steps - 1) & (task == n_task - 1)

    def last_far(i):
        at = cols(block_at(step, n_half, x_pos, y_pos))
        far_copy(2, g1s_st.at[pass_rows, :], g1er_hbm.at[n_ex - 1, :, at]).start()

    rarely(ends_all, last_far)

    @pl.when(ends_early)
    def _():
        dx_out.wait()
        tp_copy(task).start()

    ends_task = (step == n_steps - 1) & (task < n_task - 1)
    rarely(ends_task & (task + 1 >= n_ex), lambda i: tp_copy(task + 1 - n_ex).wait())
    rarely(ends_task, lambda c: in_start(task + 1, c), IN_SLOTS - 1)

    def finish(i):
        keep = pltpu.make_async_copy(ss_ref, ss_hbm.at[0], io_sem.at[0])
        keep.start()
        keep.wait()
        tp = lax.axis_index('tp')
        peers = [
            {'dp': dp, 'tp': 1 - tp}, {**x_far, 'tp': tp}, {**x_far, 'tp': 1 - tp}, {**y_far, 'tp': tp}, {**y_far, 'tp': 1 - tp}]
        sums = [
            pltpu.make_async_remote_copy(
                src_ref=ss_hbm.at[0], dst_ref=ss_hbm.at[k + 1], send_sem=ss_send.at[k], recv_sem=ss_recv.at[k],
                device_id=peer, device_id_type=MESH)
            for k, peer in enumerate(peers)]
        for cp in sums:
            cp.start()
        block('end', task, step)
        for cp in sums:
            cp.wait()
        far_copy(0, g1s_hbm, g1r_hbm).wait()
        far_copy(1, g2s_hbm, g2r_hbm).wait()
        far_copy(2, g1e_hbm, g1er_hbm).wait()
        far_copy(3, g2e_hbm, g2er_hbm).wait()

    rarely(ends_all, finish)


def run_stack(pre_act, w_in, w_out, block_in, d_out):
    n_layers, n_ex, n_tok, d_model = block_in.shape
    d_ff = pre_act.shape[3]
    n_steps = d_ff // F_BLOCK
    half_d, half_f = d_model // 2, d_ff // 2
    n_early = (n_layers - 1) * n_ex
    sds = jax.ShapeDtypeStruct
    outs = [
        sds((n_early, n_tok, d_model), BF16), sds((n_early, n_tok, d_model), BF16), sds((n_ex, n_tok, d_model), BF16),
        sds((n_early, half_d, d_ff), F32), sds((n_early, half_d, d_ff), BF16), sds((n_early, half_d, d_ff), BF16),
        sds((n_early, d_model, half_f), F32), sds((n_early, d_model, half_f), BF16), sds((n_early, d_model, half_f), BF16),
        sds((n_ex, d_model, d_ff), F32), sds((n_ex, d_model, d_ff), F32),
        sds((n_ex, d_model // 4, d_ff), BF16), sds((n_ex, d_model // 4, d_ff), BF16),
        sds((n_ex, d_model, d_ff // 4), BF16), sds((n_ex, d_model, d_ff // 4), BF16),
        sds((6, n_ex, 8, F_BLOCK), F32),
    ]
    out_specs = [pl.BlockSpec(memory_space=ANY)] * len(outs)
    vm = pltpu.VMEM
    scratch = [
        vm((n_ex, 8, F_BLOCK), F32),
        vm((2, n_tok, F_BLOCK), BF16), vm((2, d_model, F_BLOCK), BF16), vm((2, F_BLOCK, d_model), BF16),
        vm((d_model, n_tok), BF16), vm((n_tok, d_model), BF16), vm((d_model, n_tok), BF16),
        vm((n_tok, F_BLOCK), BF16), vm((n_tok, F_BLOCK), BF16), vm((n_tok, d_model), F32),
        *[vm((IN_SLOTS, T_CHUNK, d_model), BF16)] * 4,
        vm((d_model, F_BLOCK), F32), vm((half_d, F_BLOCK), BF16), vm((d_model, F_BLOCK), F32), vm((d_model, F_BLOCK), BF16),
        pltpu.SemaphoreType.DMA((3, 2)),
        pltpu.SemaphoreType.DMA((4, IN_SLOTS)), pltpu.SemaphoreType.DMA((4,)), pltpu.SemaphoreType.DMA((2,)),
        pltpu.SemaphoreType.DMA((n_early,)), pltpu.SemaphoreType.DMA((n_early,)),
        pltpu.SemaphoreType.DMA((4,)), pltpu.SemaphoreType.DMA((4,)),
        pltpu.SemaphoreType.DMA((5,)), pltpu.SemaphoreType.DMA((5,)),
    ]
    n_dots = 4 * n_early + 3 * n_ex
    return pl.pallas_call(
        functools.partial(stack_kernel, n_layers, n_ex, n_steps),
        out_shape=outs,
        grid_spec=pltpu.PrefetchScalarGridSpec(
            num_scalar_prefetch=0, grid=(n_early + n_ex, n_steps), in_specs=[pl.BlockSpec(memory_space=ANY)] * 5, out_specs=out_specs, scratch_shapes=scratch),
        compiler_params=pltpu.CompilerParams(
            dimension_semantics=('arbitrary', 'arbitrary'), vmem_limit_bytes=VMEM_LIMIT, has_side_effects=True),
        cost_estimate=pl.CostEstimate(
            flops=2 * n_dots * n_tok * d_model * d_ff, bytes_accessed=500_000_000, transcendentals=2 * n_tok * d_ff),
        name='stack',
    )(pre_act, w_in, w_out, block_in, d_out)


def norm_kernel(sq_ref, out_ref):
    for d in range(out_ref.shape[0]):
        for ex in range(out_ref.shape[1]):
            out_ref[d, ex] = jnp.sum(sq_ref[2 * d, ex] + sq_ref[2 * d + 1, ex])


def chip_norms(squares):
    return pl.pallas_call(
        norm_kernel,
        out_shape=jax.ShapeDtypeStruct((3, squares.shape[1]), F32),
        in_specs=[pl.BlockSpec(memory_space=pltpu.VMEM)],
        out_specs=pl.BlockSpec(memory_space=pltpu.SMEM),
        name='norms',
    )(squares)


def mix_kernel(factors, sc_ref, clip_ref, *refs):
    def group(r, carry):
        rows = pl.ds(pl.multiple_of(r * MIX_ROWS, MIX_ROWS), MIX_ROWS)
        total = None
        for at, ref in zip(factors, refs):
            value = ref[0, rows, :].astype(F32)
            if at is not None:
                value = value * clip_ref[at[0], at[1]]
            total = value if total is None else total + value
        refs[-1][rows, :] = total.astype(BF16)
        return carry

    lax.fori_loop(0, refs[-1].shape[0] // MIX_ROWS, group, 0)


def mix(which, shape, terms, clip, before, part, n_parts):
    rows, width = shape
    part_width = width // n_parts
    block = (rows, width // 4) if which == 0 else (rows // 4, part_width)
    n_blocks = 4 // n_parts if which == 0 else 4

    def spec(k, v, lead):
        off = part * n_blocks if which == 0 and v.shape[2] > part_width else 0
        if which == 0:
            return pl.BlockSpec((1, *block), lambda i, sc: (lead, sc[k], i + off))
        return pl.BlockSpec((1, *block), lambda i, sc: (lead, i, sc[k]))

    def place(v, p):
        return p * n_parts + part if which == 1 and v.shape[2] > part_width else p

    out_map = (lambda i, sc: (0, i)) if which == 0 else (lambda i, sc: (i, 0))
    places = jnp.stack([jnp.asarray(place(v, p), jnp.int32) for v, _, p, _ in terms])
    if before is not None:
        places, _ = lax.optimization_barrier((places, before))
    return pl.pallas_call(
        functools.partial(mix_kernel, [at for _, _, _, at in terms]),
        out_shape=jax.ShapeDtypeStruct((rows, part_width), BF16),
        grid_spec=pltpu.PrefetchScalarGridSpec(
            num_scalar_prefetch=1, grid=(n_blocks,),
            in_specs=[pl.BlockSpec(memory_space=pltpu.SMEM)] + [spec(k, v, lead) for k, (v, lead, _, _) in enumerate(terms)],
            out_specs=pl.BlockSpec(block, out_map)),
        compiler_params=pltpu.CompilerParams(dimension_semantics=('arbitrary',), vmem_limit_bytes=40_000_000),
        cost_estimate=pl.CostEstimate(
            flops=2 * len(terms) * rows * part_width, bytes_accessed=14 * rows * part_width, transcendentals=0),
        name='mix',
    )(places, clip, *[v for v, _, _, _ in terms])


def put_in_kernel(sc_ref, coef_ref, piece_ref, noise_ref, *rest):
    out_ref = rest[-1]

    def group(r, carry):
        rows = pl.ds(pl.multiple_of(r * 16, 16), 16)
        out_ref[0, 0, rows, :] = (piece_ref[rows, :].astype(F32) + coef_ref[0] * noise_ref[0, 0, rows, :]) * coef_ref[1]
        return carry

    lax.fori_loop(0, piece_ref.shape[0] // 16, group, 0)


def put_out_kernel(sc_ref, coef_ref, piece_ref, noise_ref, *rest):
    out_ref = rest[-1]

    def group(r, carry):
        at = pl.ds(pl.multiple_of(r * 128, 128), 128)
        out_ref[0, 0, :, at] = (piece_ref[at, :].astype(F32).T + coef_ref[0] * noise_ref[0, 0, :, at]) * coef_ref[1]
        return carry

    lax.fori_loop(0, piece_ref.shape[0] // 128, group, 0, unroll=piece_ref.shape[1] == 128)


def put_piece(transposed, total, layer, quarter, part, coef, piece, noise):
    if transposed:
        rows, width = piece.shape[1], piece.shape[0]
        block = 256 if rows % 256 == 0 else 128
        first = part * (rows // block)
        piece_spec = pl.BlockSpec((width, block), lambda i, sc: (0, i))
        big_spec = pl.BlockSpec((1, 1, block, width), lambda i, sc: (sc[0], sc[1], first + i, 0))
    else:
        rows, width = piece.shape
        block = rows // 2
        piece_spec = pl.BlockSpec((block, width), lambda i, sc: (i, 0))
        big_spec = pl.BlockSpec((1, 1, block, width), lambda i, sc: (sc[0], sc[1], i, part))
    args = [jnp.stack([jnp.int32(layer), quarter]), coef, piece, noise]
    in_specs = [pl.BlockSpec(memory_space=pltpu.SMEM), piece_spec, big_spec]
    aliases = {}
    if total is not None:
        args.append(total)
        in_specs.append(pl.BlockSpec(memory_space=ANY))
        aliases = {4: 0}
    return pl.pallas_call(
        put_out_kernel if transposed else put_in_kernel,
        out_shape=jax.ShapeDtypeStruct(noise.shape, F32),
        grid_spec=pltpu.PrefetchScalarGridSpec(
            num_scalar_prefetch=1, grid=(rows // block,), in_specs=in_specs, out_specs=big_spec),
        input_output_aliases=aliases,
        compiler_params=pltpu.CompilerParams(dimension_semantics=('arbitrary',), vmem_limit_bytes=40_000_000),
        cost_estimate=pl.CostEstimate(flops=4 * rows * width, bytes_accessed=10 * rows * width, transcendentals=0),
        name='put_out' if transposed else 'put_in',
    )(*args)


def solution(mesh):
    data_size = mesh.shape['dp']
    swap_x = [(i, i ^ 1) for i in range(data_size)]
    swap_y = [(i, i ^ 2) for i in range(data_size)]

    def local_step(block_in, pre_act, w_in, w_out, d_out, noise_in, noise_out, clip_norm, noise_mult):
        n_layers, local_batch, _, d_model = block_in.shape
        d_ff = pre_act.shape[3]
        batch_total = local_batch * data_size
        dp = lax.axis_index('dp')
        x_pos, y_pos = lax.rem(dp, 2), dp // 2
        over_x = lambda v: lax.ppermute(v, 'dp', swap_x)
        over_y = lambda v: lax.ppermute(v, 'dp', swap_y)
        res = run_stack(pre_act, w_in, w_out, block_in, d_out)
        g1k, _, g1r, g2k, _, g2r, g1l, g2l, _, g1er, _, g2er, squares = res[3:]
        clip = jnp.minimum(1.0, clip_norm / jnp.sqrt(chip_norms(squares)))
        coef = jnp.stack([noise_mult * clip_norm, jnp.float32(1.0 / batch_total)])

        noise_in4 = noise_in.reshape(n_layers, 4, d_model // 4, d_ff)
        noise_out4 = noise_out.reshape(n_layers, 4, d_ff // 4, d_model)

        shapes = ((d_model // 4, d_ff), (d_model, d_ff // 4))
        at_half, at_side = (x_pos, y_pos), (y_pos, x_pos)
        over_half, over_side = (over_x, over_y), (over_y, over_x)
        early, early_far, late = (g1k, g2k), (g1r, g2r), (g1l, g2l)

        def own_terms(layer, which, half_pos, pos):
            if layer == 0:
                return [(late[which], k, 2 * half_pos + pos, (0, k)) for k in range(local_batch)]
            first = (n_layers - 1 - layer) * local_batch
            return [(early[which], first + k, pos, (0, k)) for k in range(local_batch)]

        made = []

        def mixed(which, terms, part, n_parts):
            made.append(mix(which, shapes[which], terms, clip, made[-1] if made else None, part, n_parts))
            return made[-1]

        def pair_terms(layer, which, part, to_send, *more):
            pos = 1 - at_side[which] if to_send else at_side[which]
            terms = own_terms(layer, which, at_half[which], pos)
            if layer == 0 and not to_send:
                more = (far_last[part, which], *more)
            elif layer == 0:
                terms += [((g1er, g2er)[which], k, 0, (1 + which, k)) for k in range(local_batch)]
            else:
                first = (n_layers - 1 - layer) * local_batch
                terms += [(early_far[which], first + k, pos, (1 + which, k)) for k in range(local_batch)]
            return terms + [(v[None], 0, 0, None) for v in more]

        last = [(0, part, 2) for part in range(2)]
        turns = [(layer, 0, 1) for layer in range(n_layers - 1, 0, -1)] + last
        got, far_last, places = {}, {}, {}
        for _, part, n_parts in last:
            for which in (1, 0):
                terms = own_terms(0, which, 1 - at_half[which], at_side[which])
                far_last[part, which] = over_half[which](mixed(which, terms, part, n_parts))
        for layer, part, n_parts in turns:
            for which in (1, 0):
                value = mixed(which, pair_terms(layer, which, part, True), part, n_parts)
                got[layer, part, which] = over_side[which](value)
        n_first = len(made)
        for layer, part, n_parts in turns:
            for which in (1, 0):
                half_pos, pos = at_half[which], at_side[which]
                own = mixed(which, pair_terms(layer, which, part, False, got[layer, part, which]), part, n_parts)
                near = over_side[which](own)
                side = over_half[which](own)
                diag = over_half[which](near)
                places[layer, part, which] = (
                    (2 * half_pos + pos, own), (2 * half_pos + 1 - pos, near),
                    (2 * (1 - half_pos) + pos, side), (2 * (1 - half_pos) + 1 - pos, diag))
        order = [(turn, which, 0) for turn in turns for which in (1, 0)]
        order += [(turn, which, kind) for turn in turns for kind in (1, 2) for which in (1, 0)]
        order += [(turn, which, 3) for turn in turns for which in (1, 0)]
        grads, noises = [None, None], (noise_in4, noise_out4)
        for (layer, part, _), which, kind in order:
            at, piece = places[layer, part, which][kind]
            grads[which] = put_piece(which == 1, grads[which], layer, at, part, coef, piece, noises[which])
        grad_in, grad_out = grads
        assert (len(made), n_first, len(order)) == (N_SUM, N_FIRST, N_PUT)
        return grad_in.reshape(n_layers, d_model, d_ff), grad_out.reshape(n_layers, d_ff, d_model)

    return jax.shard_map(
        local_step,
        mesh=mesh,
        in_specs=(P(None, 'dp', None, None), P(None, 'dp', None, 'tp'), P(None, None, 'tp'), P(None, 'tp', None),
                  P('dp', None, None), P(None, None, 'tp'), P(None, 'tp', None), P(), P()),
        out_specs=(P(None, None, 'tp'), P(None, 'tp', None)),
        check_vma=False,
    )
```

```python
import functools

import jax
import jax.numpy as jnp
from jax import lax
from jax.experimental import pallas as pl
from jax.experimental.pallas import tpu as pltpu
from jax.sharding import PartitionSpec as P


INV_SQRT2 = 0.7071067811865476
INV_SQRT_2PI = 0.3989422804014327
LOG2_E = 1.4426950408889634
F_BLOCK = 512
T_CHUNK = 256
IN_SLOTS = 4
LOAD_CHUNKS = 2
MIX_ROWS = 32
N_SUM, N_FIRST, N_PUT = 20, 12, 32
VMEM_LIMIT = 67_000_000

F32 = jnp.float32
BF16 = jnp.bfloat16
ANY = pl.ANY
MESH = pl.DeviceIdType.MESH


def dot_nn(a, b):
    return lax.dot_general(a, b, (((1,), (0,)), ((), ())), preferred_element_type=F32)


def dot_nt(a, b):
    return lax.dot_general(a, b, (((1,), (1,)), ((), ())), preferred_element_type=F32)


def block_at(j, n_half, x_pos, y_pos):
    far = n_half * (1 - y_pos) + x_pos * j + (1 - x_pos) * (n_half - 1 - j)
    own = n_half * y_pos + j - n_half
    is_far = 1 - j // n_half
    return is_far * far + (1 - is_far) * own


def stack_kernel(n_layers, n_ex, n_steps, u_hbm, w1_hbm, w2_hbm, x_hbm, dout_hbm,
                 p_hbm, q_hbm, dzo_hbm, g1k_hbm, g1s_hbm, g1r_hbm, g2k_hbm, g2s_hbm, g2r_hbm,
                 g1l_hbm, g2l_hbm, g1e_hbm, g1er_hbm, g2e_hbm, g2er_hbm, ss_hbm, ss_ref,
                 u_buf, w1_buf, w2_buf, x_t, dz, dz_t, dh, h, acc, x_st, z_st, p_st, q_st, g1_st, g1s_st, g2_st, g2s_st,
                 block_sem, in_sem, out_sem, io_sem, tp_send, tp_recv, far_send, far_recv, ss_send, ss_recv):
    task, step = pl.program_id(0), pl.program_id(1)
    n_early = (n_layers - 1) * n_ex
    n_task = n_early + n_ex
    dp = lax.axis_index('dp')
    x_pos, y_pos = lax.rem(dp, 2), dp // 2
    x_far = {'dp': dp + 1 - 2 * x_pos}
    y_far = {'dp': dp + 2 - 4 * y_pos}
    tp_far = {'tp': 1 - lax.axis_index('tp')}
    n_tok, d_model = dz.shape
    half_d, quarter_d = d_model // 2, d_model // 4
    n_half = n_steps // 2
    half_b = F_BLOCK // 2
    n_t = n_tok // T_CHUNK
    example = lax.rem(task, n_ex)
    cols = lambda k: pl.ds(pl.multiple_of(k * F_BLOCK, F_BLOCK), F_BLOCK)
    chunk = lambda c: pl.ds(c * T_CHUNK if isinstance(c, int) else pl.multiple_of(c * T_CHUNK, T_CHUNK), T_CHUNK)

    def fetch(act, t, j, slot):
        layer, at = n_layers - 1 - t // n_ex, cols(block_at(j, n_half, x_pos, y_pos))

        def one(k, src, dst):
            getattr(pltpu.make_async_copy(src, dst.at[slot], block_sem.at[k, slot]), act)()

        one(0, u_hbm.at[layer, lax.rem(t, n_ex), :, at], u_buf)
        one(1, w2_hbm.at[layer, at, :], w2_buf)
        pl.when(t < n_early)(lambda: one(2, w1_hbm.at[layer, :, at], w1_buf))

    ends = (step + 1) // n_steps
    now = lax.rem(task * n_steps + step, 2)

    def rarely(cond, body, n=1):
        def trip(i, carry):
            body(i)
            return carry

        lax.fori_loop(0, jnp.where(cond, n, 0), trip, 0)

    is_first = (task == 0) & (step == 0)
    rarely(is_first, lambda i: fetch('start', task, step, now))

    def in_start(t, c):
        slot, rows, ex = lax.rem(c, IN_SLOTS), chunk(c), lax.rem(t, n_ex)
        copy = lambda k, src, dst: pltpu.make_async_copy(src, dst.at[slot], in_sem.at[k, slot]).start()
        copy(0, x_hbm.at[n_layers - 1 - t // n_ex, ex, rows, :], x_st)

        @pl.when(t < n_early)
        def _():
            copy(1, dout_hbm.at[ex, rows, :], z_st)

        @pl.when(t >= n_early)
        def _():
            copy(1, dzo_hbm.at[ex, rows, :], z_st)

        @pl.when(t >= n_ex)
        def _():
            copy(2, p_hbm.at[t - n_ex, rows, :], p_st)
            copy(3, q_hbm.at[t - n_ex, rows, :], q_st)

    def in_wait(c):
        slot, rows = lax.rem(c, IN_SLOTS), chunk(c)
        wait = lambda k, dst: pltpu.make_async_copy(dout_hbm.at[0, rows, :], dst.at[slot], in_sem.at[k, slot]).wait()
        wait(0, x_st)
        wait(1, z_st)

        @pl.when(task >= n_ex)
        def _():
            wait(2, p_st)
            wait(3, q_st)

    def tp_copy(t):
        return pltpu.make_async_remote_copy(
            src_ref=p_hbm.at[t], dst_ref=q_hbm.at[t], send_sem=tp_send.at[t], recv_sem=tp_recv.at[t],
            device_id=tp_far, device_id_type=MESH)

    def front(load, to_dx):
        n_in = LOAD_CHUNKS if load and not to_dx else n_t

        def trip(i, carry):
            def dx_part(rows):
                part = dot_nt(dh[rows, :], w1_buf[now])
                acc[rows, :] = part if load else acc[rows, :] + part

            for s in range(n_in):
                c = i * n_in + s
                rows = chunk(c)
                if load:
                    @pl.when((c > 0) & (c + IN_SLOTS - 1 < n_t))
                    def _():
                        in_start(task, c + IN_SLOTS - 1)

                    in_wait(c)
                    slot = lax.rem(c, IN_SLOTS)
                    z = z_st[slot]
                    moved = (z.astype(F32) + (p_st[slot].astype(F32) + q_st[slot].astype(F32))).astype(BF16)
                    z = jnp.where(task >= n_ex, moved, z) if to_dx else moved
                    dz[rows, :] = z
                    dz_t[:, rows] = z.T
                    x_t[:, rows] = x_st[slot].T
                u = u_buf[now, rows, :].astype(F32)
                t = u * INV_SQRT2
                cdf = 0.5 * lax.erf(t) + 0.5
                h[rows, :] = (u * cdf).astype(BF16)
                slope = cdf + (t * (INV_SQRT_2PI / INV_SQRT2)) * jnp.exp2((t * t) * -LOG2_E)
                dh[rows, :] = (slope * dot_nt(dz[rows, :], w2_buf[now])).astype(BF16)
                if to_dx and s:
                    dx_part(chunk(c - 1))
            if to_dx:
                dx_part(chunk(i * n_in + n_in - 1))
            return carry

        if n_in == n_t:
            trip(0, 0)
        else:
            lax.fori_loop(0, n_t // n_in, trip, 0)

    def begin(c):
        ss_ref[...] = jnp.zeros_like(ss_ref)
        in_start(task, c)

    rarely(is_first, begin, IN_SLOTS)

    fetch('wait', task, step, now)
    for load in (True, False):
        for to_dx in (True, False):
            @pl.when(((step == 0) if load else (step > 0)) & ((task < n_early) if to_dx else (task >= n_early)))
            def _():
                front(load, to_dx)

    dz_keep = pltpu.make_async_copy(dz, dzo_hbm.at[example], io_sem.at[0])
    is_mid = (task >= n_ex) & (task < n_early)
    pl.when(is_mid & (step == 0))(dz_keep.start)
    ends_early = (step == n_steps - 1) & (task < n_early)
    dx_out = pltpu.make_async_copy(dz, p_hbm.at[task], io_sem.at[1])

    @pl.when(ends_early)
    def _():
        pl.when(is_mid)(dz_keep.wait)

        def put(c, carry):
            dz[chunk(c), :] = acc[chunk(c), :].astype(BF16)
            return carry

        lax.fori_loop(0, n_t, put, 0)
        dx_out.start()

    ends_task = (step == n_steps - 1) & (task < n_task - 1)
    rarely(ends_task & (task + 1 >= n_ex), lambda i: tp_copy(task + 1 - n_ex).wait())
    rarely(ends_task, lambda c: in_start(task + 1, c), IN_SLOTS)
    pl.when(task + ends < n_task)(lambda: fetch('start', task + ends, step + 1 - n_steps * ends, 1 - now))

    def far_copy(axis, src, dst):
        return pltpu.make_async_remote_copy(
            src_ref=src, dst_ref=dst, send_sem=far_send.at[axis], recv_sem=far_recv.at[axis],
            device_id=y_far if axis % 2 else x_far, device_id_type=MESH)

    own_rows = pl.ds(pl.multiple_of(x_pos * half_d, 16), half_d)
    pass_rows = pl.ds(pl.multiple_of((1 - y_pos) * quarter_d, 16), quarter_d)
    cut_half = pl.ds(pl.multiple_of((1 - x_pos) * half_b, half_b), half_b)
    to_half = pl.ds(pl.multiple_of(x_pos * F_BLOCK, half_b), half_b)
    to_full = pl.ds(pl.multiple_of((1 - x_pos) * half_b, half_b), F_BLOCK)

    def block(act, t, j):
        far_k = x_pos * j + (1 - x_pos) * (n_half - 1 - j)
        far_at, own_at = cols(far_k), cols(j - n_half)
        fb_at = cols(block_at(j, n_half, x_pos, y_pos))

        def local(n, src, dst):
            cp = pltpu.make_async_copy(src, dst, out_sem.at[n])
            (cp.start if act == 'start' else cp.wait)()

        def far(axis, src, dst):
            if act == 'end':
                far_copy(axis, src, dst).start()

        @pl.when(t < n_early)
        def _():
            local(0, g1_st.at[own_rows, :], g1k_hbm.at[t, :, fb_at])
            local(1, g1s_st, g1s_hbm.at[t, :, fb_at])
            far(0, g1s_hbm.at[t, :, fb_at], g1r_hbm.at[t, :, fb_at])

            @pl.when(j < n_half)
            def _():
                local(2, g2s_st, g2s_hbm.at[t, :, far_at])
                far(1, g2s_hbm.at[t, :, far_at], g2r_hbm.at[t, :, far_at])

            @pl.when(j >= n_half)
            def _():
                local(3, g2_st, g2k_hbm.at[t, :, own_at])

        @pl.when(t >= n_early)
        def _():
            ex = t - n_early
            local(1, g1s_st.at[pass_rows, :], g1e_hbm.at[ex, :, fb_at])
            pl.when((t < n_task - 1) | (j < n_steps - 1))(lambda: far(2, g1e_hbm.at[ex, :, fb_at], g1er_hbm.at[ex, :, fb_at]))
            local(0, g1_st, g1l_hbm.at[ex, :, fb_at])
            local(3, g2_st, g2l_hbm.at[ex, :, fb_at])

            @pl.when(j == 0)
            def _():
                local(2, g2s_st, g2e_hbm.at[ex, :, to_full])
                far(3, g2e_hbm.at[ex, :, to_full], g2er_hbm.at[ex, :, to_full])

            @pl.when(j == 1)
            def _():
                local(2, g2s_st.at[:, cut_half], g2e_hbm.at[ex, :, to_half])
                far(3, g2e_hbm.at[ex, :, to_half], g2er_hbm.at[ex, :, to_half])

    @pl.when((task > 0) | (step > 0))
    def _():
        block('end', jnp.where(step > 0, task, task - 1), jnp.where(step > 0, step - 1, n_steps - 1))

    def square(g):
        return jnp.sum((g * g).reshape(g.shape[0] // 8, 8, g.shape[1]), axis=0)

    total = ss_ref[example]
    for r in range(2):
        part = pl.ds(r * quarter_d, quarter_d)
        own = pl.ds(pl.multiple_of(r * quarter_d + x_pos * half_d, 16), quarter_d)
        far = pl.ds(pl.multiple_of(r * quarter_d + (1 - x_pos) * half_d, 16), quarter_d)
        g = dot_nn(x_t[own, :], dh[...])
        g1_st[own, :] = g
        total = total + square(g)
        g = dot_nn(x_t[far, :], dh[...])
        g1_st[far, :] = g
        g1s_st[part, :] = g.astype(BF16)
        total = total + square(g)
        for at in (part, pl.ds(r * quarter_d + half_d, quarter_d)):
            g = dot_nn(dz_t[at, :], h[...])
            g2_st[at, :] = g
            g2s_st[at, :] = g.astype(BF16)
            total = total + square(g)
    ss_ref[example] = total
    block('start', task, step)
    ends_all = (step == n_steps - 1) & (task == n_task - 1)

    def last_far(i):
        at = cols(block_at(step, n_half, x_pos, y_pos))
        far_copy(2, g1s_st.at[pass_rows, :], g1er_hbm.at[n_ex - 1, :, at]).start()

    rarely(ends_all, last_far)

    @pl.when(ends_early)
    def _():
        dx_out.wait()
        tp_copy(task).start()

    def finish(i):
        keep = pltpu.make_async_copy(ss_ref, ss_hbm.at[0], io_sem.at[0])
        keep.start()
        keep.wait()
        tp = lax.axis_index('tp')
        peers = [
            {'dp': dp, 'tp': 1 - tp}, {**x_far, 'tp': tp}, {**x_far, 'tp': 1 - tp}, {**y_far, 'tp': tp}, {**y_far, 'tp': 1 - tp}]
        sums = [
            pltpu.make_async_remote_copy(
                src_ref=ss_hbm.at[0], dst_ref=ss_hbm.at[k + 1], send_sem=ss_send.at[k], recv_sem=ss_recv.at[k],
                device_id=peer, device_id_type=MESH)
            for k, peer in enumerate(peers)]
        for cp in sums:
            cp.start()
        block('end', task, step)
        for cp in sums:
            cp.wait()
        far_copy(0, g1s_hbm, g1r_hbm).wait()
        far_copy(1, g2s_hbm, g2r_hbm).wait()
        far_copy(2, g1e_hbm, g1er_hbm).wait()
        far_copy(3, g2e_hbm, g2er_hbm).wait()

    rarely(ends_all, finish)


def run_stack(pre_act, w_in, w_out, block_in, d_out):
    n_layers, n_ex, n_tok, d_model = block_in.shape
    d_ff = pre_act.shape[3]
    n_steps = d_ff // F_BLOCK
    half_d, half_f = d_model // 2, d_ff // 2
    n_early = (n_layers - 1) * n_ex
    sds = jax.ShapeDtypeStruct
    outs = [
        sds((n_early, n_tok, d_model), BF16), sds((n_early, n_tok, d_model), BF16), sds((n_ex, n_tok, d_model), BF16),
        sds((n_early, half_d, d_ff), F32), sds((n_early, half_d, d_ff), BF16), sds((n_early, half_d, d_ff), BF16),
        sds((n_early, d_model, half_f), F32), sds((n_early, d_model, half_f), BF16), sds((n_early, d_model, half_f), BF16),
        sds((n_ex, d_model, d_ff), F32), sds((n_ex, d_model, d_ff), F32),
        sds((n_ex, d_model // 4, d_ff), BF16), sds((n_ex, d_model // 4, d_ff), BF16),
        sds((n_ex, d_model, d_ff // 4), BF16), sds((n_ex, d_model, d_ff // 4), BF16),
        sds((6, n_ex, 8, F_BLOCK), F32),
    ]
    out_specs = [pl.BlockSpec(memory_space=ANY)] * len(outs)
    vm = pltpu.VMEM
    scratch = [
        vm((n_ex, 8, F_BLOCK), F32),
        vm((2, n_tok, F_BLOCK), BF16), vm((2, d_model, F_BLOCK), BF16), vm((2, F_BLOCK, d_model), BF16),
        vm((d_model, n_tok), BF16), vm((n_tok, d_model), BF16), vm((d_model, n_tok), BF16),
        vm((n_tok, F_BLOCK), BF16), vm((n_tok, F_BLOCK), BF16), vm((n_tok, d_model), F32),
        *[vm((IN_SLOTS, T_CHUNK, d_model), BF16)] * 4,
        vm((d_model, F_BLOCK), F32), vm((half_d, F_BLOCK), BF16), vm((d_model, F_BLOCK), F32), vm((d_model, F_BLOCK), BF16),
        pltpu.SemaphoreType.DMA((3, 2)),
        pltpu.SemaphoreType.DMA((4, IN_SLOTS)), pltpu.SemaphoreType.DMA((4,)), pltpu.SemaphoreType.DMA((2,)),
        pltpu.SemaphoreType.DMA((n_early,)), pltpu.SemaphoreType.DMA((n_early,)),
        pltpu.SemaphoreType.DMA((4,)), pltpu.SemaphoreType.DMA((4,)),
        pltpu.SemaphoreType.DMA((5,)), pltpu.SemaphoreType.DMA((5,)),
    ]
    n_dots = 4 * n_early + 3 * n_ex
    return pl.pallas_call(
        functools.partial(stack_kernel, n_layers, n_ex, n_steps),
        out_shape=outs,
        grid_spec=pltpu.PrefetchScalarGridSpec(
            num_scalar_prefetch=0, grid=(n_early + n_ex, n_steps), in_specs=[pl.BlockSpec(memory_space=ANY)] * 5, out_specs=out_specs, scratch_shapes=scratch),
        compiler_params=pltpu.CompilerParams(
            dimension_semantics=('arbitrary', 'arbitrary'), vmem_limit_bytes=VMEM_LIMIT, has_side_effects=True),
        cost_estimate=pl.CostEstimate(
            flops=2 * n_dots * n_tok * d_model * d_ff, bytes_accessed=500_000_000, transcendentals=2 * n_tok * d_ff),
        name='stack',
    )(pre_act, w_in, w_out, block_in, d_out)


def norm_kernel(sq_ref, out_ref):
    for d in range(out_ref.shape[0]):
        for ex in range(out_ref.shape[1]):
            out_ref[d, ex] = jnp.sum(sq_ref[2 * d, ex] + sq_ref[2 * d + 1, ex])


def chip_norms(squares):
    return pl.pallas_call(
        norm_kernel,
        out_shape=jax.ShapeDtypeStruct((3, squares.shape[1]), F32),
        in_specs=[pl.BlockSpec(memory_space=pltpu.VMEM)],
        out_specs=pl.BlockSpec(memory_space=pltpu.SMEM),
        name='norms',
    )(squares)


def mix_kernel(factors, sc_ref, clip_ref, *refs):
    def group(r, carry):
        rows = pl.ds(pl.multiple_of(r * MIX_ROWS, MIX_ROWS), MIX_ROWS)
        total = None
        for at, ref in zip(factors, refs):
            value = ref[0, rows, :].astype(F32)
            if at is not None:
                value = value * clip_ref[at[0], at[1]]
            total = value if total is None else total + value
        refs[-1][rows, :] = total.astype(BF16)
        return carry

    lax.fori_loop(0, refs[-1].shape[0] // MIX_ROWS, group, 0)


def mix(which, shape, terms, clip, before, part, n_parts):
    rows, width = shape
    part_width = width // n_parts
    block = (rows, width // 4) if which == 0 else (rows // 4, part_width)
    n_blocks = 4 // n_parts if which == 0 else 4

    def spec(k, v, lead):
        off = part * n_blocks if which == 0 and v.shape[2] > part_width else 0
        if which == 0:
            return pl.BlockSpec((1, *block), lambda i, sc: (lead, sc[k], i + off))
        return pl.BlockSpec((1, *block), lambda i, sc: (lead, i, sc[k]))

    def place(v, p):
        return p * n_parts + part if which == 1 and v.shape[2] > part_width else p

    out_map = (lambda i, sc: (0, i)) if which == 0 else (lambda i, sc: (i, 0))
    places = jnp.stack([jnp.asarray(place(v, p), jnp.int32) for v, _, p, _ in terms])
    if before is not None:
        places, _ = lax.optimization_barrier((places, before))
    return pl.pallas_call(
        functools.partial(mix_kernel, [at for _, _, _, at in terms]),
        out_shape=jax.ShapeDtypeStruct((rows, part_width), BF16),
        grid_spec=pltpu.PrefetchScalarGridSpec(
            num_scalar_prefetch=1, grid=(n_blocks,),
            in_specs=[pl.BlockSpec(memory_space=pltpu.SMEM)] + [spec(k, v, lead) for k, (v, lead, _, _) in enumerate(terms)],
            out_specs=pl.BlockSpec(block, out_map)),
        compiler_params=pltpu.CompilerParams(dimension_semantics=('arbitrary',), vmem_limit_bytes=40_000_000),
        cost_estimate=pl.CostEstimate(
            flops=2 * len(terms) * rows * part_width, bytes_accessed=14 * rows * part_width, transcendentals=0),
        name='mix',
    )(places, clip, *[v for v, _, _, _ in terms])


def put_in_kernel(sc_ref, coef_ref, piece_ref, noise_ref, *rest):
    out_ref = rest[-1]

    def group(r, carry):
        rows = pl.ds(pl.multiple_of(r * 16, 16), 16)
        out_ref[0, 0, rows, :] = (piece_ref[rows, :].astype(F32) + coef_ref[0] * noise_ref[0, 0, rows, :]) * coef_ref[1]
        return carry

    lax.fori_loop(0, piece_ref.shape[0] // 16, group, 0)


def put_out_kernel(sc_ref, coef_ref, piece_ref, noise_ref, *rest):
    out_ref = rest[-1]

    def group(r, carry):
        at = pl.ds(pl.multiple_of(r * 128, 128), 128)
        out_ref[0, 0, :, at] = (piece_ref[at, :].astype(F32).T + coef_ref[0] * noise_ref[0, 0, :, at]) * coef_ref[1]
        return carry

    lax.fori_loop(0, piece_ref.shape[0] // 128, group, 0, unroll=piece_ref.shape[1] == 128)


def put_piece(transposed, total, layer, quarter, part, coef, piece, noise):
    if transposed:
        rows, width = piece.shape[1], piece.shape[0]
        block = 256 if rows % 256 == 0 else 128
        first = part * (rows // block)
        piece_spec = pl.BlockSpec((width, block), lambda i, sc: (0, i))
        big_spec = pl.BlockSpec((1, 1, block, width), lambda i, sc: (sc[0], sc[1], first + i, 0))
    else:
        rows, width = piece.shape
        block = rows // 2
        piece_spec = pl.BlockSpec((block, width), lambda i, sc: (i, 0))
        big_spec = pl.BlockSpec((1, 1, block, width), lambda i, sc: (sc[0], sc[1], i, part))
    args = [jnp.stack([jnp.int32(layer), quarter]), coef, piece, noise]
    in_specs = [pl.BlockSpec(memory_space=pltpu.SMEM), piece_spec, big_spec]
    aliases = {}
    if total is not None:
        args.append(total)
        in_specs.append(pl.BlockSpec(memory_space=ANY))
        aliases = {4: 0}
    return pl.pallas_call(
        put_out_kernel if transposed else put_in_kernel,
        out_shape=jax.ShapeDtypeStruct(noise.shape, F32),
        grid_spec=pltpu.PrefetchScalarGridSpec(
            num_scalar_prefetch=1, grid=(rows // block,), in_specs=in_specs, out_specs=big_spec),
        input_output_aliases=aliases,
        compiler_params=pltpu.CompilerParams(dimension_semantics=('arbitrary',), vmem_limit_bytes=40_000_000),
        cost_estimate=pl.CostEstimate(flops=4 * rows * width, bytes_accessed=10 * rows * width, transcendentals=0),
        name='put_out' if transposed else 'put_in',
    )(*args)


def solution(mesh):
    data_size = mesh.shape['dp']
    swap_x = [(i, i ^ 1) for i in range(data_size)]
    swap_y = [(i, i ^ 2) for i in range(data_size)]

    def local_step(block_in, pre_act, w_in, w_out, d_out, noise_in, noise_out, clip_norm, noise_mult):
        n_layers, local_batch, _, d_model = block_in.shape
        d_ff = pre_act.shape[3]
        batch_total = local_batch * data_size
        dp = lax.axis_index('dp')
        x_pos, y_pos = lax.rem(dp, 2), dp // 2
        over_x = lambda v: lax.ppermute(v, 'dp', swap_x)
        over_y = lambda v: lax.ppermute(v, 'dp', swap_y)
        res = run_stack(pre_act, w_in, w_out, block_in, d_out)
        g1k, _, g1r, g2k, _, g2r, g1l, g2l, _, g1er, _, g2er, squares = res[3:]
        clip = jnp.minimum(1.0, clip_norm / jnp.sqrt(chip_norms(squares)))
        coef = jnp.stack([noise_mult * clip_norm, jnp.float32(1.0 / batch_total)])

        noise_in4 = noise_in.reshape(n_layers, 4, d_model // 4, d_ff)
        noise_out4 = noise_out.reshape(n_layers, 4, d_ff // 4, d_model)

        shapes = ((d_model // 4, d_ff), (d_model, d_ff // 4))
        at_half, at_side = (x_pos, y_pos), (y_pos, x_pos)
        over_half, over_side = (over_x, over_y), (over_y, over_x)
        early, early_far, late = (g1k, g2k), (g1r, g2r), (g1l, g2l)

        def own_terms(layer, which, half_pos, pos):
            if layer == 0:
                return [(late[which], k, 2 * half_pos + pos, (0, k)) for k in range(local_batch)]
            first = (n_layers - 1 - layer) * local_batch
            return [(early[which], first + k, pos, (0, k)) for k in range(local_batch)]

        made = []

        def mixed(which, terms, part, n_parts):
            made.append(mix(which, shapes[which], terms, clip, made[-1] if made else None, part, n_parts))
            return made[-1]

        def pair_terms(layer, which, part, to_send, *more):
            pos = 1 - at_side[which] if to_send else at_side[which]
            terms = own_terms(layer, which, at_half[which], pos)
            if layer == 0 and not to_send:
                more = (far_last[part, which], *more)
            elif layer == 0:
                terms += [((g1er, g2er)[which], k, 0, (1 + which, k)) for k in range(local_batch)]
            else:
                first = (n_layers - 1 - layer) * local_batch
                terms += [(early_far[which], first + k, pos, (1 + which, k)) for k in range(local_batch)]
            return terms + [(v[None], 0, 0, None) for v in more]

        last = [(0, part, 2) for part in range(2)]
        turns = [(layer, 0, 1) for layer in range(n_layers - 1, 0, -1)] + last
        got, far_last, places = {}, {}, {}
        for _, part, n_parts in last:
            for which in (1, 0):
                terms = own_terms(0, which, 1 - at_half[which], at_side[which])
                far_last[part, which] = over_half[which](mixed(which, terms, part, n_parts))
        for layer, part, n_parts in turns:
            for which in (1, 0):
                value = mixed(which, pair_terms(layer, which, part, True), part, n_parts)
                got[layer, part, which] = over_side[which](value)
        n_first = len(made)
        for layer, part, n_parts in turns:
            for which in (1, 0):
                half_pos, pos = at_half[which], at_side[which]
                own = mixed(which, pair_terms(layer, which, part, False, got[layer, part, which]), part, n_parts)
                near = over_side[which](own)
                side = over_half[which](own)
                diag = over_half[which](near)
                places[layer, part, which] = (
                    (2 * half_pos + pos, own), (2 * half_pos + 1 - pos, near),
                    (2 * (1 - half_pos) + pos, side), (2 * (1 - half_pos) + 1 - pos, diag))
        order = [(turn, which, 0) for turn in turns for which in (1, 0)]
        order += [(turn, which, kind) for turn in turns for kind in (1, 2) for which in (1, 0)]
        order += [(turn, which, 3) for turn in turns for which in (1, 0)]
        grads, noises = [None, None], (noise_in4, noise_out4)
        for (layer, part, _), which, kind in order:
            at, piece = places[layer, part, which][kind]
            grads[which] = put_piece(which == 1, grads[which], layer, at, part, coef, piece, noises[which])
        grad_in, grad_out = grads
        assert (len(made), n_first, len(order)) == (N_SUM, N_FIRST, N_PUT)
        return grad_in.reshape(n_layers, d_model, d_ff), grad_out.reshape(n_layers, d_ff, d_model)

    return jax.shard_map(
        local_step,
        mesh=mesh,
        in_specs=(P(None, 'dp', None, None), P(None, 'dp', None, 'tp'), P(None, None, 'tp'), P(None, 'tp', None),
                  P('dp', None, None), P(None, None, 'tp'), P(None, 'tp', None), P(), P()),
        out_specs=(P(None, None, 'tp'), P(None, 'tp', None)),
        check_vma=False,
    )
```

```python
import functools

import jax
import jax.numpy as jnp
from jax import lax
from jax.experimental import pallas as pl
from jax.experimental.pallas import tpu as pltpu
from jax.sharding import PartitionSpec as P


INV_SQRT2 = 0.7071067811865476
INV_SQRT_2PI = 0.3989422804014327
LOG2_E = 1.4426950408889634
F32_MAX = 3.4028234663852886e38
F_BLOCK = 512
T_CHUNK = 256
IN_SLOTS = 4
LOAD_CHUNKS = 2
MIX_ROWS = 32
N_PARTS = 3
N_SUM, N_FIRST, N_PUT = 8 + 6 * N_PARTS, 4 + 4 * N_PARTS, 16 + 8 * N_PARTS
VMEM_LIMIT = 67_000_000

F32 = jnp.float32
BF16 = jnp.bfloat16
ANY = pl.ANY
MESH = pl.DeviceIdType.MESH


def dot_nn(a, b):
    return lax.dot_general(a, b, (((1,), (0,)), ((), ())), preferred_element_type=F32)


def dot_nt(a, b):
    return lax.dot_general(a, b, (((1,), (1,)), ((), ())), preferred_element_type=F32)


def block_at(j, n_half, x_pos, y_pos):
    far = n_half * (1 - y_pos) + x_pos * j + (1 - x_pos) * (n_half - 1 - j)
    own = n_half * y_pos + j - n_half
    is_far = 1 - j // n_half
    return is_far * far + (1 - is_far) * own


def stack_kernel(n_layers, n_ex, n_steps, u_hbm, w1_hbm, w2_hbm, x_hbm, dout_hbm,
                 p_hbm, q_hbm, dzo_hbm, g1k_hbm, g1s_hbm, g1r_hbm, g2k_hbm, g2s_hbm, g2r_hbm,
                 g1l_hbm, g2l_hbm, g1e_hbm, g1er_hbm, g2e_hbm, g2er_hbm, ss_hbm, ss_ref,
                 u_buf, w1_buf, w2_buf, x_t, dz, dz_t, dh, h, acc, x_st, z_st, p_st, q_st, g1_st, g1s_st, g2_st, g2s_st,
                 block_sem, in_sem, out_sem, io_sem, tp_send, tp_recv, far_send, far_recv, ss_send, ss_recv):
    task, step = pl.program_id(0), pl.program_id(1)
    n_early = (n_layers - 1) * n_ex
    n_task = n_early + n_ex
    dp = lax.axis_index('dp')
    x_pos, y_pos = lax.rem(dp, 2), dp // 2
    x_far = {'dp': dp + 1 - 2 * x_pos}
    y_far = {'dp': dp + 2 - 4 * y_pos}
    tp_far = {'tp': 1 - lax.axis_index('tp')}
    n_tok, d_model = dz.shape
    half_d, quarter_d = d_model // 2, d_model // 4
    n_half = n_steps // 2
    half_b = F_BLOCK // 2
    n_t = n_tok // T_CHUNK
    example = lax.rem(task, n_ex)
    cols = lambda k: pl.ds(pl.multiple_of(k * F_BLOCK, F_BLOCK), F_BLOCK)
    chunk = lambda c: pl.ds(c * T_CHUNK if isinstance(c, int) else pl.multiple_of(c * T_CHUNK, T_CHUNK), T_CHUNK)

    def fetch(act, t, j, slot):
        layer, at = n_layers - 1 - t // n_ex, cols(block_at(j, n_half, x_pos, y_pos))

        def one(k, src, dst):
            getattr(pltpu.make_async_copy(src, dst.at[slot], block_sem.at[k, slot]), act)()

        one(0, u_hbm.at[layer, lax.rem(t, n_ex), :, at], u_buf)
        one(1, w2_hbm.at[layer, at, :], w2_buf)
        pl.when(t < n_early)(lambda: one(2, w1_hbm.at[layer, :, at], w1_buf))

    ends = (step + 1) // n_steps
    now = lax.rem(task * n_steps + step, 2)

    def rarely(cond, body, n=1):
        def trip(i, carry):
            body(i)
            return carry

        lax.fori_loop(0, jnp.where(cond, n, 0), trip, 0)

    is_first = (task == 0) & (step == 0)
    rarely(is_first, lambda i: fetch('start', task, step, now))

    def in_start(t, c):
        slot, rows, ex = lax.rem(c, IN_SLOTS), chunk(c), lax.rem(t, n_ex)
        copy = lambda k, src, dst: pltpu.make_async_copy(src, dst.at[slot], in_sem.at[k, slot]).start()
        copy(0, x_hbm.at[n_layers - 1 - t // n_ex, ex, rows, :], x_st)

        @pl.when(t < n_early)
        def _():
            copy(1, dout_hbm.at[ex, rows, :], z_st)

        @pl.when(t >= n_early)
        def _():
            copy(1, dzo_hbm.at[ex, rows, :], z_st)

        @pl.when(t >= n_ex)
        def _():
            copy(2, p_hbm.at[t - n_ex, rows, :], p_st)
            copy(3, q_hbm.at[t - n_ex, rows, :], q_st)

    def in_wait(c):
        slot, rows = lax.rem(c, IN_SLOTS), chunk(c)
        wait = lambda k, dst: pltpu.make_async_copy(dout_hbm.at[0, rows, :], dst.at[slot], in_sem.at[k, slot]).wait()
        wait(0, x_st)
        wait(1, z_st)

        @pl.when(task >= n_ex)
        def _():
            wait(2, p_st)
            wait(3, q_st)

    def tp_copy(t):
        return pltpu.make_async_remote_copy(
            src_ref=p_hbm.at[t], dst_ref=q_hbm.at[t], send_sem=tp_send.at[t], recv_sem=tp_recv.at[t],
            device_id=tp_far, device_id_type=MESH)

    def front(load, to_dx):
        n_in = LOAD_CHUNKS if load and not to_dx else n_t

        def trip(i, carry):
            def dx_part(rows):
                part = dot_nt(dh[rows, :], w1_buf[now])
                acc[rows, :] = part if load else acc[rows, :] + part

            for s in range(n_in):
                c = i * n_in + s
                rows = chunk(c)
                if load:
                    @pl.when((c > 0) & (c + IN_SLOTS - 1 < n_t))
                    def _():
                        in_start(task, c + IN_SLOTS - 1)

                    in_wait(c)
                    slot = lax.rem(c, IN_SLOTS)
                    z = z_st[slot]
                    moved = (z.astype(F32) + (p_st[slot].astype(F32) + q_st[slot].astype(F32))).astype(BF16)
                    z = jnp.where(task >= n_ex, moved, z) if to_dx else moved
                    dz[rows, :] = z
                    dz_t[:, rows] = z.T
                    x_t[:, rows] = x_st[slot].T
                u = u_buf[now, rows, :].astype(F32)
                t = u * INV_SQRT2
                cdf = 0.5 * lax.erf(t) + 0.5
                h[rows, :] = (u * cdf).astype(BF16)
                slope = cdf + (t * (INV_SQRT_2PI / INV_SQRT2)) * jnp.exp2((t * t) * -LOG2_E)
                dh[rows, :] = (slope * dot_nt(dz[rows, :], w2_buf[now])).astype(BF16)
                if to_dx and s:
                    dx_part(chunk(c - 1))
            if to_dx:
                dx_part(chunk(i * n_in + n_in - 1))
            return carry

        if n_in == n_t:
            trip(0, 0)
        else:
            lax.fori_loop(0, n_t // n_in, trip, 0)

    def begin(c):
        ss_ref[...] = jnp.zeros_like(ss_ref)
        in_start(task, c)

    rarely(is_first, begin, IN_SLOTS)

    fetch('wait', task, step, now)
    for load in (True, False):
        for to_dx in (True, False):
            @pl.when(((step == 0) if load else (step > 0)) & ((task < n_early) if to_dx else (task >= n_early)))
            def _():
                front(load, to_dx)

    dz_keep = pltpu.make_async_copy(dz, dzo_hbm.at[example], io_sem.at[0])
    is_mid = (task >= n_ex) & (task < n_early)
    pl.when(is_mid & (step == 0))(dz_keep.start)
    ends_early = (step == n_steps - 1) & (task < n_early)
    dx_out = pltpu.make_async_copy(dz, p_hbm.at[task], io_sem.at[1])

    @pl.when(ends_early)
    def _():
        pl.when(is_mid)(dz_keep.wait)

        def put(c, carry):
            dz[chunk(c), :] = acc[chunk(c), :].astype(BF16)
            return carry

        lax.fori_loop(0, n_t, put, 0)

    pl.when(task + ends < n_task)(lambda: fetch('start', task + ends, step + 1 - n_steps * ends, 1 - now))
    ends_task = (step == n_steps - 1) & (task < n_task - 1)
    rarely(ends_task & (task + 1 >= n_ex), lambda i: tp_copy(task + 1 - n_ex).wait())
    rarely(ends_task, lambda c: in_start(task + 1, c), IN_SLOTS)
    pl.when(ends_early)(dx_out.start)

    def far_copy(axis, src, dst):
        return pltpu.make_async_remote_copy(
            src_ref=src, dst_ref=dst, send_sem=far_send.at[axis], recv_sem=far_recv.at[axis],
            device_id=y_far if axis % 2 else x_far, device_id_type=MESH)

    own_rows = pl.ds(pl.multiple_of(x_pos * half_d, 16), half_d)
    pass_rows = pl.ds(pl.multiple_of((1 - y_pos) * quarter_d, 16), quarter_d)
    cut_half = pl.ds(pl.multiple_of((1 - x_pos) * half_b, half_b), half_b)
    to_half = pl.ds(pl.multiple_of(x_pos * F_BLOCK, half_b), half_b)
    to_full = pl.ds(pl.multiple_of((1 - x_pos) * half_b, half_b), F_BLOCK)

    def block(act, t, j):
        far_k = x_pos * j + (1 - x_pos) * (n_half - 1 - j)
        far_at, own_at = cols(far_k), cols(j - n_half)
        fb_at = cols(block_at(j, n_half, x_pos, y_pos))

        def local(n, src, dst):
            cp = pltpu.make_async_copy(src, dst, out_sem.at[n])
            (cp.start if act == 'start' else cp.wait)()

        def far(axis, src, dst):
            if act == 'end':
                far_copy(axis, src, dst).start()

        @pl.when(t < n_early)
        def _():
            local(0, g1_st.at[own_rows, :], g1k_hbm.at[t, :, fb_at])
            local(1, g1s_st, g1s_hbm.at[t, :, fb_at])
            far(0, g1s_hbm.at[t, :, fb_at], g1r_hbm.at[t, :, fb_at])

            @pl.when(j < n_half)
            def _():
                local(2, g2s_st, g2s_hbm.at[t, :, far_at])
                far(1, g2s_hbm.at[t, :, far_at], g2r_hbm.at[t, :, far_at])

            @pl.when(j >= n_half)
            def _():
                local(3, g2_st, g2k_hbm.at[t, :, own_at])

        @pl.when(t >= n_early)
        def _():
            ex = t - n_early
            local(1, g1s_st.at[pass_rows, :], g1e_hbm.at[ex, :, fb_at])
            pl.when((t < n_task - 1) | (j < n_steps - 1))(lambda: far(2, g1e_hbm.at[ex, :, fb_at], g1er_hbm.at[ex, :, fb_at]))
            local(0, g1_st, g1l_hbm.at[ex, :, fb_at])
            local(3, g2_st, g2l_hbm.at[ex, :, fb_at])

            @pl.when(j == 0)
            def _():
                local(2, g2s_st, g2e_hbm.at[ex, :, to_full])
                far(3, g2e_hbm.at[ex, :, to_full], g2er_hbm.at[ex, :, to_full])

            @pl.when(j == 1)
            def _():
                local(2, g2s_st.at[:, cut_half], g2e_hbm.at[ex, :, to_half])
                far(3, g2e_hbm.at[ex, :, to_half], g2er_hbm.at[ex, :, to_half])

    @pl.when((task > 0) | (step > 0))
    def _():
        block('end', jnp.where(step > 0, task, task - 1), jnp.where(step > 0, step - 1, n_steps - 1))

    def square(g):
        return jnp.sum((g * g).reshape(g.shape[0] // 8, 8, g.shape[1]), axis=0)

    total = ss_ref[example]
    for r in range(2):
        part = pl.ds(r * quarter_d, quarter_d)
        own = pl.ds(pl.multiple_of(r * quarter_d + x_pos * half_d, 16), quarter_d)
        far = pl.ds(pl.multiple_of(r * quarter_d + (1 - x_pos) * half_d, 16), quarter_d)
        g = dot_nn(x_t[own, :], dh[...])
        g1_st[own, :] = g
        total = total + square(g)
        g = dot_nn(x_t[far, :], dh[...])
        g1_st[far, :] = g
        g1s_st[part, :] = g.astype(BF16)
        total = total + square(g)
        for at in (part, pl.ds(r * quarter_d + half_d, quarter_d)):
            g = dot_nn(dz_t[at, :], h[...])
            g2_st[at, :] = g
            g2s_st[at, :] = g.astype(BF16)
            total = total + square(g)
    ss_ref[example] = total
    block('start', task, step)
    ends_all = (step == n_steps - 1) & (task == n_task - 1)

    def last_far(i):
        at = cols(block_at(step, n_half, x_pos, y_pos))
        far_copy(2, g1s_st.at[pass_rows, :], g1er_hbm.at[n_ex - 1, :, at]).start()

    rarely(ends_all, last_far)

    @pl.when(ends_early)
    def _():
        dx_out.wait()
        tp_copy(task).start()

    def finish(i):
        keep = pltpu.make_async_copy(ss_ref, ss_hbm.at[0], io_sem.at[0])
        keep.start()
        keep.wait()
        tp = lax.axis_index('tp')
        peers = [
            {'dp': dp, 'tp': 1 - tp}, {**x_far, 'tp': tp}, {**x_far, 'tp': 1 - tp}, {**y_far, 'tp': tp}, {**y_far, 'tp': 1 - tp}]
        sums = [
            pltpu.make_async_remote_copy(
                src_ref=ss_hbm.at[0], dst_ref=ss_hbm.at[k + 1], send_sem=ss_send.at[k], recv_sem=ss_recv.at[k],
                device_id=peer, device_id_type=MESH)
            for k, peer in enumerate(peers)]
        for cp in sums:
            cp.start()
        block('end', task, step)
        for cp in sums:
            cp.wait()
        far_copy(0, g1s_hbm, g1r_hbm).wait()
        far_copy(1, g2s_hbm, g2r_hbm).wait()
        far_copy(2, g1e_hbm, g1er_hbm).wait()
        far_copy(3, g2e_hbm, g2er_hbm).wait()

    rarely(ends_all, finish)


def run_stack(pre_act, w_in, w_out, block_in, d_out):
    n_layers, n_ex, n_tok, d_model = block_in.shape
    d_ff = pre_act.shape[3]
    n_steps = d_ff // F_BLOCK
    half_d, half_f = d_model // 2, d_ff // 2
    n_early = (n_layers - 1) * n_ex
    sds = jax.ShapeDtypeStruct
    outs = [
        sds((n_early, n_tok, d_model), BF16), sds((n_early, n_tok, d_model), BF16), sds((n_ex, n_tok, d_model), BF16),
        sds((n_early, half_d, d_ff), F32), sds((n_early, half_d, d_ff), BF16), sds((n_early, half_d, d_ff), BF16),
        sds((n_early, d_model, half_f), F32), sds((n_early, d_model, half_f), BF16), sds((n_early, d_model, half_f), BF16),
        sds((n_ex, d_model, d_ff), F32), sds((n_ex, d_model, d_ff), F32),
        sds((n_ex, d_model // 4, d_ff), BF16), sds((n_ex, d_model // 4, d_ff), BF16),
        sds((n_ex, d_model, d_ff // 4), BF16), sds((n_ex, d_model, d_ff // 4), BF16),
        sds((6, n_ex, 8, F_BLOCK), F32),
    ]
    out_specs = [pl.BlockSpec(memory_space=ANY)] * len(outs)
    vm = pltpu.VMEM
    scratch = [
        vm((n_ex, 8, F_BLOCK), F32),
        vm((2, n_tok, F_BLOCK), BF16), vm((2, d_model, F_BLOCK), BF16), vm((2, F_BLOCK, d_model), BF16),
        vm((d_model, n_tok), BF16), vm((n_tok, d_model), BF16), vm((d_model, n_tok), BF16),
        vm((n_tok, F_BLOCK), BF16), vm((n_tok, F_BLOCK), BF16), vm((n_tok, d_model), F32),
        *[vm((IN_SLOTS, T_CHUNK, d_model), BF16)] * 4,
        vm((d_model, F_BLOCK), F32), vm((half_d, F_BLOCK), BF16), vm((d_model, F_BLOCK), F32), vm((d_model, F_BLOCK), BF16),
        pltpu.SemaphoreType.DMA((3, 2)),
        pltpu.SemaphoreType.DMA((4, IN_SLOTS)), pltpu.SemaphoreType.DMA((4,)), pltpu.SemaphoreType.DMA((2,)),
        pltpu.SemaphoreType.DMA((n_early,)), pltpu.SemaphoreType.DMA((n_early,)),
        pltpu.SemaphoreType.DMA((4,)), pltpu.SemaphoreType.DMA((4,)),
        pltpu.SemaphoreType.DMA((5,)), pltpu.SemaphoreType.DMA((5,)),
    ]
    n_dots = 4 * n_early + 3 * n_ex
    return pl.pallas_call(
        functools.partial(stack_kernel, n_layers, n_ex, n_steps),
        out_shape=outs,
        grid_spec=pltpu.PrefetchScalarGridSpec(
            num_scalar_prefetch=0, grid=(n_early + n_ex, n_steps), in_specs=[pl.BlockSpec(memory_space=ANY)] * 5, out_specs=out_specs, scratch_shapes=scratch),
        compiler_params=pltpu.CompilerParams(
            dimension_semantics=('arbitrary', 'arbitrary'), vmem_limit_bytes=VMEM_LIMIT, has_side_effects=True),
        cost_estimate=pl.CostEstimate(
            flops=2 * n_dots * n_tok * d_model * d_ff, bytes_accessed=500_000_000, transcendentals=2 * n_tok * d_ff),
        name='stack',
    )(pre_act, w_in, w_out, block_in, d_out)


def clip_kernel(norm_ref, sq_ref, out_ref):
    limit = norm_ref[0]
    for d in range(out_ref.shape[0]):
        for ex in range(out_ref.shape[1]):
            sq = jnp.sum(sq_ref[2 * d, ex] + sq_ref[2 * d + 1, ex], keepdims=True)
            root = jnp.sqrt(sq)
            factor = jnp.where(root > limit, limit / root, 1.0)
            out_ref[d, ex] = jnp.where(sq > F32_MAX, 0.0, factor)[0, 0]


def clip_factors(squares, clip_norm):
    return pl.pallas_call(
        clip_kernel,
        out_shape=jax.ShapeDtypeStruct((3, squares.shape[1]), F32),
        in_specs=[pl.BlockSpec(memory_space=pltpu.SMEM), pl.BlockSpec(memory_space=pltpu.VMEM)],
        out_specs=pl.BlockSpec(memory_space=pltpu.SMEM),
        name='clip',
    )(clip_norm.reshape(1), squares)


def mix_kernel(factors, sc_ref, clip_ref, *refs):
    def group(r, carry):
        rows = pl.ds(pl.multiple_of(r * MIX_ROWS, MIX_ROWS), MIX_ROWS)
        total = None
        for at, ref in zip(factors, refs):
            value = ref[0, rows, :].astype(F32)
            if at is not None:
                value = value * clip_ref[at[0], at[1]]
            total = value if total is None else total + value
        refs[-1][rows, :] = total.astype(BF16)
        return carry

    lax.fori_loop(0, refs[-1].shape[0] // MIX_ROWS, group, 0)


def mix(which, shape, terms, clip, before, part, n_parts):
    rows, width = shape
    part_width = width // n_parts
    n_blocks = 4 if n_parts == 1 else 2
    block = (rows, part_width // n_blocks) if which == 0 else (rows // n_blocks, part_width)

    def spec(k, v, lead):
        off = part * n_blocks if which == 0 and v.shape[2] > part_width else 0
        if which == 0:
            return pl.BlockSpec((1, *block), lambda i, sc: (lead, sc[k], i + off))
        return pl.BlockSpec((1, *block), lambda i, sc: (lead, i, sc[k]))

    def place(v, p):
        return p * n_parts + part if which == 1 and v.shape[2] > part_width else p

    out_map = (lambda i, sc: (0, i)) if which == 0 else (lambda i, sc: (i, 0))
    places = jnp.stack([jnp.asarray(place(v, p), jnp.int32) for v, _, p, _ in terms])
    if before is not None:
        places, _ = lax.optimization_barrier((places, before))
    return pl.pallas_call(
        functools.partial(mix_kernel, [at for _, _, _, at in terms]),
        out_shape=jax.ShapeDtypeStruct((rows, part_width), BF16),
        grid_spec=pltpu.PrefetchScalarGridSpec(
            num_scalar_prefetch=1, grid=(n_blocks,),
            in_specs=[pl.BlockSpec(memory_space=pltpu.SMEM)] + [spec(k, v, lead) for k, (v, lead, _, _) in enumerate(terms)],
            out_specs=pl.BlockSpec(block, out_map)),
        compiler_params=pltpu.CompilerParams(dimension_semantics=('arbitrary',), vmem_limit_bytes=40_000_000),
        cost_estimate=pl.CostEstimate(
            flops=2 * len(terms) * rows * part_width, bytes_accessed=14 * rows * part_width, transcendentals=0),
        name='mix',
    )(places, clip, *[v for v, _, _, _ in terms])


def put_in_kernel(sc_ref, coef_ref, piece_ref, noise_ref, *rest):
    out_ref = rest[-1]

    def group(r, carry):
        rows = pl.ds(pl.multiple_of(r * 16, 16), 16)
        out_ref[0, 0, rows, :] = (piece_ref[rows, :].astype(F32) + coef_ref[0] * noise_ref[0, 0, rows, :]) * coef_ref[1]
        return carry

    lax.fori_loop(0, piece_ref.shape[0] // 16, group, 0)


def put_out_kernel(sc_ref, coef_ref, piece_ref, noise_ref, *rest):
    out_ref = rest[-1]

    def group(r, carry):
        at = pl.ds(pl.multiple_of(r * 128, 128), 128)
        out_ref[0, 0, :, at] = (piece_ref[at, :].astype(F32).T + coef_ref[0] * noise_ref[0, 0, :, at]) * coef_ref[1]
        return carry

    lax.fori_loop(0, piece_ref.shape[0] // 128, group, 0, unroll=piece_ref.shape[1] == 128)


def put_piece(transposed, total, layer, quarter, part, coef, piece, noise):
    if transposed:
        rows, width = piece.shape[1], piece.shape[0]
        block = 256 if rows > 512 else 128
        first = part * (rows // block)
        piece_spec = pl.BlockSpec((width, block), lambda i, sc: (0, i))
        big_spec = pl.BlockSpec((1, 1, block, width), lambda i, sc: (sc[0], sc[1], first + i, 0))
    else:
        rows, width = piece.shape
        block = rows // 2
        piece_spec = pl.BlockSpec((block, width), lambda i, sc: (i, 0))
        big_spec = pl.BlockSpec((1, 1, block, width), lambda i, sc: (sc[0], sc[1], i, part))
    args = [jnp.stack([jnp.int32(layer), quarter]), coef, piece, noise]
    in_specs = [pl.BlockSpec(memory_space=pltpu.SMEM), piece_spec, big_spec]
    aliases = {}
    if total is not None:
        args.append(total)
        in_specs.append(pl.BlockSpec(memory_space=ANY))
        aliases = {4: 0}
    return pl.pallas_call(
        put_out_kernel if transposed else put_in_kernel,
        out_shape=jax.ShapeDtypeStruct(noise.shape, F32),
        grid_spec=pltpu.PrefetchScalarGridSpec(
            num_scalar_prefetch=1, grid=(rows // block,), in_specs=in_specs, out_specs=big_spec),
        input_output_aliases=aliases,
        compiler_params=pltpu.CompilerParams(dimension_semantics=('arbitrary',), vmem_limit_bytes=40_000_000),
        cost_estimate=pl.CostEstimate(flops=4 * rows * width, bytes_accessed=10 * rows * width, transcendentals=0),
        name='put_out' if transposed else 'put_in',
    )(*args)


def solution(mesh):
    data_size = mesh.shape['dp']
    swap_x = [(i, i ^ 1) for i in range(data_size)]
    swap_y = [(i, i ^ 2) for i in range(data_size)]

    def local_step(block_in, pre_act, w_in, w_out, d_out, noise_in, noise_out, clip_norm, noise_mult):
        n_layers, local_batch, _, d_model = block_in.shape
        d_ff = pre_act.shape[3]
        batch_total = local_batch * data_size
        dp = lax.axis_index('dp')
        x_pos, y_pos = lax.rem(dp, 2), dp // 2
        over_x = lambda v: lax.ppermute(v, 'dp', swap_x)
        over_y = lambda v: lax.ppermute(v, 'dp', swap_y)
        res = run_stack(pre_act, w_in, w_out, block_in, d_out)
        g1k, _, g1r, g2k, _, g2r, g1l, g2l, _, g1er, _, g2er, squares = res[3:]
        clip = clip_factors(squares, clip_norm)
        coef = jnp.stack([noise_mult * clip_norm, jnp.float32(1.0 / batch_total)])

        noise_in4 = noise_in.reshape(n_layers, 4, d_model // 4, d_ff)
        noise_out4 = noise_out.reshape(n_layers, 4, d_ff // 4, d_model)

        shapes = ((d_model // 4, d_ff), (d_model, d_ff // 4))
        at_half, at_side = (x_pos, y_pos), (y_pos, x_pos)
        over_half, over_side = (over_x, over_y), (over_y, over_x)
        early, early_far, late = (g1k, g2k), (g1r, g2r), (g1l, g2l)

        def own_terms(layer, which, half_pos, pos):
            if layer == 0:
                return [(late[which], k, 2 * half_pos + pos, (0, k)) for k in range(local_batch)]
            first = (n_layers - 1 - layer) * local_batch
            return [(early[which], first + k, pos, (0, k)) for k in range(local_batch)]

        made = []

        def mixed(which, terms, part, n_parts):
            made.append(mix(which, shapes[which], terms, clip, made[-1] if made else None, part, n_parts))
            return made[-1]

        def pair_terms(layer, which, part, to_send, *more):
            pos = 1 - at_side[which] if to_send else at_side[which]
            terms = own_terms(layer, which, at_half[which], pos)
            if layer == 0 and not to_send:
                more = (far_last[part, which], *more)
            elif layer == 0:
                terms += [((g1er, g2er)[which], k, 0, (1 + which, k)) for k in range(local_batch)]
            else:
                first = (n_layers - 1 - layer) * local_batch
                terms += [(early_far[which], first + k, pos, (1 + which, k)) for k in range(local_batch)]
            return terms + [(v[None], 0, 0, None) for v in more]

        last = [(0, part, N_PARTS) for part in range(N_PARTS)]
        turns = [(layer, 0, 1) for layer in range(n_layers - 1, 0, -1)] + last
        got, far_last, places = {}, {}, {}
        for _, part, n_parts in last:
            for which in (1, 0):
                terms = own_terms(0, which, 1 - at_half[which], at_side[which])
                far_last[part, which] = over_half[which](mixed(which, terms, part, n_parts))
        for layer, part, n_parts in turns:
            for which in (1, 0):
                value = mixed(which, pair_terms(layer, which, part, True), part, n_parts)
                got[layer, part, which] = over_side[which](value)
        n_first = len(made)
        for layer, part, n_parts in turns:
            for which in (1, 0):
                half_pos, pos = at_half[which], at_side[which]
                own = mixed(which, pair_terms(layer, which, part, False, got[layer, part, which]), part, n_parts)
                near = over_side[which](own)
                side = over_half[which](own)
                diag = over_half[which](near)
                places[layer, part, which] = (
                    (2 * half_pos + pos, own), (2 * half_pos + 1 - pos, near),
                    (2 * (1 - half_pos) + pos, side), (2 * (1 - half_pos) + 1 - pos, diag))
        order = [(turn, which, 0) for turn in turns for which in (1, 0)]
        order += [(turn, which, kind) for turn in turns for kind in (1, 2) for which in (1, 0)]
        order += [(turn, which, 3) for turn in turns for which in (1, 0)]
        grads, noises = [None, None], (noise_in4, noise_out4)
        for (layer, part, _), which, kind in order:
            at, piece = places[layer, part, which][kind]
            grads[which] = put_piece(which == 1, grads[which], layer, at, part, coef, piece, noises[which])
        grad_in, grad_out = grads
        assert (len(made), n_first, len(order)) == (N_SUM, N_FIRST, N_PUT)
        return grad_in.reshape(n_layers, d_model, d_ff), grad_out.reshape(n_layers, d_ff, d_model)

    return jax.shard_map(
        local_step,
        mesh=mesh,
        in_specs=(P(None, 'dp', None, None), P(None, 'dp', None, 'tp'), P(None, None, 'tp'), P(None, 'tp', None),
                  P('dp', None, None), P(None, None, 'tp'), P(None, 'tp', None), P(), P()),
        out_specs=(P(None, None, 'tp'), P(None, 'tp', None)),
        check_vma=False,
    )
```
